32 devices in a mesh: batch: 2 (over x), seq: 16 (over z, y, core).
Axes of the slice: x: 2, y: 2, z: 4, core: 2. Of those that a mesh axis runs over, the one named last changes fastest.
Arguments:
- hidden: bfloat16 [32, 4, 7168], P('batch'), parts along dimension 0
- cache_lens: int32 [32], P('batch'), parts along dimension 0
- c_kv: bfloat16 [32, 16384, 512], P('batch', 'seq'), parts along dimension 0
- k_r: bfloat16 [32, 16384, 64], P('batch', 'seq'), parts along dimension 0
- w_uq: bfloat16 [7168, 128, 128], P(None, 'seq')
- w_qr: bfloat16 [7168, 128, 64], P(None, 'seq')
- w_uk: bfloat16 [128, 128, 512], P('seq')
- w_uv: bfloat16 [128, 512, 128], P('seq')
- w_o: bfloat16 [128, 128, 7168], P('seq')
Outputs:
- output: bfloat16 [32, 4, 7168], P('batch'), parts along dimension 0
There are 2 independent parts. The reference program is written for one: setup_inputs(seed, part) draws one part's arguments, and reference() takes and returns one part's arrays. A program takes and returns all parts, laid end to end along the dimension named above; an argument that names none is the same for every part.
All inputs are finite; a program needn't handle non-finite values.
Results may differ from the reference program's by a relative error of at most 0.00665442.
Values are sent between devices in bfloat16 or wider.
A program may use at most 1 GiB of HBM per device.

```python
import jax
import jax.numpy as jnp
from jax import lax

ROW_COUNT = 16
CTX_LEN = 16384
Q_LEN = 4
MODEL_DIM = 7168
NUM_HEADS = 128
NOPE_DIM = 128
ROPE_DIM = 64
LATENT_DIM = 512
VALUE_DIM = 128


def setup_inputs(seed: int = 0, part: int = 0) -> dict:
    part_key = jax.random.fold_in(jax.random.key(seed), part)
    key_x, key_lens, key_cache, key_rope = jax.random.split(part_key, 4)
    key_uq, key_qr, key_uk, key_uv, key_wo = jax.random.split(jax.random.key(seed + 1), 5)
    hidden = jax.random.normal(key_x, (ROW_COUNT, Q_LEN, MODEL_DIM), jnp.float32)
    short_by = jax.random.randint(key_lens, (ROW_COUNT,), 0, CTX_LEN // 4 + 1)
    cache_lens = (CTX_LEN - Q_LEN - short_by).at[0].set(CTX_LEN - Q_LEN)
    c_kv = jax.random.normal(key_cache, (ROW_COUNT, CTX_LEN, LATENT_DIM), jnp.float32)
    k_r = jax.random.normal(key_rope, (ROW_COUNT, CTX_LEN, ROPE_DIM), jnp.float32)
    w_uq = jax.random.normal(key_uq, (MODEL_DIM, NUM_HEADS, NOPE_DIM), jnp.float32) * MODEL_DIM ** -0.5
    w_qr = jax.random.normal(key_qr, (MODEL_DIM, NUM_HEADS, ROPE_DIM), jnp.float32) * (2.0 * MODEL_DIM ** -0.5)
    w_uk = jax.random.normal(key_uk, (NUM_HEADS, NOPE_DIM, LATENT_DIM), jnp.float32) * (2.0 * NOPE_DIM ** -0.5)
    w_uv = jax.random.normal(key_uv, (NUM_HEADS, LATENT_DIM, VALUE_DIM), jnp.float32) * LATENT_DIM ** -0.5
    w_o = jax.random.normal(key_wo, (NUM_HEADS, VALUE_DIM, MODEL_DIM), jnp.float32) * (2.0 * (NUM_HEADS * VALUE_DIM) ** -0.5)
    return {
        "hidden": hidden.astype(jnp.bfloat16),
        "cache_lens": cache_lens.astype(jnp.int32),
        "c_kv": c_kv.astype(jnp.bfloat16),
        "k_r": k_r.astype(jnp.bfloat16),
        "w_uq": w_uq.astype(jnp.bfloat16),
        "w_qr": w_qr.astype(jnp.bfloat16),
        "w_uk": w_uk.astype(jnp.bfloat16),
        "w_uv": w_uv.astype(jnp.bfloat16),
        "w_o": w_o.astype(jnp.bfloat16),
    }


def reference(hidden, cache_lens, c_kv, k_r, w_uq, w_qr, w_uk, w_uv, w_o):
    hidden_wide = hidden.astype(jnp.float32)
    q_nope = jnp.einsum("bqd,dhk->bqhk", hidden_wide, w_uq.astype(jnp.float32)).astype(jnp.bfloat16)
    q_rope = jnp.einsum("bqd,dhr->bqhr", hidden_wide, w_qr.astype(jnp.float32)).astype(jnp.bfloat16)
    q_lat = jnp.einsum("bqhk,hkc->bqhc", q_nope.astype(jnp.float32), w_uk.astype(jnp.float32)).astype(jnp.bfloat16)
    score_scale = (NOPE_DIM + ROPE_DIM) ** -0.5
    positions = jnp.arange(CTX_LEN)
    offsets = jnp.arange(Q_LEN)

    def row_attend(row_args):
        lat_row, rope_row, cache_row, key_row, row_len = row_args
        cache_wide = cache_row.astype(jnp.float32)
        scores = (jnp.einsum("qhc,tc->qht", lat_row.astype(jnp.float32), cache_wide)
                  + jnp.einsum("qhr,tr->qht", rope_row.astype(jnp.float32), key_row.astype(jnp.float32))) * score_scale
        visible = positions[None, None, :] <= (row_len + offsets)[:, None, None]
        probs = jax.nn.softmax(jnp.where(visible, scores, -jnp.inf), axis=-1)
        return jnp.einsum("qht,tc->qhc", probs, cache_wide)

    o_lat = lax.map(row_attend, (q_lat, q_rope, c_kv, k_r, cache_lens)).astype(jnp.bfloat16)
    o_val = jnp.einsum("bqhc,hcv->bqhv", o_lat.astype(jnp.float32), w_uv.astype(jnp.float32)).astype(jnp.bfloat16)
    y_sum = jnp.einsum("bqhv,hvd->bqd", o_val.astype(jnp.float32), w_o.astype(jnp.float32))
    return (hidden_wide + y_sum).astype(jnp.bfloat16)
```

```python
import functools
import math

import jax
import jax.numpy as jnp
from jax import lax
from jax.experimental import pallas as pl
from jax.experimental.pallas import tpu as pltpu
from jax.sharding import PartitionSpec as P

MASK_FILL = -1e30
NZ, NY, NC = 4, 2, 2
MESH = pl.DeviceIdType.MESH
f32, bf16 = jnp.float32, jnp.bfloat16


def place():
    s = lax.axis_index("seq")
    return s, s // (NY * NC), (s // NC) % NY, s % NC


def seq_of(z, y, c):
    return (z * NY + y) * NC + c


def remote(src, dst, send_sem, recv_sem, seq):
    return pltpu.make_async_remote_copy(
        src_ref=src, dst_ref=dst, send_sem=send_sem, recv_sem=recv_sem,
        device_id={"seq": seq}, device_id_type=MESH)


def meet(peers):
    barrier = pltpu.get_barrier_semaphore()
    for p in peers:
        pl.semaphore_signal(barrier, inc=1, device_id={"seq": p}, device_id_type=MESH)
    pl.semaphore_wait(barrier, len(peers))


def columns(rows):
    pad = jnp.zeros((128 - rows.shape[0], 128), f32)
    return jnp.concatenate([rows, pad], axis=0).T


def attend_kernel(scale, lens, q_hbm, c_hbm, k_hbm, out,
                  qbuf, ck, kr, o_full, ml0, ml1, ml2, rc_c, ml_c, rc_y, ml_y, rc_z, ml_z, wcol,
                  q_sem, c_sem, k_sem,
                  az_s, az_r, ay_s, ay_r, ac_s, ac_r,
                  oc_s, oc_r, oy_s, oy_r, oz_s, oz_r,
                  mc_s, mc_r, my_s, my_r, mz_s, mz_r):
    nb, slots = q_hbm.shape[0], ck.shape[0]
    local_len = ck.shape[1]
    s, z, y, c = place()
    core_peer, y_peer = seq_of(z, y, 1 - c), seq_of(z, 1 - y, c)
    zs = [lax.rem(z + d, NZ) for d in (1, 2, 3)]
    zf = [lax.rem(z + NZ - d, NZ) for d in (1, 2, 3)]
    base = c * 8 + y * 4
    mine = base + z

    own_q = pltpu.make_async_copy(q_hbm, qbuf.at[:, mine], q_sem)
    own_q.start()

    def cache(b):
        k = lax.rem(b, slots)
        return (pltpu.make_async_copy(c_hbm.at[b], ck.at[k], c_sem.at[k]),
                pltpu.make_async_copy(k_hbm.at[b], kr.at[k], k_sem.at[k]))

    for b in range(slots - 1):
        for cp in cache(b):
            cp.start()

    meet([core_peer, y_peer] + [seq_of(p, y, c) for p in zs])
    own_q.wait()

    def gather_z(b, d, peer, blk):
        return remote(qbuf.at[b, blk], qbuf.at[b, blk], az_s.at[b, d], az_r.at[b, d], seq_of(peer, y, c))

    def gather_y(b, yy):
        part = qbuf.at[b, pl.ds(c * 8 + yy * 4, 4)]
        return remote(part, part, ay_s.at[b], ay_r.at[b], y_peer)

    def gather_c(b, cc):
        part = qbuf.at[b, pl.ds(cc * 8, 8)]
        return remote(part, part, ac_s.at[b], ac_r.at[b], core_peer)

    def sum_c(b):
        return (remote(o_full.at[b, pl.ds((1 - c) * 8, 8)], rc_c.at[b], oc_s.at[b], oc_r.at[b], core_peer),
                remote(ml0.at[b, 1 - c], ml_c.at[b], mc_s.at[b], mc_r.at[b], core_peer))

    def sum_y(b):
        return (remote(o_full.at[b, pl.ds(c * 8 + (1 - y) * 4, 4)], rc_y.at[b], oy_s.at[b], oy_r.at[b], y_peer),
                remote(ml1.at[b], ml_y.at[b], my_s.at[b], my_r.at[b], y_peer))

    def sum_z(b, d):
        peer = seq_of(zs[d], y, c)
        return (remote(o_full.at[b, base + zs[d]], rc_z.at[d, b], oz_s.at[b, d], oz_r.at[b, d], peer),
                remote(ml2.at[b], ml_z.at[d, b], mz_s.at[b, d], mz_r.at[b, d], peer))

    def send_z(b):
        for d in range(3):
            gather_z(b, d, zs[d], mine).start()

    def step_a(b):
        for d in range(3):
            gather_z(b, d, zs[d], base + zf[d]).wait_recv()
        gather_y(b, y).start()

    def step_b(b):
        gather_y(b, 1 - y).wait_recv()
        gather_c(b, c).start()

    def attend(b):
        gather_c(b, 1 - c).wait_recv()
        for cp in cache(b):
            cp.wait()

        @pl.when(b + slots - 1 < nb)
        def _():
            for cp in cache(b + slots - 1):
                cp.start()

        k = lax.rem(b, slots)
        row_len = lens[b]
        pos = s * local_len + lax.broadcasted_iota(jnp.int32, (256, local_len), 1)
        token = lax.rem(lax.broadcasted_iota(jnp.int32, (256, 1), 0), 16) // 8
        lane = lax.broadcasted_iota(jnp.int32, (256, 128), 1)
        for hf in range(2):
            q = jnp.concatenate([qbuf[b, :, hf * 4 + j].reshape(256, 128) for j in range(4)], axis=1)
            qr = qbuf[b, :, 8].reshape(256, 128)[:, hf * 64:(hf + 1) * 64]
            sc = lax.dot_general(q, ck[k], (((1,), (1,)), ((), ())), preferred_element_type=f32)
            sc = sc + jnp.dot(qr, kr[k], preferred_element_type=f32)
            sc = jnp.where(pos <= row_len + hf * 2 + token, sc, MASK_FILL)
            m = jnp.max(sc, axis=1, keepdims=True)
            p = jnp.exp2((sc - m) * scale)
            l = jnp.sum(p, axis=1, keepdims=True)
            o = jnp.dot(p.astype(bf16), ck[k], preferred_element_type=f32)
            o_full[b, :, hf * 16:(hf + 1) * 16, :] = o.reshape(16, 16, o.shape[1])
            stat = jnp.where(lane == 0, m * scale, jnp.where(lane == 1, l, 0.0)).T
            for cc in range(2):
                ml0[b, cc, hf * 2:hf * 2 + 2, :] = stat[0:2, cc * 128:(cc + 1) * 128]
        for cp in sum_c(b):
            cp.start()

    def merge_stats(a, r):
        stats, factors = [], []
        for hf in range(2):
            ma, la, mb, lb = (a[2 * hf:2 * hf + 1], a[2 * hf + 1:2 * hf + 2], r[2 * hf:2 * hf + 1], r[2 * hf + 1:2 * hf + 2])
            top = jnp.maximum(ma, mb)
            wa, wb = jnp.exp2(ma - top), jnp.exp2(mb - top)
            stats += [top, la * wa + lb * wb]
            factors += [wa, wb]
        return jnp.concatenate(stats, axis=0), columns(jnp.concatenate(factors, axis=0))

    def step_d(b):
        for cp in sum_c(b):
            cp.wait_recv()
        stats, cols = merge_stats(ml0[b, c, 0:4], ml_c[b, 0:4])
        ml1[b, 0:4, :] = stats
        for hf in range(2):
            rows = pl.ds(hf * 16, 16)
            wa, wb = (cols[:, 2 * hf + j:2 * hf + j + 1].reshape(8, 16, 1) for j in range(2))
            part = pl.ds(c * 8, 8)
            o_full[b, part, rows, :] = o_full[b, part, rows, :] * wa + rc_c[b, :, rows, :] * wb
        for cp in sum_y(b):
            cp.start()

    def step_e(b):
        for cp in sum_y(b):
            cp.wait_recv()
        stats, cols = merge_stats(ml1[b, 0:4], ml_y[b, 0:4])
        ml2[b, 0:4, :] = stats
        wcol[...] = cols
        cols = wcol[pl.ds(pl.multiple_of(y * 64, 64), 64), :]
        for hf in range(2):
            rows = pl.ds(hf * 16, 16)
            wa, wb = (cols[:, 2 * hf + j:2 * hf + j + 1].reshape(4, 16, 1) for j in range(2))
            part = pl.ds(base, 4)
            o_full[b, part, rows, :] = o_full[b, part, rows, :] * wa + rc_y[b, :, rows, :] * wb
        for d in range(3):
            for cp in sum_z(b, d):
                cp.start()

    def step_f(b):
        for d in range(3):
            for cp in sum_z(b, d):
                cp.wait_recv()
        parts = [ml2[b, 0:4]] + [ml_z[d, b, 0:4] for d in range(3)]
        factors = []
        for hf in range(2):
            ms, ls = [p[2 * hf:2 * hf + 1] for p in parts], [p[2 * hf + 1:2 * hf + 2] for p in parts]
            top = functools.reduce(jnp.maximum, ms)
            ws = [jnp.exp2(m - top) for m in ms]
            total = sum(w * l for w, l in zip(ws, ls))
            factors += [w / total for w in ws]
        wcol[...] = columns(jnp.concatenate(factors, axis=0))
        cols = wcol[pl.ds(pl.multiple_of((y * 4 + z) * 16, 16), 16), :]
        for hf in range(2):
            rows = pl.ds(hf * 16, 16)
            w = [cols[:, 4 * hf + j:4 * hf + j + 1] for j in range(4)]
            o = o_full[b, mine, rows, :] * w[0]
            for d in range(3):
                o = o + rc_z[d, b, rows, :] * w[d + 1]
            out[b, rows, :] = o.astype(bf16)

    ahead = 3
    for b in range(ahead):
        send_z(b)

    steps = ((0, -ahead, send_z), (0, 0, step_a), (0, 1, step_b), (0, 4, step_d), (0, 6, step_e), (0, 8, step_f), (0, 2, attend))

    @pl.loop(0, nb + 8)
    def _(it):
        for _, lag, fn in steps:
            b = it - lag

            @pl.when((b >= 0) & (b < nb))
            def _(fn=fn, b=b):
                fn(b)

    @pl.loop(0, nb)
    def _(b):
        gather_y(b, y).wait_send()
        gather_c(b, c).wait_send()
        for d in range(3):
            gather_z(b, d, zs[d], mine).wait_send()
            for cp in sum_z(b, d):
                cp.wait_send()
        for cp in sum_c(b) + sum_y(b):
            cp.wait_send()


def attend_all(q, lens, c_kv, k_t, score_scale):
    nb, local_len, lat = c_kv.shape
    slots = 3
    dma = pltpu.SemaphoreType.DMA
    return pl.pallas_call(
        functools.partial(attend_kernel, score_scale * math.log2(math.e)),
        out_shape=jax.ShapeDtypeStruct((nb, 32, lat), bf16),
        in_specs=[pl.BlockSpec(memory_space=pltpu.SMEM)] + [pl.BlockSpec(memory_space=pl.ANY)] * 3,
        out_specs=pl.BlockSpec(memory_space=pltpu.VMEM),
        scratch_shapes=[
            pltpu.VMEM((nb, 16, 9, 16, 128), bf16),
            pltpu.VMEM((slots, local_len, lat), bf16),
            pltpu.VMEM((slots, k_t.shape[1], local_len), bf16),
            pltpu.VMEM((nb, 16, 32, lat), f32),
            pltpu.VMEM((nb, 2, 8, 128), f32),
            pltpu.VMEM((nb, 8, 128), f32),
            pltpu.VMEM((nb, 8, 128), f32),
            pltpu.VMEM((nb, 8, 32, lat), f32),
            pltpu.VMEM((nb, 8, 128), f32),
            pltpu.VMEM((nb, 4, 32, lat), f32),
            pltpu.VMEM((nb, 8, 128), f32),
            pltpu.VMEM((3, nb, 32, lat), f32),
            pltpu.VMEM((3, nb, 8, 128), f32),
            pltpu.VMEM((128, 128), f32),
            dma, dma((slots,)), dma((slots,)),
            dma((nb, 3)), dma((nb, 3)), dma((nb,)), dma((nb,)), dma((nb,)), dma((nb,)),
            dma((nb,)), dma((nb,)), dma((nb,)), dma((nb,)), dma((nb, 3)), dma((nb, 3)),
            dma((nb,)), dma((nb,)), dma((nb,)), dma((nb,)), dma((nb, 3)), dma((nb, 3)),
        ],
        compiler_params=pltpu.CompilerParams(
            collective_id=0, has_side_effects=True, vmem_limit_bytes=64 * 1024 * 1024 - 65536),
        name="attend_all",
    )(lens, q, c_kv, k_t)


def total_kernel(y_ref, h_ref, out, acc, rc1, rc2, gat, s1, r1, s2, r2, s3, r3, s4, r4):
    _, z, y, c = place()
    rows, half = y_ref.shape[0], y_ref.shape[1] // 2
    wide, deep = half // NY, rows // NZ
    core_peer = seq_of(z, y, 1 - c)
    me = z * NY + y
    tos = [lax.rem(me + d, 8) for d in range(1, 8)]
    froms = [lax.rem(me + 8 - d, 8) for d in range(1, 8)]
    meet([core_peer] + [t * NC + c for t in tos])

    def lanes(cc):
        return pl.ds(pl.multiple_of(cc * half, 128), half)

    swap = remote(y_ref.at[:, lanes(1 - c)], rc1, s1, r1, core_peer)
    swap.start()
    swap.wait_recv()
    acc[...] = y_ref[:, lanes(c)] + rc1[...]

    def piece(chip):
        return pl.ds((chip // NY) * deep, deep), pl.ds(pl.multiple_of((chip % NY) * wide, 128), wide)

    def out_piece(chip):
        return pl.ds((chip // NY) * deep, deep), pl.ds(pl.multiple_of(c * half + (chip % NY) * wide, 128), wide)

    first = [remote(acc.at[piece(tos[d])], rc2.at[d], s2.at[d], r2.at[d], tos[d] * NC + c) for d in range(7)]
    for cp in first:
        cp.start()
    for cp in first:
        cp.wait_recv()
    total = acc[piece(me)]
    for d in range(7):
        total = total + rc2[d]
    gat[out_piece(me)] = (h_ref[out_piece(me)].astype(f32) + total).astype(bf16)
    second = [remote(gat.at[out_piece(me)], gat.at[out_piece(me)], s3.at[d], r3.at[d], tos[d] * NC + c) for d in range(7)]
    for cp in second:
        cp.start()
    for d in range(7):
        blk = gat.at[out_piece(froms[d])]
        remote(blk, blk, s3.at[d], r3.at[d], tos[d] * NC + c).wait_recv()
    last = remote(gat.at[:, lanes(c)], gat.at[:, lanes(c)], s4, r4, core_peer)
    last.start()
    other = gat.at[:, lanes(1 - c)]
    remote(other, other, s4, r4, core_peer).wait_recv()
    out[...] = gat[...]
    for cp in [swap, last] + first + second:
        cp.wait_send()


def total_all(y_part, hidden):
    n, dim = y_part.shape
    dma = pltpu.SemaphoreType.DMA
    vm = pl.BlockSpec(memory_space=pltpu.VMEM)
    return pl.pallas_call(
        total_kernel,
        out_shape=jax.ShapeDtypeStruct((n, dim), bf16),
        in_specs=[vm, vm],
        out_specs=vm,
        scratch_shapes=[
            pltpu.VMEM((n, dim // 2), f32), pltpu.VMEM((n, dim // 2), f32),
            pltpu.VMEM((7, n // NZ, dim // 4), f32), pltpu.VMEM((n, dim), bf16),
            dma, dma, dma((7,)), dma((7,)), dma((7,)), dma((7,)), dma, dma,
        ],
        compiler_params=pltpu.CompilerParams(
            collective_id=1, has_side_effects=True, vmem_limit_bytes=32 * 1024 * 1024),
        name="total_all",
    )(y_part, hidden)


def solution(mesh):
    def local_step(hidden, cache_lens, c_kv, k_r, w_uq, w_qr, w_uk, w_uv, w_o):
        score_scale = (w_uq.shape[2] + w_qr.shape[2]) ** -0.5
        nb, nq, dim = hidden.shape
        nh, lat = w_uk.shape[0], w_uk.shape[2]
        q_nope = jnp.einsum("cre,eil->cril", hidden, w_uq, preferred_element_type=f32).astype(bf16)
        q_rope = jnp.einsum("cre,eis->cris", hidden, w_qr, preferred_element_type=f32).astype(bf16)
        q_lat = jnp.einsum("bqhk,hkc->bqhc", q_nope, w_uk, preferred_element_type=f32).astype(bf16)
        q_a = q_lat.reshape(nb, 2, 16, 4, 128).transpose(0, 1, 3, 2, 4).reshape(nb, 8, 16, 128)
        q_b = q_rope.reshape(nb, 2, 16, 64).transpose(0, 2, 1, 3).reshape(nb, 1, 16, 128)
        q = jnp.concatenate([q_a, q_b], axis=1)
        o_lat = attend_all(q, cache_lens, c_kv, jnp.swapaxes(k_r, 1, 2), score_scale)
        o_lat = o_lat.reshape(nb * nq, nh, lat)
        o_val = jnp.einsum("nhc,hcv->nhv", o_lat, w_uv, preferred_element_type=f32).astype(bf16)
        y_part = jnp.einsum("niw,iwe->ne", o_val, w_o, preferred_element_type=f32)
        return total_all(y_part, hidden.reshape(nb * nq, dim)).reshape(nb, nq, dim)

    specs_in = (P("batch", None, None), P("batch"), P("batch", "seq", None), P("batch", "seq", None),
                P(None, "seq", None), P(None, "seq", None), P("seq", None, None), P("seq", None, None),
                P("seq", None, None))
    return jax.shard_map(local_step, mesh=mesh, in_specs=specs_in, out_specs=P("batch", None, None), check_vma=False)
```

```python
import functools
import math

import jax
import jax.numpy as jnp
from jax import lax
from jax.experimental import pallas as pl
from jax.experimental.pallas import tpu as pltpu
from jax.sharding import PartitionSpec as P

MASK_FILL = -1e30
NZ, NY, NC = 4, 2, 2
MESH = pl.DeviceIdType.MESH
f32, bf16 = jnp.float32, jnp.bfloat16


def place():
    s = lax.axis_index("seq")
    return s, s // (NY * NC), (s // NC) % NY, s % NC


def seq_of(z, y, c):
    return (z * NY + y) * NC + c


def remote(src, dst, send_sem, recv_sem, seq):
    return pltpu.make_async_remote_copy(
        src_ref=src, dst_ref=dst, send_sem=send_sem, recv_sem=recv_sem,
        device_id={"seq": seq}, device_id_type=MESH)


def meet(peers):
    barrier = pltpu.get_barrier_semaphore()
    for p in peers:
        pl.semaphore_signal(barrier, inc=1, device_id={"seq": p}, device_id_type=MESH)
    pl.semaphore_wait(barrier, len(peers))


def columns(rows):
    pad = jnp.zeros((128 - rows.shape[0], 128), f32)
    return jnp.concatenate([rows, pad], axis=0).T


def attend_kernel(scale, lens, q_hbm, c_hbm, k_hbm, out,
                  qbuf, ck, kr, o_full, ml0, ml1, ml2, rc_c, ml_c, rc_y, ml_y,
                  rc_u, ml_u, ml_us, rc_d, ml_d, ml_ds, wcol,
                  q_sem, c_sem, k_sem,
                  ay_s, ay_r, au_s, au_r, ad_s, ad_r, ac_s, ac_r,
                  oc_s, oc_r, oy_s, oy_r, ou_s, ou_r, od_s, od_r,
                  mc_s, mc_r, my_s, my_r, mu_s, mu_r, md_s, md_r):
    nb, slots = q_hbm.shape[0], ck.shape[0]
    local_len = ck.shape[1]
    s, z, y, c = place()
    core_peer, y_peer = seq_of(z, y, 1 - c), seq_of(z, 1 - y, c)
    upper, lower = seq_of(lax.rem(z + 1, NZ), y, c), seq_of(lax.rem(z + NZ - 1, NZ), y, c)

    own_q = pltpu.make_async_copy(q_hbm, qbuf.at[:, c, y, z], q_sem)
    own_q.start()

    def cache(b):
        k = lax.rem(b, slots)
        return (pltpu.make_async_copy(c_hbm.at[b], ck.at[k], c_sem.at[k]),
                pltpu.make_async_copy(k_hbm.at[b], kr.at[k], k_sem.at[k]))

    for b in range(slots - 1):
        for cp in cache(b):
            cp.start()

    meet([core_peer, y_peer, upper, lower])
    own_q.wait()

    def gather_y(b, yy):
        part = qbuf.at[b, c, yy, z]
        return remote(part, part, ay_s.at[b], ay_r.at[b], y_peer)

    def gather_up(b, origin, d):
        part = qbuf.at[b, c, :, origin]
        return remote(part, part, au_s.at[b, d - 1], au_r.at[b, d - 1], upper)

    def gather_down(b, origin, d):
        part = qbuf.at[b, c, :, origin]
        return remote(part, part, ad_s.at[b, d - 1], ad_r.at[b, d - 1], lower)

    def gather_c(b, cc):
        part = qbuf.at[b, cc]
        return remote(part, part, ac_s.at[b], ac_r.at[b], core_peer)

    def sum_c(b, hf):
        rows = pl.ds(hf * 16, 16)
        return remote(o_full.at[b, 1 - c, :, :, rows], rc_c.at[b, :, :, rows], oc_s.at[b, hf], oc_r.at[b, hf], core_peer)

    def stat_c(b):
        return remote(ml0.at[b, 1 - c], ml_c.at[b], mc_s.at[b], mc_r.at[b], core_peer)

    def sum_y(b):
        return (remote(o_full.at[b, c, 1 - y], rc_y.at[b], oy_s.at[b], oy_r.at[b], y_peer),
                remote(ml1.at[b], ml_y.at[b], my_s.at[b], my_r.at[b], y_peer))

    def sum_up(b, dest, d):
        return remote(o_full.at[b, c, y, dest], rc_u.at[b, dest], ou_s.at[b, d - 1], ou_r.at[b, d - 1], upper)

    def stat_up(b, stat):
        return remote(stat.at[b], ml_u.at[b], mu_s.at[b], mu_r.at[b], upper)

    def sum_down(b, dest, d):
        return remote(o_full.at[b, c, y, dest], rc_d.at[b, dest], od_s.at[b, d - 1], od_r.at[b, d - 1], lower)

    def stat_down(b, stat):
        return remote(stat.at[b], ml_d.at[b], md_s.at[b], md_r.at[b], lower)

    def pass_on(b, d):
        @pl.when((z < NZ - 1) & (z - (d - 1) >= 0))
        def _():
            gather_up(b, z - (d - 1), d).start()

        @pl.when((z > 0) & (z + (d - 1) < NZ))
        def _():
            gather_down(b, z + (d - 1), d).start()

    def arrive(b, d):
        @pl.when(z - d >= 0)
        def _():
            gather_up(b, z - d, d).wait_recv()

        @pl.when(z + d < NZ)
        def _():
            gather_down(b, z + d, d).wait_recv()

    def step_z1(b):
        gather_y(b, 1 - y).wait_recv()
        pass_on(b, 1)

    def step_z2(b):
        arrive(b, 1)
        pass_on(b, 2)

    def step_z3(b):
        arrive(b, 2)
        pass_on(b, 3)

    def step_z4(b):
        arrive(b, 3)
        gather_c(b, c).start()

    def attend(b):
        gather_c(b, 1 - c).wait_recv()
        for cp in cache(b):
            cp.wait()

        @pl.when(b + slots - 1 < nb)
        def _():
            for cp in cache(b + slots - 1):
                cp.start()

        k = lax.rem(b, slots)
        row_len = lens[b]
        pos = s * local_len + lax.broadcasted_iota(jnp.int32, (256, local_len), 1)
        token = lax.rem(lax.broadcasted_iota(jnp.int32, (256, 1), 0), 16) // 8
        lane = lax.broadcasted_iota(jnp.int32, (256, 128), 1)
        for hf in range(2):
            q = jnp.concatenate([qbuf[b, :, :, :, hf * 4 + j].reshape(256, 128) for j in range(4)], axis=1)
            qr = qbuf[b, :, :, :, 8].reshape(256, 128)[:, hf * 64:(hf + 1) * 64]
            sc = lax.dot_general(q, ck[k], (((1,), (1,)), ((), ())), preferred_element_type=f32)
            sc = sc + jnp.dot(qr, kr[k], preferred_element_type=f32)
            sc = jnp.where(pos <= row_len + hf * 2 + token, sc, MASK_FILL)
            m = jnp.max(sc, axis=1, keepdims=True)
            p = jnp.exp2((sc - m) * scale)
            l = jnp.sum(p, axis=1, keepdims=True)
            o = jnp.dot(p.astype(bf16), ck[k], preferred_element_type=f32)
            o_full[b, :, :, :, hf * 16:(hf + 1) * 16, :] = o.reshape(2, 2, 4, 16, o.shape[1])
            stat = jnp.where(lane == 0, m * scale, jnp.where(lane == 1, l, 0.0)).T
            for cc in range(2):
                ml0[b, cc, hf * 2:hf * 2 + 2, :] = stat[0:2, cc * 128:(cc + 1) * 128]
            sum_c(b, hf).start()
        stat_c(b).start()

    def merge_stats(parts, final):
        stats, factors = [], []
        for hf in range(2):
            ms, ls = [p[2 * hf:2 * hf + 1] for p in parts], [p[2 * hf + 1:2 * hf + 2] for p in parts]
            top = functools.reduce(jnp.maximum, ms)
            ws = [jnp.exp2(m - top) for m in ms]
            total = sum(w * l for w, l in zip(ws, ls))
            stats += [top, total]
            factors += [w / total for w in ws] if final else ws
        return jnp.concatenate(stats, axis=0), columns(jnp.concatenate(factors, axis=0))

    def step_d(b):
        for hf in range(2):
            sum_c(b, hf).wait_recv()
        stat_c(b).wait_recv()
        stats, cols = merge_stats([ml0[b, c, 0:4], ml_c[b, 0:4]], False)
        ml1[b, 0:4, :] = stats
        for hf in range(2):
            rows = pl.ds(hf * 16, 16)
            wa, wb = (cols[:, 2 * hf + j:2 * hf + j + 1].reshape(2, 4, 16, 1) for j in range(2))
            o_full[b, c, :, :, rows, :] = o_full[b, c, :, :, rows, :] * wa + rc_c[b, :, :, rows, :] * wb
        for cp in sum_y(b):
            cp.start()

    def step_e(b):
        for cp in sum_y(b):
            cp.wait_recv()
        stats, cols = merge_stats([ml1[b, 0:4], ml_y[b, 0:4]], False)
        ml2[b, 0:4, :] = stats
        wcol[...] = cols
        cols = wcol[pl.ds(pl.multiple_of(y * 64, 64), 64), :]
        for hf in range(2):
            rows = pl.ds(hf * 16, 16)
            wa, wb = (cols[:, 2 * hf + j:2 * hf + j + 1].reshape(4, 16, 1) for j in range(2))
            o_full[b, c, y, :, rows, :] = o_full[b, c, y, :, rows, :] * wa + rc_y[b, :, rows, :] * wb

        @pl.when(z == 0)
        def _():
            send_up(b, 0, ml2)

        @pl.when(z == NZ - 1)
        def _():
            send_down(b, NZ - 1, ml2)

    def send_up(b, at, stat):
        for dest in range(at + 1, NZ):
            sum_up(b, dest, dest - at).start()
        stat_up(b, stat).start()

    def send_down(b, at, stat):
        for dest in range(at - 1, -1, -1):
            sum_down(b, dest, at - dest).start()
        stat_down(b, stat).start()

    def recv_up(b, at, dests):
        for dest in dests:
            sum_up(b, dest, dest - at + 1).wait_recv()

    def recv_down(b, at, dests):
        for dest in dests:
            sum_down(b, dest, at - dest + 1).wait_recv()

    def relay(b, arrived, stat_in, stat_out, dests):
        stats, cols = merge_stats([ml2[b, 0:4], stat_in[b, 0:4]], False)
        stat_out[b, 0:4, :] = stats
        wcol[...] = cols
        for dest in dests:
            cols = wcol[pl.ds(pl.multiple_of(y * 64 + dest * 16, 16), 16), :]
            for hf in range(2):
                rows = pl.ds(hf * 16, 16)
                wa, wb = (cols[:, 2 * hf + j:2 * hf + j + 1] for j in range(2))
                o_full[b, c, y, dest, rows, :] = o_full[b, c, y, dest, rows, :] * wa + arrived[b, dest, rows, :] * wb

    def step_g(hop, b):
        @pl.when(z == hop)
        def _():
            stat_up(b, ml2).wait_recv()
            recv_up(b, hop, range(hop + 1, NZ))
            relay(b, rc_u, ml_u, ml_us, range(hop + 1, NZ))
            send_up(b, hop, ml_us)

        at = NZ - 1 - hop

        @pl.when(z == at)
        def _():
            stat_down(b, ml2).wait_recv()
            recv_down(b, at, range(at - 1, -1, -1))
            relay(b, rc_d, ml_d, ml_ds, range(at - 1, -1, -1))
            send_down(b, at, ml_ds)

    def finish(b, at):
        parts, sums = [ml2[b, 0:4]], [o_full.at[b, c, y, at]]
        if at > 0:
            recv_up(b, at, [at])
            if at == NZ - 1:
                stat_up(b, ml2).wait_recv()
            parts.append(ml_u[b, 0:4])
            sums.append(rc_u.at[b, at])
        if at < NZ - 1:
            recv_down(b, at, [at])
            if at == 0:
                stat_down(b, ml2).wait_recv()
            parts.append(ml_d[b, 0:4])
            sums.append(rc_d.at[b, at])
        wcol[...] = merge_stats(parts, True)[1]
        cols = wcol[pl.ds(pl.multiple_of(y * 64 + at * 16, 16), 16), :]
        n = len(parts)
        for hf in range(2):
            rows = pl.ds(hf * 16, 16)
            o = sum(part[rows, :] * cols[:, n * hf + j:n * hf + j + 1] for j, part in enumerate(sums))
            out[b, rows, :] = o.astype(bf16)

    def step_f(b):
        for at in range(NZ):
            @pl.when(z == at)
            def _(at=at):
                finish(b, at)

    @pl.loop(0, nb)
    def _(b):
        gather_y(b, y).start()

    steps = ((7, step_e), (8, functools.partial(step_g, 1)), (9, functools.partial(step_g, 2)), (10, step_f),
             (0, step_z1), (1, step_z2), (2, step_z3), (3, step_z4), (5, step_d), (4, attend))

    @pl.loop(0, nb + 10)
    def _(it):
        for lag, fn in steps:
            b = it - lag

            @pl.when((b >= 0) & (b < nb))
            def _(fn=fn, b=b):
                fn(b)

    @pl.loop(0, nb)
    def _(b):
        gather_y(b, y).wait_send()
        gather_c(b, c).wait_send()
        for d in (1, 2, 3):
            @pl.when((z < NZ - 1) & (z - (d - 1) >= 0))
            def _(d=d):
                gather_up(b, z - (d - 1), d).wait_send()

            @pl.when((z > 0) & (z + (d - 1) < NZ))
            def _(d=d):
                gather_down(b, z + (d - 1), d).wait_send()
        sum_c(b, 0).wait_send()
        sum_c(b, 1).wait_send()
        stat_c(b).wait_send()
        for cp in sum_y(b):
            cp.wait_send()
        for at in range(NZ):
            @pl.when(z == at)
            def _(at=at):
                for dest in range(at + 1, NZ):
                    sum_up(b, dest, dest - at).wait_send()
                if at < NZ - 1:
                    stat_up(b, ml2).wait_send()
                for dest in range(at):
                    sum_down(b, dest, at - dest).wait_send()
                if at > 0:
                    stat_down(b, ml2).wait_send()


def attend_all(q, lens, c_kv, k_t, score_scale):
    nb, local_len, lat = c_kv.shape
    slots = 3
    dma = pltpu.SemaphoreType.DMA
    return pl.pallas_call(
        functools.partial(attend_kernel, score_scale * math.log2(math.e)),
        out_shape=jax.ShapeDtypeStruct((nb, 32, lat), bf16),
        in_specs=[pl.BlockSpec(memory_space=pltpu.SMEM)] + [pl.BlockSpec(memory_space=pl.ANY)] * 3,
        out_specs=pl.BlockSpec(memory_space=pltpu.VMEM),
        scratch_shapes=[
            pltpu.VMEM((nb, 2, 2, 4, 9, 16, 128), bf16),
            pltpu.VMEM((slots, local_len, lat), bf16),
            pltpu.VMEM((slots, k_t.shape[1], local_len), bf16),
            pltpu.VMEM((nb, 2, 2, 4, 32, lat), f32),
            pltpu.VMEM((nb, 2, 8, 128), f32),
            pltpu.VMEM((nb, 8, 128), f32),
            pltpu.VMEM((nb, 8, 128), f32),
            pltpu.VMEM((nb, 2, 4, 32, lat), f32),
            pltpu.VMEM((nb, 8, 128), f32),
            pltpu.VMEM((nb, 4, 32, lat), f32),
            pltpu.VMEM((nb, 8, 128), f32),
            pltpu.VMEM((nb, 4, 32, lat), f32),
            pltpu.VMEM((nb, 8, 128), f32),
            pltpu.VMEM((nb, 8, 128), f32),
            pltpu.VMEM((nb, 4, 32, lat), f32),
            pltpu.VMEM((nb, 8, 128), f32),
            pltpu.VMEM((nb, 8, 128), f32),
            pltpu.VMEM((128, 128), f32),
            dma, dma((slots,)), dma((slots,)),
            dma((nb,)), dma((nb,)), dma((nb, 3)), dma((nb, 3)), dma((nb, 3)), dma((nb, 3)), dma((nb,)), dma((nb,)),
            dma((nb, 2)), dma((nb, 2)), dma((nb,)), dma((nb,)), dma((nb, 3)), dma((nb, 3)), dma((nb, 3)), dma((nb, 3)),
            dma((nb,)), dma((nb,)), dma((nb,)), dma((nb,)), dma((nb,)), dma((nb,)), dma((nb,)), dma((nb,)),
        ],
        compiler_params=pltpu.CompilerParams(
            collective_id=0, has_side_effects=True, vmem_limit_bytes=64 * 1024 * 1024 - 65536),
        name="attend_all",
    )(lens, q, c_kv, k_t)


def total_kernel(y_ref, h_ref, out, acc, rc1, rc2, gat, s1, r1, s2, r2, s3, r3, s4, r4):
    _, z, y, c = place()
    rows, half = y_ref.shape[0], y_ref.shape[1] // 2
    wide, deep = half // NY, rows // NZ
    core_peer = seq_of(z, y, 1 - c)
    me = z * NY + y
    tos = [lax.rem(me + d, 8) for d in range(1, 8)]
    froms = [lax.rem(me + 8 - d, 8) for d in range(1, 8)]
    meet([core_peer] + [t * NC + c for t in tos])

    def lanes(cc):
        return pl.ds(pl.multiple_of(cc * half, 128), half)

    swap = remote(y_ref.at[:, lanes(1 - c)], rc1, s1, r1, core_peer)
    swap.start()
    swap.wait_recv()
    acc[...] = y_ref[:, lanes(c)] + rc1[...]

    def piece(chip):
        return pl.ds((chip // NY) * deep, deep), pl.ds(pl.multiple_of((chip % NY) * wide, 128), wide)

    def out_piece(chip):
        return pl.ds((chip // NY) * deep, deep), pl.ds(pl.multiple_of(c * half + (chip % NY) * wide, 128), wide)

    first = [remote(acc.at[piece(tos[d])], rc2.at[d], s2.at[d], r2.at[d], tos[d] * NC + c) for d in range(7)]
    for cp in first:
        cp.start()
    for cp in first:
        cp.wait_recv()
    total = acc[piece(me)]
    for d in range(7):
        total = total + rc2[d]
    gat[out_piece(me)] = (h_ref[out_piece(me)].astype(f32) + total).astype(bf16)
    second = [remote(gat.at[out_piece(me)], gat.at[out_piece(me)], s3.at[d], r3.at[d], tos[d] * NC + c) for d in range(7)]
    for cp in second:
        cp.start()
    for d in range(7):
        blk = gat.at[out_piece(froms[d])]
        remote(blk, blk, s3.at[d], r3.at[d], tos[d] * NC + c).wait_recv()
    last = remote(gat.at[:, lanes(c)], gat.at[:, lanes(c)], s4, r4, core_peer)
    last.start()
    other = gat.at[:, lanes(1 - c)]
    remote(other, other, s4, r4, core_peer).wait_recv()
    out[...] = gat[...]
    for cp in [swap, last] + first + second:
        cp.wait_send()


def total_all(y_part, hidden):
    n, dim = y_part.shape
    dma = pltpu.SemaphoreType.DMA
    vm = pl.BlockSpec(memory_space=pltpu.VMEM)
    return pl.pallas_call(
        total_kernel,
        out_shape=jax.ShapeDtypeStruct((n, dim), bf16),
        in_specs=[vm, vm],
        out_specs=vm,
        scratch_shapes=[
            pltpu.VMEM((n, dim // 2), f32), pltpu.VMEM((n, dim // 2), f32),
            pltpu.VMEM((7, n // NZ, dim // 4), f32), pltpu.VMEM((n, dim), bf16),
            dma, dma, dma((7,)), dma((7,)), dma((7,)), dma((7,)), dma, dma,
        ],
        compiler_params=pltpu.CompilerParams(
            collective_id=1, has_side_effects=True, vmem_limit_bytes=32 * 1024 * 1024),
        name="total_all",
    )(y_part, hidden)


def solution(mesh):
    def local_step(hidden, cache_lens, c_kv, k_r, w_uq, w_qr, w_uk, w_uv, w_o):
        score_scale = (w_uq.shape[2] + w_qr.shape[2]) ** -0.5
        nb, nq, dim = hidden.shape
        nh, lat = w_uk.shape[0], w_uk.shape[2]
        q_nope = jnp.einsum("cre,eil->cril", hidden, w_uq, preferred_element_type=f32).astype(bf16)
        q_rope = jnp.einsum("cre,eis->cris", hidden, w_qr, preferred_element_type=f32).astype(bf16)
        q_lat = jnp.einsum("bqhk,hkc->bqhc", q_nope, w_uk, preferred_element_type=f32).astype(bf16)
        q_a = q_lat.reshape(nb, 2, 16, 4, 128).transpose(0, 1, 3, 2, 4).reshape(nb, 8, 16, 128)
        q_b = q_rope.reshape(nb, 2, 16, 64).transpose(0, 2, 1, 3).reshape(nb, 1, 16, 128)
        q = jnp.concatenate([q_a, q_b], axis=1)
        o_lat = attend_all(q, cache_lens, c_kv, jnp.swapaxes(k_r, 1, 2), score_scale)
        o_lat = o_lat.reshape(nb * nq, nh, lat)
        o_val = jnp.einsum("nhc,hcv->nhv", o_lat, w_uv, preferred_element_type=f32).astype(bf16)
        y_part = jnp.einsum("niw,iwe->ne", o_val, w_o, preferred_element_type=f32)
        return total_all(y_part, hidden.reshape(nb * nq, dim)).reshape(nb, nq, dim)

    specs_in = (P("batch", None, None), P("batch"), P("batch", "seq", None), P("batch", "seq", None),
                P(None, "seq", None), P(None, "seq", None), P("seq", None, None), P("seq", None, None),
                P("seq", None, None))
    return jax.shard_map(local_step, mesh=mesh, in_specs=specs_in, out_specs=P("batch", None, None), check_vma=False)
```

```python
import functools
import math

import jax
import jax.numpy as jnp
from jax import lax
from jax.experimental import pallas as pl
from jax.experimental.pallas import tpu as pltpu
from jax.sharding import PartitionSpec as P

MASK_FILL = -1e30
NZ, NY, NC = 4, 2, 2
MESH = pl.DeviceIdType.MESH
f32, bf16 = jnp.float32, jnp.bfloat16


def place():
    s = lax.axis_index("seq")
    return s, s // (NY * NC), (s // NC) % NY, s % NC


def seq_of(z, y, c):
    return (z * NY + y) * NC + c


def remote(src, dst, send_sem, recv_sem, seq):
    return pltpu.make_async_remote_copy(
        src_ref=src, dst_ref=dst, send_sem=send_sem, recv_sem=recv_sem,
        device_id={"seq": seq}, device_id_type=MESH)


def meet(peers):
    barrier = pltpu.get_barrier_semaphore()
    for p in peers:
        pl.semaphore_signal(barrier, inc=1, device_id={"seq": p}, device_id_type=MESH)
    pl.semaphore_wait(barrier, len(peers))


def columns(rows):
    pad = jnp.zeros((128 - rows.shape[0], 128), f32)
    return jnp.concatenate([rows, pad], axis=0).T


def attend_kernel(scale, lens, q_hbm, c_hbm, k_hbm, wuv, out,
                  qbuf, ck, kr, o_full, ml0, ml1, ml2, rc_c, ml_c, rc_y, ml_y,
                  rc_u, ml_u, ml_us, rc_d, ml_d, ml_ds, wcol,
                  q_sem, c_sem, k_sem,
                  ay_s, ay_r, au_s, au_r, ad_s, ad_r, ac_s, ac_r,
                  oc_s, oc_r, oy_s, oy_r, ou_s, ou_r, od_s, od_r,
                  mc_s, mc_r, my_s, my_r, mu_s, mu_r, md_s, md_r):
    nb, slots = q_hbm.shape[0], ck.shape[0]
    local_len = ck.shape[1]
    s, z, y, c = place()
    core_peer, y_peer = seq_of(z, y, 1 - c), seq_of(z, 1 - y, c)
    upper, lower = seq_of(lax.rem(z + 1, NZ), y, c), seq_of(lax.rem(z + NZ - 1, NZ), y, c)

    own_q = pltpu.make_async_copy(q_hbm, qbuf.at[:, c, y, z], q_sem)
    own_q.start()

    def cache(b):
        k = lax.rem(b, slots)
        return (pltpu.make_async_copy(c_hbm.at[b], ck.at[k], c_sem.at[k]),
                pltpu.make_async_copy(k_hbm.at[b], kr.at[k], k_sem.at[k]))

    for b in range(slots - 1):
        for cp in cache(b):
            cp.start()

    meet([core_peer, y_peer, upper, lower])
    own_q.wait()

    def gather_y(b, yy):
        part = qbuf.at[b, c, yy, z]
        return remote(part, part, ay_s.at[b], ay_r.at[b], y_peer)

    def gather_up(b, origin, d):
        part = qbuf.at[b, c, :, origin]
        return remote(part, part, au_s.at[b, d - 1], au_r.at[b, d - 1], upper)

    def gather_down(b, origin, d):
        part = qbuf.at[b, c, :, origin]
        return remote(part, part, ad_s.at[b, d - 1], ad_r.at[b, d - 1], lower)

    def gather_c(b, cc):
        part = qbuf.at[b, cc]
        return remote(part, part, ac_s.at[b], ac_r.at[b], core_peer)

    def sum_c(b, hf):
        rows = pl.ds(hf * 16, 16)
        return remote(o_full.at[b, 1 - c, :, :, rows], rc_c.at[b, :, :, rows], oc_s.at[b, hf], oc_r.at[b, hf], core_peer)

    def stat_c(b):
        return remote(ml0.at[b, 1 - c], ml_c.at[b], mc_s.at[b], mc_r.at[b], core_peer)

    def sum_y(b):
        return (remote(o_full.at[b, c, 1 - y], rc_y.at[b], oy_s.at[b], oy_r.at[b], y_peer),
                remote(ml1.at[b], ml_y.at[b], my_s.at[b], my_r.at[b], y_peer))

    def sum_up(b, dest, d):
        return remote(o_full.at[b, c, y, dest], rc_u.at[b, dest], ou_s.at[b, d - 1], ou_r.at[b, d - 1], upper)

    def stat_up(b, stat):
        return remote(stat.at[b], ml_u.at[b], mu_s.at[b], mu_r.at[b], upper)

    def sum_down(b, dest, d):
        return remote(o_full.at[b, c, y, dest], rc_d.at[b, dest], od_s.at[b, d - 1], od_r.at[b, d - 1], lower)

    def stat_down(b, stat):
        return remote(stat.at[b], ml_d.at[b], md_s.at[b], md_r.at[b], lower)

    def pass_on(b, d):
        @pl.when((z < NZ - 1) & (z - (d - 1) >= 0))
        def _():
            gather_up(b, z - (d - 1), d).start()

        @pl.when((z > 0) & (z + (d - 1) < NZ))
        def _():
            gather_down(b, z + (d - 1), d).start()

    def arrive(b, d):
        @pl.when(z - d >= 0)
        def _():
            gather_up(b, z - d, d).wait_recv()

        @pl.when(z + d < NZ)
        def _():
            gather_down(b, z + d, d).wait_recv()

    def step_z1(b):
        gather_y(b, 1 - y).wait_recv()
        pass_on(b, 1)

    def step_z2(b):
        arrive(b, 1)
        pass_on(b, 2)

    def step_z3(b):
        arrive(b, 2)
        pass_on(b, 3)

    def step_z4(b):
        arrive(b, 3)
        gather_c(b, c).start()

    def attend(b):
        gather_c(b, 1 - c).wait_recv()
        for cp in cache(b):
            cp.wait()

        @pl.when(b + slots - 1 < nb)
        def _():
            for cp in cache(b + slots - 1):
                cp.start()

        k = lax.rem(b, slots)
        row_len = lens[b]
        pos = s * local_len + lax.broadcasted_iota(jnp.int32, (256, local_len), 1)
        token = lax.rem(lax.broadcasted_iota(jnp.int32, (256, 1), 0), 16) // 8
        lane = lax.broadcasted_iota(jnp.int32, (256, 128), 1)
        for hf in range(2):
            q = jnp.concatenate([qbuf[b, :, :, :, hf * 4 + j].reshape(256, 128) for j in range(4)], axis=1)
            qr = qbuf[b, :, :, :, 8].reshape(256, 128)[:, hf * 64:(hf + 1) * 64]
            sc = lax.dot_general(q, ck[k], (((1,), (1,)), ((), ())), preferred_element_type=f32)
            sc = sc + jnp.dot(qr, kr[k], preferred_element_type=f32)
            sc = jnp.where(pos <= row_len + hf * 2 + token, sc, MASK_FILL)
            m = jnp.max(sc, axis=1, keepdims=True)
            p = jnp.exp2((sc - m) * scale)
            l = jnp.sum(p, axis=1, keepdims=True)
            o = jnp.dot(p.astype(bf16), ck[k], preferred_element_type=f32)
            o_full[b, :, :, :, hf * 16:(hf + 1) * 16, :] = o.reshape(2, 2, 4, 16, o.shape[1])
            stat = jnp.where(lane == 0, m * scale, jnp.where(lane == 1, l, 0.0)).T
            for cc in range(2):
                ml0[b, cc, hf * 2:hf * 2 + 2, :] = stat[0:2, cc * 128:(cc + 1) * 128]
            sum_c(b, hf).start()
        stat_c(b).start()

    def merge_stats(parts, final):
        stats, factors = [], []
        for hf in range(2):
            ms, ls = [p[2 * hf:2 * hf + 1] for p in parts], [p[2 * hf + 1:2 * hf + 2] for p in parts]
            top = functools.reduce(jnp.maximum, ms)
            ws = [jnp.exp2(m - top) for m in ms]
            total = sum(w * l for w, l in zip(ws, ls))
            stats += [top, total]
            factors += [w / total for w in ws] if final else ws
        return jnp.concatenate(stats, axis=0), columns(jnp.concatenate(factors, axis=0))

    def step_d(b):
        for hf in range(2):
            sum_c(b, hf).wait_recv()
        stat_c(b).wait_recv()
        stats, cols = merge_stats([ml0[b, c, 0:4], ml_c[b, 0:4]], False)
        ml1[b, 0:4, :] = stats
        for hf in range(2):
            rows = pl.ds(hf * 16, 16)
            wa, wb = (cols[:, 2 * hf + j:2 * hf + j + 1].reshape(2, 4, 16, 1) for j in range(2))
            o_full[b, c, :, :, rows, :] = o_full[b, c, :, :, rows, :] * wa + rc_c[b, :, :, rows, :] * wb
        for cp in sum_y(b):
            cp.start()

    def step_e(b):
        for cp in sum_y(b):
            cp.wait_recv()
        stats, cols = merge_stats([ml1[b, 0:4], ml_y[b, 0:4]], False)
        ml2[b, 0:4, :] = stats
        wcol[...] = cols
        cols = wcol[pl.ds(pl.multiple_of(y * 64, 64), 64), :]
        for hf in range(2):
            rows = pl.ds(hf * 16, 16)
            wa, wb = (cols[:, 2 * hf + j:2 * hf + j + 1].reshape(4, 16, 1) for j in range(2))
            o_full[b, c, y, :, rows, :] = o_full[b, c, y, :, rows, :] * wa + rc_y[b, :, rows, :] * wb

        @pl.when(z == 0)
        def _():
            send_up(b, 0, ml2)

        @pl.when(z == NZ - 1)
        def _():
            send_down(b, NZ - 1, ml2)

    def send_up(b, at, stat):
        for dest in range(at + 1, NZ):
            sum_up(b, dest, dest - at).start()
        stat_up(b, stat).start()

    def send_down(b, at, stat):
        for dest in range(at - 1, -1, -1):
            sum_down(b, dest, at - dest).start()
        stat_down(b, stat).start()

    def recv_up(b, at, dests):
        for dest in dests:
            sum_up(b, dest, dest - at + 1).wait_recv()

    def recv_down(b, at, dests):
        for dest in dests:
            sum_down(b, dest, at - dest + 1).wait_recv()

    def relay(b, arrived, stat_in, stat_out, dests):
        stats, cols = merge_stats([ml2[b, 0:4], stat_in[b, 0:4]], False)
        stat_out[b, 0:4, :] = stats
        wcol[...] = cols
        for dest in dests:
            cols = wcol[pl.ds(pl.multiple_of(y * 64 + dest * 16, 16), 16), :]
            for hf in range(2):
                rows = pl.ds(hf * 16, 16)
                wa, wb = (cols[:, 2 * hf + j:2 * hf + j + 1] for j in range(2))
                o_full[b, c, y, dest, rows, :] = o_full[b, c, y, dest, rows, :] * wa + arrived[b, dest, rows, :] * wb

    def step_g(hop, b):
        @pl.when(z == hop)
        def _():
            stat_up(b, ml2).wait_recv()
            recv_up(b, hop, range(hop + 1, NZ))
            relay(b, rc_u, ml_u, ml_us, range(hop + 1, NZ))
            send_up(b, hop, ml_us)

        at = NZ - 1 - hop

        @pl.when(z == at)
        def _():
            stat_down(b, ml2).wait_recv()
            recv_down(b, at, range(at - 1, -1, -1))
            relay(b, rc_d, ml_d, ml_ds, range(at - 1, -1, -1))
            send_down(b, at, ml_ds)

    def finish(b, at):
        parts, sums = [ml2[b, 0:4]], [o_full.at[b, c, y, at]]
        if at > 0:
            recv_up(b, at, [at])
            if at == NZ - 1:
                stat_up(b, ml2).wait_recv()
            parts.append(ml_u[b, 0:4])
            sums.append(rc_u.at[b, at])
        if at < NZ - 1:
            recv_down(b, at, [at])
            if at == 0:
                stat_down(b, ml2).wait_recv()
            parts.append(ml_d[b, 0:4])
            sums.append(rc_d.at[b, at])
        wcol[...] = merge_stats(parts, True)[1]
        cols = wcol[pl.ds(pl.multiple_of(y * 64 + at * 16, 16), 16), :]
        n = len(parts)
        halves = []
        for hf in range(2):
            rows = pl.ds(hf * 16, 16)
            o = sum(part[rows, :] * cols[:, n * hf + j:n * hf + j + 1] for j, part in enumerate(sums))
            halves.append(o.astype(bf16))
        o = jnp.concatenate(halves, axis=0)
        head = lax.rem(lax.broadcasted_iota(jnp.int32, (32, 128), 0), 8)
        for h in range(8):
            v = jnp.dot(o, wuv[h], preferred_element_type=f32)
            v = jnp.where(head == h, v, 0.0).reshape(4, 8, 128).sum(axis=1)
            out[b, :, h * 128:(h + 1) * 128] = v.astype(bf16)

    def step_f(b):
        for at in range(NZ):
            @pl.when(z == at)
            def _(at=at):
                finish(b, at)

    @pl.loop(0, nb)
    def _(b):
        gather_y(b, y).start()

    steps = ((7, step_e), (8, functools.partial(step_g, 1)), (9, functools.partial(step_g, 2)), (10, step_f),
             (0, step_z1), (1, step_z2), (2, step_z3), (3, step_z4), (5, step_d), (4, attend))

    @pl.loop(0, nb + 10)
    def _(it):
        for lag, fn in steps:
            b = it - lag

            @pl.when((b >= 0) & (b < nb))
            def _(fn=fn, b=b):
                fn(b)

    @pl.loop(0, nb)
    def _(b):
        gather_y(b, y).wait_send()
        gather_c(b, c).wait_send()
        for d in (1, 2, 3):
            @pl.when((z < NZ - 1) & (z - (d - 1) >= 0))
            def _(d=d):
                gather_up(b, z - (d - 1), d).wait_send()

            @pl.when((z > 0) & (z + (d - 1) < NZ))
            def _(d=d):
                gather_down(b, z + (d - 1), d).wait_send()
        sum_c(b, 0).wait_send()
        sum_c(b, 1).wait_send()
        stat_c(b).wait_send()
        for cp in sum_y(b):
            cp.wait_send()
        for at in range(NZ):
            @pl.when(z == at)
            def _(at=at):
                for dest in range(at + 1, NZ):
                    sum_up(b, dest, dest - at).wait_send()
                if at < NZ - 1:
                    stat_up(b, ml2).wait_send()
                for dest in range(at):
                    sum_down(b, dest, at - dest).wait_send()
                if at > 0:
                    stat_down(b, ml2).wait_send()


def attend_all(q, lens, c_kv, k_t, w_uv, score_scale):
    nb, local_len, lat = c_kv.shape
    slots = 3
    dma = pltpu.SemaphoreType.DMA
    return pl.pallas_call(
        functools.partial(attend_kernel, score_scale * math.log2(math.e)),
        out_shape=jax.ShapeDtypeStruct((nb, 4, w_uv.shape[0] * w_uv.shape[2]), bf16),
        in_specs=[pl.BlockSpec(memory_space=pltpu.SMEM)] + [pl.BlockSpec(memory_space=pl.ANY)] * 3
        + [pl.BlockSpec(memory_space=pltpu.VMEM)],
        out_specs=pl.BlockSpec(memory_space=pltpu.VMEM),
        scratch_shapes=[
            pltpu.VMEM((nb, 2, 2, 4, 9, 16, 128), bf16),
            pltpu.VMEM((slots, local_len, lat), bf16),
            pltpu.VMEM((slots, k_t.shape[1], local_len), bf16),
            pltpu.VMEM((nb, 2, 2, 4, 32, lat), f32),
            pltpu.VMEM((nb, 2, 8, 128), f32),
            pltpu.VMEM((nb, 8, 128), f32),
            pltpu.VMEM((nb, 8, 128), f32),
            pltpu.VMEM((nb, 2, 4, 32, lat), f32),
            pltpu.VMEM((nb, 8, 128), f32),
            pltpu.VMEM((nb, 4, 32, lat), f32),
            pltpu.VMEM((nb, 8, 128), f32),
            pltpu.VMEM((nb, 4, 32, lat), f32),
            pltpu.VMEM((nb, 8, 128), f32),
            pltpu.VMEM((nb, 8, 128), f32),
            pltpu.VMEM((nb, 4, 32, lat), f32),
            pltpu.VMEM((nb, 8, 128), f32),
            pltpu.VMEM((nb, 8, 128), f32),
            pltpu.VMEM((128, 128), f32),
            dma, dma((slots,)), dma((slots,)),
            dma((nb,)), dma((nb,)), dma((nb, 3)), dma((nb, 3)), dma((nb, 3)), dma((nb, 3)), dma((nb,)), dma((nb,)),
            dma((nb, 2)), dma((nb, 2)), dma((nb,)), dma((nb,)), dma((nb, 3)), dma((nb, 3)), dma((nb, 3)), dma((nb, 3)),
            dma((nb,)), dma((nb,)), dma((nb,)), dma((nb,)), dma((nb,)), dma((nb,)), dma((nb,)), dma((nb,)),
        ],
        compiler_params=pltpu.CompilerParams(
            collective_id=0, has_side_effects=True, vmem_limit_bytes=64 * 1024 * 1024 - 65536),
        name="attend_all",
    )(lens, q, c_kv, k_t, w_uv)


def total_kernel(ov_ref, w_hbm, h_hbm, out, wbuf, hbuf, part, gat, rc_c, rc_y, rc_z,
                 w_sem, h_sem, sc_s, sc_r, sy_s, sy_r, sz_s, sz_r, gz_s, gz_r, gy_s, gy_r, gc_s, gc_r):
    _, z, y, c = place()
    chunks, lanes = wbuf.shape[0], wbuf.shape[4]
    deep = part.shape[3] // NZ
    core_peer, y_peer = seq_of(z, y, 1 - c), seq_of(z, 1 - y, c)
    zs = [lax.rem(z + d, NZ) for d in (1, 2, 3)]
    zf = [lax.rem(z + NZ - d, NZ) for d in (1, 2, 3)]

    def where(cc, yy, k):
        return pl.ds(pl.multiple_of((cc * NY + yy) * (chunks * lanes) + k * lanes, 128), lanes)

    def weights(k):
        return [pltpu.make_async_copy(w_hbm.at[:, where(cc, yy, k)], wbuf.at[k, cc, yy], w_sem.at[k, cc * 2 + yy])
                for cc in range(2) for yy in range(2)]

    for k in range(chunks):
        for cp in weights(k):
            cp.start()
    nb = h_hbm.shape[0]
    own_h = pltpu.make_async_copy(
        h_hbm.at[pl.ds(z * (nb // NZ), nb // NZ), :, pl.ds(pl.multiple_of((c * NY + y) * (chunks * lanes), 128), chunks * lanes)],
        hbuf, h_sem)
    own_h.start()
    meet([core_peer, y_peer] + [seq_of(p, y, c) for p in zs])
    own_h.wait()

    def band(at):
        return pl.ds(pl.multiple_of(at * deep, deep), deep)

    def sum_c(k):
        return remote(part.at[k, 1 - c], rc_c.at[k], sc_s.at[k], sc_r.at[k], core_peer)

    def sum_y(k):
        return remote(part.at[k, c, 1 - y], rc_y.at[k], sy_s.at[k], sy_r.at[k], y_peer)

    def sum_z(k, d):
        return remote(part.at[k, c, y, band(zs[d])], rc_z.at[k, d], sz_s.at[k, d], sz_r.at[k, d], seq_of(zs[d], y, c))

    def give_z(k, d, at):
        piece = gat.at[k, c, y, band(at)]
        return remote(piece, piece, gz_s.at[k, d], gz_r.at[k, d], seq_of(zs[d], y, c))

    def give_y(k, yy):
        return remote(gat.at[k, c, yy], gat.at[k, c, yy], gy_s.at[k], gy_r.at[k], y_peer)

    def give_c(k, cc):
        return remote(gat.at[k, cc], gat.at[k, cc], gc_s.at[k], gc_r.at[k], core_peer)

    def multiply(k):
        for cp in weights(k):
            cp.wait()
        ov = ov_ref[...]
        for cc in (1 - c, c):
            for yy in range(2):
                part[k, cc, yy] = jnp.dot(ov, wbuf[k, cc, yy], preferred_element_type=f32)
            if cc is not c:
                sum_c(k).start()

    def step_d(k):
        sum_c(k).wait_recv()
        part[k, c] = part[k, c] + rc_c[k]
        sum_y(k).start()

    def step_e(k):
        sum_y(k).wait_recv()
        part[k, c, y] = part[k, c, y] + rc_y[k]
        for d in range(3):
            sum_z(k, d).start()

    def step_f(k):
        for d in range(3):
            sum_z(k, d).wait_recv()
        total = part[k, c, y, band(z)] + rc_z[k, 0] + rc_z[k, 1] + rc_z[k, 2]
        own = hbuf[:, :, pl.ds(pl.multiple_of(k * lanes, 128), lanes)].astype(f32).reshape(deep, lanes)
        gat[k, c, y, band(z)] = (own + total).astype(bf16)
        for d in range(3):
            give_z(k, d, z).start()

    def step_h(k):
        for d in range(3):
            give_z(k, d, zf[d]).wait_recv()
        give_y(k, y).start()

    def step_i(k):
        give_y(k, 1 - y).wait_recv()
        give_c(k, c).start()

    def step_j(k):
        give_c(k, 1 - c).wait_recv()
        for cc in range(2):
            for yy in range(2):
                out[:, :, where(cc, yy, k)] = gat[k, cc, yy].astype(f32).reshape(nb, -1, lanes).astype(bf16)

    steps = ((10, step_j), (9, step_i), (7, step_h), (5, step_f), (3, step_e), (1, step_d), (0, multiply))

    @pl.loop(0, chunks + 10)
    def _(it):
        for lag, fn in steps:
            k = it - lag

            @pl.when((k >= 0) & (k < chunks))
            def _(fn=fn, k=k):
                fn(k)

    @pl.loop(0, chunks)
    def _(k):
        sum_c(k).wait_send()
        sum_y(k).wait_send()
        for d in range(3):
            sum_z(k, d).wait_send()
            give_z(k, d, z).wait_send()
        give_y(k, y).wait_send()
        give_c(k, c).wait_send()


def total_all(ov, w_o, hidden):
    n, dim = ov.shape[0], w_o.shape[1]
    nb, nq, _ = hidden.shape
    chunks = next(k for k in (7, 1) if dim % (4 * k * 128) == 0)
    lanes = dim // (4 * chunks)
    dma = pltpu.SemaphoreType.DMA
    vm, hbm = pl.BlockSpec(memory_space=pltpu.VMEM), pl.BlockSpec(memory_space=pl.ANY)
    one, three = dma((chunks,)), dma((chunks, 3))
    return pl.pallas_call(
        total_kernel,
        out_shape=jax.ShapeDtypeStruct((nb, nq, dim), bf16),
        in_specs=[vm, hbm, hbm],
        out_specs=vm,
        scratch_shapes=[
            pltpu.VMEM((chunks, 2, 2, w_o.shape[0], lanes), bf16),
            pltpu.VMEM((nb // NZ, nq, chunks * lanes), bf16),
            pltpu.VMEM((chunks, 2, 2, n, lanes), f32),
            pltpu.VMEM((chunks, 2, 2, n, lanes), bf16),
            pltpu.VMEM((chunks, 2, n, lanes), f32),
            pltpu.VMEM((chunks, n, lanes), f32),
            pltpu.VMEM((chunks, 3, n // NZ, lanes), f32),
            dma((chunks, 4)), dma, one, one, one, one, three, three, three, three, one, one, one, one,
        ],
        compiler_params=pltpu.CompilerParams(
            collective_id=1, has_side_effects=True, vmem_limit_bytes=40 * 1024 * 1024),
        name="total_all",
    )(ov, w_o, hidden)


def solution(mesh):
    def local_step(hidden, cache_lens, c_kv, k_r, w_uq, w_qr, w_uk, w_uv, w_o):
        score_scale = (w_uq.shape[2] + w_qr.shape[2]) ** -0.5
        nb, nq, dim = hidden.shape
        nh, lat = w_uk.shape[0], w_uk.shape[2]
        q_nope = jnp.einsum("cre,eil->cril", hidden, w_uq, preferred_element_type=f32).astype(bf16)
        q_rope = jnp.einsum("cre,eis->cris", hidden, w_qr, preferred_element_type=f32).astype(bf16)
        q_lat = jnp.einsum("bqhk,hkc->bqhc", q_nope, w_uk, preferred_element_type=f32).astype(bf16)
        q_a = q_lat.reshape(nb, 2, 16, 4, 128).transpose(0, 1, 3, 2, 4).reshape(nb, 8, 16, 128)
        q_b = q_rope.reshape(nb, 2, 16, 64).transpose(0, 2, 1, 3).reshape(nb, 1, 16, 128)
        q = jnp.concatenate([q_a, q_b], axis=1)
        o_val = attend_all(q, cache_lens, c_kv, jnp.swapaxes(k_r, 1, 2), w_uv, score_scale)
        return total_all(o_val.reshape(nb * nq, -1), w_o.reshape(-1, dim), hidden)

    specs_in = (P("batch", None, None), P("batch"), P("batch", "seq", None), P("batch", "seq", None),
                P(None, "seq", None), P(None, "seq", None), P("seq", None, None), P("seq", None, None),
                P("seq", None, None))
    return jax.shard_map(local_step, mesh=mesh, in_specs=specs_in, out_specs=P("batch", None, None), check_vma=False)
```

```python
import functools
import math

import jax
import jax.numpy as jnp
from jax import lax
from jax.experimental import pallas as pl
from jax.experimental.pallas import tpu as pltpu
from jax.sharding import PartitionSpec as P

MASK_FILL = -1e30
NZ, NY, NC = 4, 2, 2
MESH = pl.DeviceIdType.MESH
f32, bf16 = jnp.float32, jnp.bfloat16


def place():
    s = lax.axis_index("seq")
    return s, s // (NY * NC), (s // NC) % NY, s % NC


def seq_of(z, y, c):
    return (z * NY + y) * NC + c


def remote(src, dst, send_sem, recv_sem, seq):
    return pltpu.make_async_remote_copy(
        src_ref=src, dst_ref=dst, send_sem=send_sem, recv_sem=recv_sem,
        device_id={"seq": seq}, device_id_type=MESH)


def meet(peers):
    barrier = pltpu.get_barrier_semaphore()
    for p in peers:
        pl.semaphore_signal(barrier, inc=1, device_id={"seq": p}, device_id_type=MESH)
    pl.semaphore_wait(barrier, len(peers))


def columns(rows):
    pad = jnp.zeros((128 - rows.shape[0], 128), f32)
    return jnp.concatenate([rows, pad], axis=0).T


def attend_kernel(scale, lens, q_hbm, r_hbm, c_hbm, k_hbm, h_hbm, wuv, out, h_out,
                  qbuf, ck, kr, o_full, ml0, ml1, ml2, rc_c, ml_c, rc_y, ml_y,
                  rc_u, ml_u, ml_us, rc_d, ml_d, ml_ds, wcol,
                  q_sem, h_sem, c_sem, k_sem,
                  ay_s, ay_r, au_s, au_r, ad_s, ad_r, ac_s, ac_r,
                  oc_s, oc_r, oy_s, oy_r, ou_s, ou_r, od_s, od_r,
                  mc_s, mc_r, my_s, my_r, mu_s, mu_r, md_s, md_r):
    nb, slots = q_hbm.shape[0], ck.shape[0]
    local_len = ck.shape[1]
    s, z, y, c = place()
    core_peer, y_peer = seq_of(z, y, 1 - c), seq_of(z, 1 - y, c)
    upper, lower = seq_of(lax.rem(z + 1, NZ), y, c), seq_of(lax.rem(z + NZ - 1, NZ), y, c)

    own_q = (pltpu.make_async_copy(q_hbm, qbuf.at[:, c, y, z, pl.ds(0, 8)], q_sem.at[0]),
             pltpu.make_async_copy(r_hbm, qbuf.at[:, c, y, z, 8], q_sem.at[1]))
    for cp in own_q:
        cp.start()

    def cache(b):
        k = lax.rem(b, slots)
        return (pltpu.make_async_copy(c_hbm.at[b], ck.at[k], c_sem.at[k]),
                pltpu.make_async_copy(k_hbm.at[b], kr.at[k], k_sem.at[k]))

    for b in range(slots - 1):
        for cp in cache(b):
            cp.start()

    deep, wide = h_out.shape[0], h_out.shape[2]
    own_h = pltpu.make_async_copy(
        h_hbm.at[pl.ds(z * deep, deep), :, pl.ds(pl.multiple_of((c * NY + y) * wide, 128), wide)], h_out, h_sem)
    own_h.start()
    meet([core_peer, y_peer, upper, lower])
    for cp in own_q:
        cp.wait()

    def gather_y(b, yy):
        part = qbuf.at[b, c, yy, z]
        return remote(part, part, ay_s.at[b], ay_r.at[b], y_peer)

    def gather_up(b, origin, d):
        part = qbuf.at[b, c, :, origin]
        return remote(part, part, au_s.at[b, d - 1], au_r.at[b, d - 1], upper)

    def gather_down(b, origin, d):
        part = qbuf.at[b, c, :, origin]
        return remote(part, part, ad_s.at[b, d - 1], ad_r.at[b, d - 1], lower)

    def gather_c(b, cc):
        part = qbuf.at[b, cc]
        return remote(part, part, ac_s.at[b], ac_r.at[b], core_peer)

    def sum_c(b, hf):
        rows = pl.ds(hf * 16, 16)
        return remote(o_full.at[b, 1 - c, :, :, rows], rc_c.at[b, :, :, rows], oc_s.at[b, hf], oc_r.at[b, hf], core_peer)

    def stat_c(b):
        return remote(ml0.at[b, 1 - c], ml_c.at[b], mc_s.at[b], mc_r.at[b], core_peer)

    def sum_y(b):
        return (remote(o_full.at[b, c, 1 - y], rc_y.at[b], oy_s.at[b], oy_r.at[b], y_peer),
                remote(ml1.at[b], ml_y.at[b], my_s.at[b], my_r.at[b], y_peer))

    def sum_up(b, dest, d):
        return remote(o_full.at[b, c, y, dest], rc_u.at[b, dest], ou_s.at[b, d - 1], ou_r.at[b, d - 1], upper)

    def stat_up(b, stat):
        return remote(stat.at[b], ml_u.at[b], mu_s.at[b], mu_r.at[b], upper)

    def sum_down(b, dest, d):
        return remote(o_full.at[b, c, y, dest], rc_d.at[b, dest], od_s.at[b, d - 1], od_r.at[b, d - 1], lower)

    def stat_down(b, stat):
        return remote(stat.at[b], ml_d.at[b], md_s.at[b], md_r.at[b], lower)

    def pass_on(b, d):
        @pl.when((z < NZ - 1) & (z - (d - 1) >= 0))
        def _():
            gather_up(b, z - (d - 1), d).start()

        @pl.when((z > 0) & (z + (d - 1) < NZ))
        def _():
            gather_down(b, z + (d - 1), d).start()

    def arrive(b, d):
        @pl.when(z - d >= 0)
        def _():
            gather_up(b, z - d, d).wait_recv()

        @pl.when(z + d < NZ)
        def _():
            gather_down(b, z + d, d).wait_recv()

    def step_z1(b):
        gather_y(b, 1 - y).wait_recv()
        pass_on(b, 1)

    def step_z2(b):
        arrive(b, 1)
        pass_on(b, 2)

    def step_z3(b):
        arrive(b, 2)
        pass_on(b, 3)

    def step_z4(b):
        arrive(b, 3)
        gather_c(b, c).start()

    def attend(b):
        gather_c(b, 1 - c).wait_recv()
        for cp in cache(b):
            cp.wait()

        @pl.when(b + slots - 1 < nb)
        def _():
            for cp in cache(b + slots - 1):
                cp.start()

        k = lax.rem(b, slots)
        row_len = lens[b]
        pos = s * local_len + lax.broadcasted_iota(jnp.int32, (256, local_len), 1)
        token = lax.rem(lax.broadcasted_iota(jnp.int32, (256, 1), 0), 16) // 8
        lane = lax.broadcasted_iota(jnp.int32, (256, 128), 1)
        for hf in range(2):
            q = jnp.concatenate([qbuf[b, :, :, :, hf * 4 + j].reshape(256, 128) for j in range(4)], axis=1)
            qr = qbuf[b, :, :, :, 8].reshape(256, 128)[:, hf * 64:(hf + 1) * 64]
            sc = lax.dot_general(q, ck[k], (((1,), (1,)), ((), ())), preferred_element_type=f32)
            sc = sc + jnp.dot(qr, kr[k], preferred_element_type=f32)
            sc = jnp.where(pos <= row_len + hf * 2 + token, sc, MASK_FILL)
            m = jnp.max(sc, axis=1, keepdims=True)
            p = jnp.exp2((sc - m) * scale)
            l = jnp.sum(p, axis=1, keepdims=True)
            o = jnp.dot(p.astype(bf16), ck[k], preferred_element_type=f32)
            o_full[b, :, :, :, hf * 16:(hf + 1) * 16, :] = o.reshape(2, 2, 4, 16, o.shape[1])
            stat = jnp.where(lane == 0, m * scale, jnp.where(lane == 1, l, 0.0)).T
            for cc in range(2):
                ml0[b, cc, hf * 2:hf * 2 + 2, :] = stat[0:2, cc * 128:(cc + 1) * 128]
            sum_c(b, hf).start()
        stat_c(b).start()

    def merge_stats(parts, final):
        stats, factors = [], []
        for hf in range(2):
            ms, ls = [p[2 * hf:2 * hf + 1] for p in parts], [p[2 * hf + 1:2 * hf + 2] for p in parts]
            top = functools.reduce(jnp.maximum, ms)
            ws = [jnp.exp2(m - top) for m in ms]
            total = sum(w * l for w, l in zip(ws, ls))
            stats += [top, total]
            factors += [w / total for w in ws] if final else ws
        return jnp.concatenate(stats, axis=0), columns(jnp.concatenate(factors, axis=0))

    def step_d(b):
        for hf in range(2):
            sum_c(b, hf).wait_recv()
        stat_c(b).wait_recv()
        stats, cols = merge_stats([ml0[b, c, 0:4], ml_c[b, 0:4]], False)
        ml1[b, 0:4, :] = stats
        for hf in range(2):
            rows = pl.ds(hf * 16, 16)
            wa, wb = (cols[:, 2 * hf + j:2 * hf + j + 1].reshape(2, 4, 16, 1) for j in range(2))
            o_full[b, c, :, :, rows, :] = o_full[b, c, :, :, rows, :] * wa + rc_c[b, :, :, rows, :] * wb
        for cp in sum_y(b):
            cp.start()

    def step_e(b):
        for cp in sum_y(b):
            cp.wait_recv()
        stats, cols = merge_stats([ml1[b, 0:4], ml_y[b, 0:4]], False)
        ml2[b, 0:4, :] = stats
        wcol[...] = cols
        cols = wcol[pl.ds(pl.multiple_of(y * 64, 64), 64), :]
        for hf in range(2):
            rows = pl.ds(hf * 16, 16)
            wa, wb = (cols[:, 2 * hf + j:2 * hf + j + 1].reshape(4, 16, 1) for j in range(2))
            o_full[b, c, y, :, rows, :] = o_full[b, c, y, :, rows, :] * wa + rc_y[b, :, rows, :] * wb

        @pl.when(z == 0)
        def _():
            stat_up(b, ml2).start()
            for dest in range(NZ - 1, 0, -1):
                sum_up(b, dest, dest).start()

        @pl.when(z == NZ - 1)
        def _():
            stat_down(b, ml2).start()
            for dest in range(NZ - 1):
                sum_down(b, dest, NZ - 1 - dest).start()

    def relay(b, dests, stats_in, stats_out, arrived, wait, send):
        stats, cols = merge_stats([ml2[b, 0:4], stats_in[b, 0:4]], False)
        stats_out[b, 0:4, :] = stats
        wcol[...] = cols
        for i, dest in enumerate(dests):
            wait(dest)
            cols = wcol[pl.ds(pl.multiple_of(y * 64 + dest * 16, 16), 16), :]
            for hf in range(2):
                rows = pl.ds(hf * 16, 16)
                wa, wb = (cols[:, 2 * hf + j:2 * hf + j + 1] for j in range(2))
                o_full[b, c, y, dest, rows, :] = o_full[b, c, y, dest, rows, :] * wa + arrived[b, dest, rows, :] * wb
            if i == 0:
                send(None)
            send(dest)

    def step_g(hop, b):
        at = NZ - 1 - hop

        @pl.when(z == hop)
        def _():
            def send(dest):
                (stat_up(b, ml_us) if dest is None else sum_up(b, dest, dest - hop)).start()
            stat_up(b, ml2).wait_recv()
            relay(b, range(NZ - 1, hop, -1), ml_u, ml_us, rc_u, lambda dest: sum_up(b, dest, dest - hop + 1).wait_recv(), send)

        @pl.when(z == at)
        def _():
            def send(dest):
                (stat_down(b, ml_ds) if dest is None else sum_down(b, dest, at - dest)).start()
            stat_down(b, ml2).wait_recv()
            relay(b, range(at), ml_d, ml_ds, rc_d, lambda dest: sum_down(b, dest, at - dest + 1).wait_recv(), send)

    def finish(b, at):
        parts, sums = [ml2[b, 0:4]], [o_full.at[b, c, y, at]]
        if at > 0:
            sum_up(b, at, 1).wait_recv()
            if at == NZ - 1:
                stat_up(b, ml2).wait_recv()
            parts.append(ml_u[b, 0:4])
            sums.append(rc_u.at[b, at])
        if at < NZ - 1:
            sum_down(b, at, 1).wait_recv()
            if at == 0:
                stat_down(b, ml2).wait_recv()
            parts.append(ml_d[b, 0:4])
            sums.append(rc_d.at[b, at])
        wcol[...] = merge_stats(parts, True)[1]
        cols = wcol[pl.ds(pl.multiple_of(y * 64 + at * 16, 16), 16), :]
        n = len(parts)
        halves = []
        for hf in range(2):
            rows = pl.ds(hf * 16, 16)
            o = sum(part[rows, :] * cols[:, n * hf + j:n * hf + j + 1] for j, part in enumerate(sums))
            halves.append(o.astype(bf16))
        o = jnp.concatenate(halves, axis=0)
        head = lax.rem(lax.broadcasted_iota(jnp.int32, (32, 128), 0), 8)
        for h in range(8):
            v = jnp.dot(o, wuv[h], preferred_element_type=f32)
            v = jnp.where(head == h, v, 0.0).reshape(4, 8, 128).sum(axis=1)
            out[b, :, h * 128:(h + 1) * 128] = v.astype(bf16)

    def step_f(b):
        for at in range(NZ):
            @pl.when(z == at)
            def _(at=at):
                finish(b, at)

    @pl.loop(0, nb)
    def _(b):
        gather_y(b, y).start()

    steps = ((7, step_e), (8, functools.partial(step_g, 1)), (9, functools.partial(step_g, 2)), (10, step_f),
             (0, step_z1), (1, step_z2), (2, step_z3), (3, step_z4), (5, step_d), (4, attend))

    @pl.loop(0, nb + 10)
    def _(it):
        for lag, fn in steps:
            b = it - lag

            @pl.when((b >= 0) & (b < nb))
            def _(fn=fn, b=b):
                fn(b)

    own_h.wait()

    @pl.loop(0, nb)
    def _(b):
        gather_y(b, y).wait_send()
        gather_c(b, c).wait_send()
        for d in (1, 2, 3):
            @pl.when((z < NZ - 1) & (z - (d - 1) >= 0))
            def _(d=d):
                gather_up(b, z - (d - 1), d).wait_send()

            @pl.when((z > 0) & (z + (d - 1) < NZ))
            def _(d=d):
                gather_down(b, z + (d - 1), d).wait_send()
        sum_c(b, 0).wait_send()
        sum_c(b, 1).wait_send()
        stat_c(b).wait_send()
        for cp in sum_y(b):
            cp.wait_send()
        for at in range(NZ):
            @pl.when(z == at)
            def _(at=at):
                for dest in range(at + 1, NZ):
                    sum_up(b, dest, dest - at).wait_send()
                if at < NZ - 1:
                    stat_up(b, ml2).wait_send()
                for dest in range(at):
                    sum_down(b, dest, at - dest).wait_send()
                if at > 0:
                    stat_down(b, ml2).wait_send()


def attend_all(q, q_rope, lens, c_kv, k_t, hidden, w_uv, score_scale):
    nb, local_len, lat = c_kv.shape
    nq, dim = hidden.shape[1:]
    slots = 3
    dma = pltpu.SemaphoreType.DMA
    return pl.pallas_call(
        functools.partial(attend_kernel, score_scale * math.log2(math.e)),
        out_shape=(jax.ShapeDtypeStruct((nb, nq, w_uv.shape[0] * w_uv.shape[2]), bf16),
                   jax.ShapeDtypeStruct((nb // NZ, nq, dim // 4), bf16)),
        in_specs=[pl.BlockSpec(memory_space=pltpu.SMEM)] + [pl.BlockSpec(memory_space=pl.ANY)] * 5
        + [pl.BlockSpec(memory_space=pltpu.VMEM)],
        out_specs=(pl.BlockSpec(memory_space=pltpu.VMEM), pl.BlockSpec(memory_space=pltpu.VMEM)),
        scratch_shapes=[
            pltpu.VMEM((nb, 2, 2, 4, 9, 16, 128), bf16),
            pltpu.VMEM((slots, local_len, lat), bf16),
            pltpu.VMEM((slots, k_t.shape[1], local_len), bf16),
            pltpu.VMEM((nb, 2, 2, 4, 32, lat), f32),
            pltpu.VMEM((nb, 2, 8, 128), f32),
            pltpu.VMEM((nb, 8, 128), f32),
            pltpu.VMEM((nb, 8, 128), f32),
            pltpu.VMEM((nb, 2, 4, 32, lat), f32),
            pltpu.VMEM((nb, 8, 128), f32),
            pltpu.VMEM((nb, 4, 32, lat), f32),
            pltpu.VMEM((nb, 8, 128), f32),
            pltpu.VMEM((nb, 4, 32, lat), f32),
            pltpu.VMEM((nb, 8, 128), f32),
            pltpu.VMEM((nb, 8, 128), f32),
            pltpu.VMEM((nb, 4, 32, lat), f32),
            pltpu.VMEM((nb, 8, 128), f32),
            pltpu.VMEM((nb, 8, 128), f32),
            pltpu.VMEM((128, 128), f32),
            dma((2,)), dma, dma((slots,)), dma((slots,)),
            dma((nb,)), dma((nb,)), dma((nb, 3)), dma((nb, 3)), dma((nb, 3)), dma((nb, 3)), dma((nb,)), dma((nb,)),
            dma((nb, 2)), dma((nb, 2)), dma((nb,)), dma((nb,)), dma((nb, 3)), dma((nb, 3)), dma((nb, 3)), dma((nb, 3)),
            dma((nb,)), dma((nb,)), dma((nb,)), dma((nb,)), dma((nb,)), dma((nb,)), dma((nb,)), dma((nb,)),
        ],
        compiler_params=pltpu.CompilerParams(
            collective_id=0, has_side_effects=True, vmem_limit_bytes=64 * 1024 * 1024 - 65536),
        name="attend_all",
    )(lens, q, q_rope, c_kv, k_t, hidden, w_uv)


def rope_kernel(h_ref, w_ref, out, acc, rows):
    step = pl.program_id(0)
    nb, nq, lanes = h_ref.shape
    h = h_ref[...].astype(f32).reshape(nb * nq, lanes).astype(bf16)
    part = lax.dot_general(h, w_ref[...], (((1,), (1,)), ((), ())), preferred_element_type=f32)

    @pl.when(step == 0)
    def _():
        acc[...] = part

    @pl.when(step > 0)
    def _():
        acc[...] += part

    @pl.when(step == pl.num_programs(0) - 1)
    def _():
        for h in range(8):
            rows[:, h, :] = acc[:, h * 64:(h + 1) * 64]
        pairs = rows[...].reshape(nb, 2, 16, 64)
        out[...] = jnp.concatenate([pairs[:, 0], pairs[:, 1]], axis=-1).astype(bf16)


def rope_queries(hidden, w_t):
    nb, nq, dim = hidden.shape
    wide = w_t.shape[0]
    steps = next(k for k in (7, 4, 1) if dim % (k * 128) == 0)
    return pl.pallas_call(
        rope_kernel,
        grid=(steps,),
        out_shape=jax.ShapeDtypeStruct((nb, 16, 128), bf16),
        in_specs=[pl.BlockSpec((nb, nq, dim // steps), lambda i: (0, 0, i)), pl.BlockSpec((wide, dim // steps), lambda i: (0, i))],
        out_specs=pl.BlockSpec((nb, 16, 128), lambda i: (0, 0, 0)),
        scratch_shapes=[pltpu.VMEM((nb * nq, wide), f32), pltpu.VMEM((nb * nq, 8, 64), f32)],
        compiler_params=pltpu.CompilerParams(dimension_semantics=("arbitrary",)),
        name="rope_queries",
    )(hidden, w_t)


def total_kernel(ov_ref, w_hbm, hbuf, out, ov_rows, wbuf, part, gat, rc_c, rc_y, rc_z,
                 w_sem, sc_s, sc_r, sy_s, sy_r, sz_s, sz_r, gz_s, gz_r, gy_s, gy_r, gc_s, gc_r):
    _, z, y, c = place()
    chunks, lanes = wbuf.shape[0], wbuf.shape[4]
    deep = part.shape[3] // NZ
    core_peer, y_peer = seq_of(z, y, 1 - c), seq_of(z, 1 - y, c)
    zs = [lax.rem(z + d, NZ) for d in (1, 2, 3)]
    zf = [lax.rem(z + NZ - d, NZ) for d in (1, 2, 3)]

    def where(cc, yy, k):
        return pl.ds(pl.multiple_of((cc * NY + yy) * (chunks * lanes) + k * lanes, 128), lanes)

    def weights(k):
        return [pltpu.make_async_copy(w_hbm.at[:, where(cc, yy, k)], wbuf.at[k, cc, yy], w_sem.at[k, cc * 2 + yy])
                for cc in range(2) for yy in range(2)]

    for k in range(chunks):
        for cp in weights(k):
            cp.start()
    nb = ov_ref.shape[0]
    ov_rows[...] = ov_ref[...].astype(f32).reshape(ov_rows.shape).astype(bf16)
    meet([core_peer, y_peer] + [seq_of(p, y, c) for p in zs])

    def band(at):
        return pl.ds(pl.multiple_of(at * deep, deep), deep)

    def sum_c(k):
        return remote(part.at[k, 1 - c], rc_c.at[k], sc_s.at[k], sc_r.at[k], core_peer)

    def sum_y(k):
        return remote(part.at[k, c, 1 - y], rc_y.at[k], sy_s.at[k], sy_r.at[k], y_peer)

    def sum_z(k, d):
        return remote(part.at[k, c, y, band(zs[d])], rc_z.at[k, d], sz_s.at[k, d], sz_r.at[k, d], seq_of(zs[d], y, c))

    def give_z(k, d, at):
        piece = gat.at[k, c, y, band(at)]
        return remote(piece, piece, gz_s.at[k, d], gz_r.at[k, d], seq_of(zs[d], y, c))

    def give_y(k, yy):
        return remote(gat.at[k, c, yy], gat.at[k, c, yy], gy_s.at[k], gy_r.at[k], y_peer)

    def give_c(k, cc):
        return remote(gat.at[k, cc], gat.at[k, cc], gc_s.at[k], gc_r.at[k], core_peer)

    def multiply(k):
        for cp in weights(k):
            cp.wait()
        ov = ov_rows[...]
        for cc in (1 - c, c):
            for yy in range(2):
                part[k, cc, yy] = jnp.dot(ov, wbuf[k, cc, yy], preferred_element_type=f32)
            if cc is not c:
                sum_c(k).start()

    def step_d(k):
        sum_c(k).wait_recv()
        part[k, c] = part[k, c] + rc_c[k]
        sum_y(k).start()

    def step_e(k):
        sum_y(k).wait_recv()
        part[k, c, y] = part[k, c, y] + rc_y[k]
        for d in range(3):
            sum_z(k, d).start()

    def step_f(k):
        for d in range(3):
            sum_z(k, d).wait_recv()
        total = part[k, c, y, band(z)] + rc_z[k, 0] + rc_z[k, 1] + rc_z[k, 2]
        own = hbuf[:, :, pl.ds(pl.multiple_of(k * lanes, 128), lanes)].astype(f32).reshape(deep, lanes)
        gat[k, c, y, band(z)] = (own + total).astype(bf16)
        for d in range(3):
            give_z(k, d, z).start()

    def step_h(k):
        for d in range(3):
            give_z(k, d, zf[d]).wait_recv()
        give_y(k, y).start()

    def step_i(k):
        give_y(k, 1 - y).wait_recv()
        give_c(k, c).start()

    def step_j(k):
        give_c(k, 1 - c).wait_recv()
        for cc in range(2):
            for yy in range(2):
                out[:, :, where(cc, yy, k)] = gat[k, cc, yy].astype(f32).reshape(nb, -1, lanes).astype(bf16)

    steps = ((10, step_j), (9, step_i), (7, step_h), (5, step_f), (3, step_e), (1, step_d), (0, multiply))

    @pl.loop(0, chunks + 10)
    def _(it):
        for lag, fn in steps:
            k = it - lag

            @pl.when((k >= 0) & (k < chunks))
            def _(fn=fn, k=k):
                fn(k)

    @pl.loop(0, chunks)
    def _(k):
        sum_c(k).wait_send()
        sum_y(k).wait_send()
        for d in range(3):
            sum_z(k, d).wait_send()
            give_z(k, d, z).wait_send()
        give_y(k, y).wait_send()
        give_c(k, c).wait_send()


def total_all(ov, w_o, own_h):
    (nb, nq, _), dim = ov.shape, w_o.shape[1]
    n = nb * nq
    chunks = next(k for k in (7, 1) if dim % (4 * k * 128) == 0)
    lanes = dim // (4 * chunks)
    dma = pltpu.SemaphoreType.DMA
    vm, hbm = pl.BlockSpec(memory_space=pltpu.VMEM), pl.BlockSpec(memory_space=pl.ANY)
    one, three = dma((chunks,)), dma((chunks, 3))
    return pl.pallas_call(
        total_kernel,
        out_shape=jax.ShapeDtypeStruct((nb, nq, dim), bf16),
        in_specs=[vm, hbm, vm],
        out_specs=vm,
        scratch_shapes=[
            pltpu.VMEM((n, w_o.shape[0]), bf16),
            pltpu.VMEM((chunks, 2, 2, w_o.shape[0], lanes), bf16),
            pltpu.VMEM((chunks, 2, 2, n, lanes), f32),
            pltpu.VMEM((chunks, 2, 2, n, lanes), bf16),
            pltpu.VMEM((chunks, 2, n, lanes), f32),
            pltpu.VMEM((chunks, n, lanes), f32),
            pltpu.VMEM((chunks, 3, n // NZ, lanes), f32),
            dma((chunks, 4)), one, one, one, one, three, three, three, three, one, one, one, one,
        ],
        compiler_params=pltpu.CompilerParams(
            collective_id=1, has_side_effects=True, vmem_limit_bytes=40 * 1024 * 1024),
        name="total_all",
    )(ov, w_o, own_h)


def solution(mesh):
    def local_step(hidden, cache_lens, c_kv, k_r, w_uq, w_qr, w_uk, w_uv, w_o):
        score_scale = (w_uq.shape[2] + w_qr.shape[2]) ** -0.5
        nb, nq, dim = hidden.shape
        nh, lat = w_uk.shape[0], w_uk.shape[2]
        q_nope = jnp.einsum("cre,eil->cril", hidden, w_uq, preferred_element_type=f32).astype(bf16)
        q_lat = jnp.einsum("bqhk,hkc->bqhc", q_nope, w_uk, preferred_element_type=f32).astype(bf16)
        q = q_lat.reshape(nb, 2, 16, 4, 128).transpose(0, 1, 3, 2, 4).reshape(nb, 8, 16, 128)
        q_rope = rope_queries(hidden, w_qr.transpose(1, 2, 0).reshape(-1, dim))
        o_val, own_h = attend_all(q, q_rope, cache_lens, c_kv, jnp.swapaxes(k_r, 1, 2), hidden, w_uv, score_scale)
        return total_all(o_val, w_o.reshape(-1, dim), own_h)

    specs_in = (P("batch", None, None), P("batch"), P("batch", "seq", None), P("batch", "seq", None),
                P(None, "seq", None), P(None, "seq", None), P("seq", None, None), P("seq", None, None),
                P("seq", None, None))
    return jax.shard_map(local_step, mesh=mesh, in_specs=specs_in, out_specs=P("batch", None, None), check_vma=False)
```

```python
import functools
import math

import jax
import jax.numpy as jnp
from jax import lax
from jax.experimental import pallas as pl
from jax.experimental.pallas import tpu as pltpu
from jax.sharding import PartitionSpec as P

MASK_FILL = -1e30
NZ, NY, NC = 4, 2, 2
MESH = pl.DeviceIdType.MESH
f32, bf16 = jnp.float32, jnp.bfloat16


def place():
    s = lax.axis_index("seq")
    return s, s // (NY * NC), (s // NC) % NY, s % NC


def seq_of(z, y, c):
    return (z * NY + y) * NC + c


def remote(src, dst, send_sem, recv_sem, seq):
    return pltpu.make_async_remote_copy(
        src_ref=src, dst_ref=dst, send_sem=send_sem, recv_sem=recv_sem,
        device_id={"seq": seq}, device_id_type=MESH)


def meet(peers):
    barrier = pltpu.get_barrier_semaphore()
    for p in peers:
        pl.semaphore_signal(barrier, inc=1, device_id={"seq": p}, device_id_type=MESH)
    pl.semaphore_wait(barrier, len(peers))


def columns(rows):
    pad = jnp.zeros((128 - rows.shape[0], 128), f32)
    return jnp.concatenate([rows, pad], axis=0).T


def attend_kernel(scale, lens, q_hbm, r_hbm, c_hbm, k_hbm, h_hbm, wuv, out, h_out,
                  qbuf, ck, kr, o_full, ml0, ml1, ml2, rc_c, ml_c, rc_y, ml_y,
                  rc_u, ml_u, ml_us, rc_d, ml_d, ml_ds, wcol,
                  q_sem, h_sem, c_sem, k_sem,
                  ay_s, ay_r, au_s, au_r, ad_s, ad_r, ac_s, ac_r,
                  oc_s, oc_r, oy_s, oy_r, ou_s, ou_r, od_s, od_r,
                  mc_s, mc_r, my_s, my_r, mu_s, mu_r, md_s, md_r):
    nb, slots = q_hbm.shape[0], ck.shape[0]
    local_len = ck.shape[1]
    s, z, y, c = place()
    core_peer, y_peer = seq_of(z, y, 1 - c), seq_of(z, 1 - y, c)
    upper, lower = seq_of(lax.rem(z + 1, NZ), y, c), seq_of(lax.rem(z + NZ - 1, NZ), y, c)

    own_q = (pltpu.make_async_copy(q_hbm, qbuf.at[:, c, y, z, pl.ds(0, 8)], q_sem.at[0]),
             pltpu.make_async_copy(r_hbm, qbuf.at[:, c, y, z, 8], q_sem.at[1]))
    for cp in own_q:
        cp.start()

    def cache(b):
        k = lax.rem(b, slots)
        return (pltpu.make_async_copy(c_hbm.at[b], ck.at[k], c_sem.at[k]),
                pltpu.make_async_copy(k_hbm.at[b], kr.at[k], k_sem.at[k]))

    for b in range(slots - 1):
        for cp in cache(b):
            cp.start()

    deep, wide = h_out.shape[0], h_out.shape[2]
    own_h = pltpu.make_async_copy(
        h_hbm.at[pl.ds(z * deep, deep), :, pl.ds(pl.multiple_of((c * NY + y) * wide, 128), wide)], h_out, h_sem)
    own_h.start()
    meet([core_peer, y_peer] + [seq_of(lax.rem(z + d, NZ), y, c) for d in (1, 2, 3)])
    for cp in own_q:
        cp.wait()

    def gather_y(b, yy):
        part = qbuf.at[b, c, yy, z]
        return remote(part, part, ay_s.at[b], ay_r.at[b], y_peer)

    def gather_up(b, origin, d):
        part = qbuf.at[b, c, :, origin]
        return remote(part, part, au_s.at[b, d - 1], au_r.at[b, d - 1], upper)

    def gather_down(b, origin, d):
        part = qbuf.at[b, c, :, origin]
        return remote(part, part, ad_s.at[b, d - 1], ad_r.at[b, d - 1], lower)

    def gather_c(b, cc):
        part = qbuf.at[b, cc]
        return remote(part, part, ac_s.at[b], ac_r.at[b], core_peer)

    def sum_c(b, hf):
        rows = pl.ds(hf * 16, 16)
        return remote(o_full.at[b, 1 - c, :, :, rows], rc_c.at[b, :, :, rows], oc_s.at[b, hf], oc_r.at[b, hf], core_peer)

    def stat_c(b):
        return remote(ml0.at[b, 1 - c], ml_c.at[b], mc_s.at[b], mc_r.at[b], core_peer)

    def sum_y(b):
        return (remote(o_full.at[b, c, 1 - y], rc_y.at[b], oy_s.at[b], oy_r.at[b], y_peer),
                remote(ml1.at[b], ml_y.at[b], my_s.at[b], my_r.at[b], y_peer))

    def sum_up(b, dest, d):
        return remote(o_full.at[b, c, y, dest], rc_u.at[b, dest], ou_s.at[b, d - 1], ou_r.at[b, d - 1], upper)

    def stat_up(b, stat):
        return remote(stat.at[b], ml_u.at[b], mu_s.at[b], mu_r.at[b], upper)

    def sum_down(b, dest, d):
        return remote(o_full.at[b, c, y, dest], rc_d.at[b, dest], od_s.at[b, d - 1], od_r.at[b, d - 1], lower)

    def stat_down(b, stat):
        return remote(stat.at[b], ml_d.at[b], md_s.at[b], md_r.at[b], lower)

    def pass_on(b, d):
        @pl.when((z < NZ - 1) & (z - (d - 1) >= 0))
        def _():
            gather_up(b, z - (d - 1), d).start()

        @pl.when((z > 0) & (z + (d - 1) < NZ))
        def _():
            gather_down(b, z + (d - 1), d).start()

    def arrive(b, d):
        @pl.when(z - d >= 0)
        def _():
            gather_up(b, z - d, d).wait_recv()

        @pl.when(z + d < NZ)
        def _():
            gather_down(b, z + d, d).wait_recv()

    direct = 1

    def straight(b, d, go):
        part = qbuf.at[b, c, :, z]

        @pl.when(z + d < NZ)
        def _():
            go(remote(part, part, au_s.at[b, d - 1], au_r.at[b, d - 1], seq_of(lax.rem(z + d, NZ), y, c)))

        @pl.when(z - d >= 0)
        def _():
            go(remote(part, part, ad_s.at[b, d - 1], ad_r.at[b, d - 1], seq_of(lax.rem(z + NZ - d, NZ), y, c)))

    def step_z1(b):
        gather_y(b, 1 - y).wait_recv()

        @pl.when(b < direct)
        def _():
            for d in (3, 2, 1):
                straight(b, d, lambda cp: cp.start())

        @pl.when(b >= direct)
        def _():
            pass_on(b, 1)

    def step_z2(b):
        arrive(b, 1)

        @pl.when(b >= direct)
        def _():
            pass_on(b, 2)

    def step_z3(b):
        arrive(b, 2)

        @pl.when(b >= direct)
        def _():
            pass_on(b, 3)

    def step_z4(b):
        arrive(b, 3)
        gather_c(b, c).start()

    def attend(b):
        gather_c(b, 1 - c).wait_recv()
        for cp in cache(b):
            cp.wait()

        @pl.when(b + slots - 1 < nb)
        def _():
            for cp in cache(b + slots - 1):
                cp.start()

        k = lax.rem(b, slots)
        row_len = lens[b]
        pos = s * local_len + lax.broadcasted_iota(jnp.int32, (256, local_len), 1)
        token = lax.rem(lax.broadcasted_iota(jnp.int32, (256, 1), 0), 16) // 8
        lane = lax.broadcasted_iota(jnp.int32, (256, 128), 1)
        for hf in range(2):
            q = jnp.concatenate([qbuf[b, :, :, :, hf * 4 + j].reshape(256, 128) for j in range(4)], axis=1)
            qr = qbuf[b, :, :, :, 8].reshape(256, 128)[:, hf * 64:(hf + 1) * 64]
            sc = lax.dot_general(q, ck[k], (((1,), (1,)), ((), ())), preferred_element_type=f32)
            sc = sc + jnp.dot(qr, kr[k], preferred_element_type=f32)
            sc = jnp.where(pos <= row_len + hf * 2 + token, sc, MASK_FILL)
            m = jnp.max(sc, axis=1, keepdims=True)
            p = jnp.exp2((sc - m) * scale)
            l = jnp.sum(p, axis=1, keepdims=True)
            o = jnp.dot(p.astype(bf16), ck[k], preferred_element_type=f32)
            o_full[b, :, :, :, hf * 16:(hf + 1) * 16, :] = o.reshape(2, 2, 4, 16, o.shape[1])
            stat = jnp.where(lane == 0, m * scale, jnp.where(lane == 1, l, 0.0)).T
            for cc in range(2):
                ml0[b, cc, hf * 2:hf * 2 + 2, :] = stat[0:2, cc * 128:(cc + 1) * 128]
            sum_c(b, hf).start()
        stat_c(b).start()

    def merge_stats(parts, final):
        stats, factors = [], []
        for hf in range(2):
            ms, ls = [p[2 * hf:2 * hf + 1] for p in parts], [p[2 * hf + 1:2 * hf + 2] for p in parts]
            top = functools.reduce(jnp.maximum, ms)
            ws = [jnp.exp2(m - top) for m in ms]
            total = sum(w * l for w, l in zip(ws, ls))
            stats += [top, total]
            factors += [w / total for w in ws] if final else ws
        return jnp.concatenate(stats, axis=0), columns(jnp.concatenate(factors, axis=0))

    def step_d(b):
        for hf in range(2):
            sum_c(b, hf).wait_recv()
        stat_c(b).wait_recv()
        stats, cols = merge_stats([ml0[b, c, 0:4], ml_c[b, 0:4]], False)
        ml1[b, 0:4, :] = stats
        for hf in range(2):
            rows = pl.ds(hf * 16, 16)
            wa, wb = (cols[:, 2 * hf + j:2 * hf + j + 1].reshape(2, 4, 16, 1) for j in range(2))
            o_full[b, c, :, :, rows, :] = o_full[b, c, :, :, rows, :] * wa + rc_c[b, :, :, rows, :] * wb
        for cp in sum_y(b):
            cp.start()

    def step_e(b):
        for cp in sum_y(b):
            cp.wait_recv()
        stats, cols = merge_stats([ml1[b, 0:4], ml_y[b, 0:4]], False)
        ml2[b, 0:4, :] = stats
        wcol[...] = cols
        cols = wcol[pl.ds(pl.multiple_of(y * 64, 64), 64), :]
        for hf in range(2):
            rows = pl.ds(hf * 16, 16)
            wa, wb = (cols[:, 2 * hf + j:2 * hf + j + 1].reshape(4, 16, 1) for j in range(2))
            o_full[b, c, y, :, rows, :] = o_full[b, c, y, :, rows, :] * wa + rc_y[b, :, rows, :] * wb

        @pl.when(z == 0)
        def _():
            stat_up(b, ml2).start()
            for dest in range(NZ - 1, 0, -1):
                sum_up(b, dest, dest).start()

        @pl.when(z == NZ - 1)
        def _():
            stat_down(b, ml2).start()
            for dest in range(NZ - 1):
                sum_down(b, dest, NZ - 1 - dest).start()

    def relay(b, dests, stats_in, stats_out, arrived, wait, send):
        stats, cols = merge_stats([ml2[b, 0:4], stats_in[b, 0:4]], False)
        stats_out[b, 0:4, :] = stats
        wcol[...] = cols
        for i, dest in enumerate(dests):
            wait(dest)
            cols = wcol[pl.ds(pl.multiple_of(y * 64 + dest * 16, 16), 16), :]
            for hf in range(2):
                rows = pl.ds(hf * 16, 16)
                wa, wb = (cols[:, 2 * hf + j:2 * hf + j + 1] for j in range(2))
                o_full[b, c, y, dest, rows, :] = o_full[b, c, y, dest, rows, :] * wa + arrived[b, dest, rows, :] * wb
            if i == 0:
                send(None)
            send(dest)

    def step_g(hop, b):
        at = NZ - 1 - hop

        @pl.when(z == hop)
        def _():
            def send(dest):
                (stat_up(b, ml_us) if dest is None else sum_up(b, dest, dest - hop)).start()
            stat_up(b, ml2).wait_recv()
            relay(b, range(NZ - 1, hop, -1), ml_u, ml_us, rc_u, lambda dest: sum_up(b, dest, dest - hop + 1).wait_recv(), send)

        @pl.when(z == at)
        def _():
            def send(dest):
                (stat_down(b, ml_ds) if dest is None else sum_down(b, dest, at - dest)).start()
            stat_down(b, ml2).wait_recv()
            relay(b, range(at), ml_d, ml_ds, rc_d, lambda dest: sum_down(b, dest, at - dest + 1).wait_recv(), send)

    def finish(b, at):
        parts, sums = [ml2[b, 0:4]], [o_full.at[b, c, y, at]]
        if at > 0:
            sum_up(b, at, 1).wait_recv()
            if at == NZ - 1:
                stat_up(b, ml2).wait_recv()
            parts.append(ml_u[b, 0:4])
            sums.append(rc_u.at[b, at])
        if at < NZ - 1:
            sum_down(b, at, 1).wait_recv()
            if at == 0:
                stat_down(b, ml2).wait_recv()
            parts.append(ml_d[b, 0:4])
            sums.append(rc_d.at[b, at])
        wcol[...] = merge_stats(parts, True)[1]
        cols = wcol[pl.ds(pl.multiple_of(y * 64 + at * 16, 16), 16), :]
        n = len(parts)
        halves = []
        for hf in range(2):
            rows = pl.ds(hf * 16, 16)
            o = sum(part[rows, :] * cols[:, n * hf + j:n * hf + j + 1] for j, part in enumerate(sums))
            halves.append(o.astype(bf16))
        o = jnp.concatenate(halves, axis=0)
        head = lax.rem(lax.broadcasted_iota(jnp.int32, (32, 128), 0), 8)
        for h in range(8):
            v = jnp.dot(o, wuv[h], preferred_element_type=f32)
            v = jnp.where(head == h, v, 0.0).reshape(4, 8, 128).sum(axis=1)
            out[b, :, h * 128:(h + 1) * 128] = v.astype(bf16)

    def step_f(b):
        for at in range(NZ):
            @pl.when(z == at)
            def _(at=at):
                finish(b, at)

    @pl.loop(0, nb)
    def _(b):
        gather_y(b, y).start()

    steps = ((7, step_e), (8, functools.partial(step_g, 1)), (9, functools.partial(step_g, 2)), (10, step_f),
             (0, step_z1), (1, step_z2), (2, step_z3), (3, step_z4), (5, step_d), (4, attend))

    @pl.loop(0, nb + 10)
    def _(it):
        for lag, fn in steps:
            b = it - lag

            @pl.when((b >= 0) & (b < nb))
            def _(fn=fn, b=b):
                fn(b)

    own_h.wait()

    @pl.loop(0, nb)
    def _(b):
        gather_y(b, y).wait_send()
        gather_c(b, c).wait_send()
        @pl.when(b < direct)
        def _():
            for d in (1, 2, 3):
                straight(b, d, lambda cp: cp.wait_send())

        @pl.when(b >= direct)
        def _():
            for d in (1, 2, 3):
                @pl.when((z < NZ - 1) & (z - (d - 1) >= 0))
                def _(d=d):
                    gather_up(b, z - (d - 1), d).wait_send()

                @pl.when((z > 0) & (z + (d - 1) < NZ))
                def _(d=d):
                    gather_down(b, z + (d - 1), d).wait_send()
        sum_c(b, 0).wait_send()
        sum_c(b, 1).wait_send()
        stat_c(b).wait_send()
        for cp in sum_y(b):
            cp.wait_send()
        for at in range(NZ):
            @pl.when(z == at)
            def _(at=at):
                for dest in range(at + 1, NZ):
                    sum_up(b, dest, dest - at).wait_send()
                if at < NZ - 1:
                    stat_up(b, ml2).wait_send()
                for dest in range(at):
                    sum_down(b, dest, at - dest).wait_send()
                if at > 0:
                    stat_down(b, ml2).wait_send()


def attend_all(q, q_rope, lens, c_kv, k_t, hidden, w_uv, score_scale):
    nb, local_len, lat = c_kv.shape
    nq, dim = hidden.shape[1:]
    slots = 3
    dma = pltpu.SemaphoreType.DMA
    return pl.pallas_call(
        functools.partial(attend_kernel, score_scale * math.log2(math.e)),
        out_shape=(jax.ShapeDtypeStruct((nb, nq, w_uv.shape[0] * w_uv.shape[2]), bf16),
                   jax.ShapeDtypeStruct((nb // NZ, nq, dim // 4), bf16)),
        in_specs=[pl.BlockSpec(memory_space=pltpu.SMEM)] + [pl.BlockSpec(memory_space=pl.ANY)] * 5
        + [pl.BlockSpec(memory_space=pltpu.VMEM)],
        out_specs=(pl.BlockSpec(memory_space=pltpu.VMEM), pl.BlockSpec(memory_space=pltpu.VMEM)),
        scratch_shapes=[
            pltpu.VMEM((nb, 2, 2, 4, 9, 16, 128), bf16),
            pltpu.VMEM((slots, local_len, lat), bf16),
            pltpu.VMEM((slots, k_t.shape[1], local_len), bf16),
            pltpu.VMEM((nb, 2, 2, 4, 32, lat), f32),
            pltpu.VMEM((nb, 2, 8, 128), f32),
            pltpu.VMEM((nb, 8, 128), f32),
            pltpu.VMEM((nb, 8, 128), f32),
            pltpu.VMEM((nb, 2, 4, 32, lat), f32),
            pltpu.VMEM((nb, 8, 128), f32),
            pltpu.VMEM((nb, 4, 32, lat), f32),
            pltpu.VMEM((nb, 8, 128), f32),
            pltpu.VMEM((nb, 4, 32, lat), f32),
            pltpu.VMEM((nb, 8, 128), f32),
            pltpu.VMEM((nb, 8, 128), f32),
            pltpu.VMEM((nb, 4, 32, lat), f32),
            pltpu.VMEM((nb, 8, 128), f32),
            pltpu.VMEM((nb, 8, 128), f32),
            pltpu.VMEM((128, 128), f32),
            dma((2,)), dma, dma((slots,)), dma((slots,)),
            dma((nb,)), dma((nb,)), dma((nb, 3)), dma((nb, 3)), dma((nb, 3)), dma((nb, 3)), dma((nb,)), dma((nb,)),
            dma((nb, 2)), dma((nb, 2)), dma((nb,)), dma((nb,)), dma((nb, 3)), dma((nb, 3)), dma((nb, 3)), dma((nb, 3)),
            dma((nb,)), dma((nb,)), dma((nb,)), dma((nb,)), dma((nb,)), dma((nb,)), dma((nb,)), dma((nb,)),
        ],
        compiler_params=pltpu.CompilerParams(
            collective_id=0, has_side_effects=True, vmem_limit_bytes=64 * 1024 * 1024 - 65536),
        name="attend_all",
    )(lens, q, q_rope, c_kv, k_t, hidden, w_uv)


def rope_kernel(h_ref, w_ref, out, acc, rows):
    step = pl.program_id(0)
    nb, nq, lanes = h_ref.shape
    h = h_ref[...].astype(f32).reshape(nb * nq, lanes).astype(bf16)
    part = lax.dot_general(w_ref[...], h, (((1,), (1,)), ((), ())), preferred_element_type=f32)

    @pl.when(step == 0)
    def _():
        acc[...] = part

    @pl.when(step > 0)
    def _():
        acc[...] += part

    @pl.when(step == pl.num_programs(0) - 1)
    def _():
        for h in range(8):
            rows[:, h, :] = acc[h * 64:(h + 1) * 64, :].T
        pairs = rows[...].reshape(nb, 2, 16, 64)
        out[...] = jnp.concatenate([pairs[:, 0], pairs[:, 1]], axis=-1).astype(bf16)


def rope_queries(hidden, w_t):
    nb, nq, dim = hidden.shape
    wide = w_t.shape[0]
    steps = next(k for k in (7, 4, 1) if dim % (k * 128) == 0)
    return pl.pallas_call(
        rope_kernel,
        grid=(steps,),
        out_shape=jax.ShapeDtypeStruct((nb, 16, 128), bf16),
        in_specs=[pl.BlockSpec((nb, nq, dim // steps), lambda i: (0, 0, i)), pl.BlockSpec((wide, dim // steps), lambda i: (0, i))],
        out_specs=pl.BlockSpec((nb, 16, 128), lambda i: (0, 0, 0)),
        scratch_shapes=[pltpu.VMEM((wide, nb * nq), f32), pltpu.VMEM((nb * nq, 8, 64), f32)],
        compiler_params=pltpu.CompilerParams(dimension_semantics=("arbitrary",)),
        name="rope_queries",
    )(hidden, w_t)


def total_kernel(ov_hbm, w_hbm, h_hbm, out, ov_ref, hbuf, ov_rows, wbuf, part, gat, rc_c, rc_y, rc_z,
                 in_sem, w_sem, sc_s, sc_r, sy_s, sy_r, sz_s, sz_r, gz_s, gz_r, gy_s, gy_r, gc_s, gc_r):
    _, z, y, c = place()
    chunks, lanes = wbuf.shape[0], wbuf.shape[4]
    deep = part.shape[3] // NZ
    core_peer, y_peer = seq_of(z, y, 1 - c), seq_of(z, 1 - y, c)
    zs = [lax.rem(z + d, NZ) for d in (1, 2, 3)]
    zf = [lax.rem(z + NZ - d, NZ) for d in (1, 2, 3)]

    def where(cc, yy, k):
        return pl.ds(pl.multiple_of((cc * NY + yy) * (chunks * lanes) + k * lanes, 128), lanes)

    def weights(k):
        return [pltpu.make_async_copy(w_hbm.at[:, where(cc, yy, k)], wbuf.at[k, cc, yy], w_sem.at[k, cc * 2 + yy])
                for cc in range(2) for yy in range(2)]

    inputs = (pltpu.make_async_copy(ov_hbm, ov_ref, in_sem.at[0]), pltpu.make_async_copy(h_hbm, hbuf, in_sem.at[1]))
    for cp in inputs:
        cp.start()
    for k in range(chunks):
        for cp in weights(k):
            cp.start()
    nb = ov_ref.shape[0]
    for cp in inputs:
        cp.wait()
    ov_rows[...] = ov_ref[...].astype(f32).reshape(ov_rows.shape).astype(bf16)
    meet([core_peer, y_peer] + [seq_of(p, y, c) for p in zs])

    def band(at):
        return pl.ds(pl.multiple_of(at * deep, deep), deep)

    def sum_c(k):
        return remote(part.at[k, 1 - c], rc_c.at[k], sc_s.at[k], sc_r.at[k], core_peer)

    def sum_y(k):
        return remote(part.at[k, c, 1 - y], rc_y.at[k], sy_s.at[k], sy_r.at[k], y_peer)

    def sum_z(k, d):
        return remote(part.at[k, c, y, band(zs[d])], rc_z.at[k, d], sz_s.at[k, d], sz_r.at[k, d], seq_of(zs[d], y, c))

    def give_z(k, d, at):
        piece = gat.at[k, c, y, band(at)]
        return remote(piece, piece, gz_s.at[k, d], gz_r.at[k, d], seq_of(zs[d], y, c))

    def give_y(k, yy):
        return remote(gat.at[k, c, yy], gat.at[k, c, yy], gy_s.at[k], gy_r.at[k], y_peer)

    def give_c(k, cc):
        return remote(gat.at[k, cc], gat.at[k, cc], gc_s.at[k], gc_r.at[k], core_peer)

    def multiply(k):
        for cp in weights(k):
            cp.wait()
        ov = ov_rows[...]
        for cc in (1 - c, c):
            for yy in range(2):
                part[k, cc, yy] = jnp.dot(ov, wbuf[k, cc, yy], preferred_element_type=f32)
            if cc is not c:
                sum_c(k).start()

    def step_d(k):
        sum_c(k).wait_recv()
        part[k, c] = part[k, c] + rc_c[k]
        sum_y(k).start()

    def step_e(k):
        sum_y(k).wait_recv()
        part[k, c, y] = part[k, c, y] + rc_y[k]
        for d in range(3):
            sum_z(k, d).start()

    def step_f(k):
        for d in range(3):
            sum_z(k, d).wait_recv()
        total = part[k, c, y, band(z)] + rc_z[k, 0] + rc_z[k, 1] + rc_z[k, 2]
        own = hbuf[:, :, pl.ds(pl.multiple_of(k * lanes, 128), lanes)].astype(f32).reshape(deep, lanes)
        gat[k, c, y, band(z)] = (own + total).astype(bf16)
        for d in range(3):
            give_z(k, d, z).start()

    def step_h(k):
        for d in range(3):
            give_z(k, d, zf[d]).wait_recv()
        give_y(k, y).start()

    def step_i(k):
        give_y(k, 1 - y).wait_recv()
        give_c(k, c).start()

    def step_j(k):
        give_c(k, 1 - c).wait_recv()
        for cc in range(2):
            for yy in range(2):
                out[:, :, where(cc, yy, k)] = gat[k, cc, yy].astype(f32).reshape(nb, -1, lanes).astype(bf16)

    steps = ((10, step_j), (9, step_i), (7, step_h), (5, step_f), (3, step_e), (1, step_d), (0, multiply))

    @pl.loop(0, chunks + 10)
    def _(it):
        for lag, fn in steps:
            k = it - lag

            @pl.when((k >= 0) & (k < chunks))
            def _(fn=fn, k=k):
                fn(k)

    @pl.loop(0, chunks)
    def _(k):
        sum_c(k).wait_send()
        sum_y(k).wait_send()
        for d in range(3):
            sum_z(k, d).wait_send()
            give_z(k, d, z).wait_send()
        give_y(k, y).wait_send()
        give_c(k, c).wait_send()


def total_all(ov, w_o, own_h):
    (nb, nq, _), dim = ov.shape, w_o.shape[1]
    n = nb * nq
    chunks = next(k for k in (7, 1) if dim % (4 * k * 128) == 0)
    lanes = dim // (4 * chunks)
    dma = pltpu.SemaphoreType.DMA
    vm, hbm = pl.BlockSpec(memory_space=pltpu.VMEM), pl.BlockSpec(memory_space=pl.ANY)
    one, three = dma((chunks,)), dma((chunks, 3))
    return pl.pallas_call(
        total_kernel,
        out_shape=jax.ShapeDtypeStruct((nb, nq, dim), bf16),
        in_specs=[hbm, hbm, hbm],
        out_specs=vm,
        scratch_shapes=[
            pltpu.VMEM(ov.shape, bf16),
            pltpu.VMEM(own_h.shape, bf16),
            pltpu.VMEM((n, w_o.shape[0]), bf16),
            pltpu.VMEM((chunks, 2, 2, w_o.shape[0], lanes), bf16),
            pltpu.VMEM((chunks, 2, 2, n, lanes), f32),
            pltpu.VMEM((chunks, 2, 2, n, lanes), bf16),
            pltpu.VMEM((chunks, 2, n, lanes), f32),
            pltpu.VMEM((chunks, n, lanes), f32),
            pltpu.VMEM((chunks, 3, n // NZ, lanes), f32),
            dma((2,)), dma((chunks, 4)), one, one, one, one, three, three, three, three, one, one, one, one,
        ],
        compiler_params=pltpu.CompilerParams(
            collective_id=1, has_side_effects=True, vmem_limit_bytes=64 * 1024 * 1024 - 65536),
        name="total_all",
    )(ov, w_o, own_h)


def solution(mesh):
    def local_step(hidden, cache_lens, c_kv, k_r, w_uq, w_qr, w_uk, w_uv, w_o):
        score_scale = (w_uq.shape[2] + w_qr.shape[2]) ** -0.5
        nb, nq, dim = hidden.shape
        nh, lat = w_uk.shape[0], w_uk.shape[2]
        q_nope = jnp.einsum("cre,eil->cril", hidden, w_uq, preferred_element_type=f32).astype(bf16)
        q_lat = jnp.einsum("bqhk,hkc->bqhc", q_nope, w_uk, preferred_element_type=f32).astype(bf16)
        q = q_lat.reshape(nb, 2, 16, 4, 128).transpose(0, 1, 3, 2, 4).reshape(nb, 8, 16, 128)
        q_rope = rope_queries(hidden, w_qr.transpose(1, 2, 0).reshape(-1, dim))
        o_val, own_h = attend_all(q, q_rope, cache_lens, c_kv, jnp.swapaxes(k_r, 1, 2), hidden, w_uv, score_scale)
        return total_all(o_val, w_o.reshape(-1, dim), own_h)

    specs_in = (P("batch", None, None), P("batch"), P("batch", "seq", None), P("batch", "seq", None),
                P(None, "seq", None), P(None, "seq", None), P("seq", None, None), P("seq", None, None),
                P("seq", None, None))
    return jax.shard_map(local_step, mesh=mesh, in_specs=specs_in, out_specs=P("batch", None, None), check_vma=False)
```

```python
import functools
import math

import jax
import jax.numpy as jnp
from jax import lax
from jax.experimental import pallas as pl
from jax.experimental.pallas import tpu as pltpu
from jax.sharding import PartitionSpec as P

MASK_FILL = -1e30
NZ, NY, NC = 4, 2, 2
MESH = pl.DeviceIdType.MESH
f32, bf16 = jnp.float32, jnp.bfloat16


def place():
    s = lax.axis_index("seq")
    return s, s // (NY * NC), (s // NC) % NY, s % NC


def seq_of(z, y, c):
    return (z * NY + y) * NC + c


def remote(src, dst, send_sem, recv_sem, seq):
    return pltpu.make_async_remote_copy(
        src_ref=src, dst_ref=dst, send_sem=send_sem, recv_sem=recv_sem,
        device_id={"seq": seq}, device_id_type=MESH)


def meet(peers):
    barrier = pltpu.get_barrier_semaphore()
    for p in peers:
        pl.semaphore_signal(barrier, inc=1, device_id={"seq": p}, device_id_type=MESH)
    pl.semaphore_wait(barrier, len(peers))


def columns(rows):
    pad = jnp.zeros((128 - rows.shape[0], 128), f32)
    return jnp.concatenate([rows, pad], axis=0).T


def attend_kernel(scale, lens, q_hbm, r_hbm, c_hbm, k_hbm, h_hbm, wuv, out, h_out,
                  qbuf, ck, kr, o_full, ml0, ml1, ml2, rc_c, ml_c, rc_y, ml_y,
                  rc_u, ml_u, ml_us, rc_d, ml_d, ml_ds, wcol,
                  q_sem, h_sem, c_sem, k_sem,
                  ay_s, ay_r, au_s, au_r, ad_s, ad_r, ac_s, ac_r,
                  oc_s, oc_r, oy_s, oy_r, ou_s, ou_r, od_s, od_r,
                  mc_s, mc_r, my_s, my_r, mu_s, mu_r, md_s, md_r):
    nb, slots = q_hbm.shape[0], ck.shape[0]
    local_len = ck.shape[1]
    s, z, y, c = place()
    core_peer, y_peer = seq_of(z, y, 1 - c), seq_of(z, 1 - y, c)
    upper, lower = seq_of(lax.rem(z + 1, NZ), y, c), seq_of(lax.rem(z + NZ - 1, NZ), y, c)

    own_q = (pltpu.make_async_copy(q_hbm, qbuf.at[:, c, y, z, pl.ds(0, 8)], q_sem.at[0]),
             pltpu.make_async_copy(r_hbm, qbuf.at[:, c, y, z, 8], q_sem.at[1]))
    for cp in own_q:
        cp.start()

    def cache(b):
        k = lax.rem(b, slots)
        return (pltpu.make_async_copy(c_hbm.at[b], ck.at[k], c_sem.at[k]),
                pltpu.make_async_copy(k_hbm.at[b], kr.at[k], k_sem.at[k]))

    for b in range(slots - 1):
        for cp in cache(b):
            cp.start()

    deep, wide = h_out.shape[0], h_out.shape[2]
    own_h = pltpu.make_async_copy(
        h_hbm.at[pl.ds(z * deep, deep), :, pl.ds(pl.multiple_of((c * NY + y) * wide, 128), wide)], h_out, h_sem)
    own_h.start()
    meet([core_peer, y_peer, upper, lower])
    for cp in own_q:
        cp.wait()

    def gather_y(b, yy):
        part = qbuf.at[b, c, yy, z]
        return remote(part, part, ay_s.at[b], ay_r.at[b], y_peer)

    def gather_up(b, origin, d):
        part = qbuf.at[b, c, :, origin]
        return remote(part, part, au_s.at[b, d - 1], au_r.at[b, d - 1], upper)

    def gather_down(b, origin, d):
        part = qbuf.at[b, c, :, origin]
        return remote(part, part, ad_s.at[b, d - 1], ad_r.at[b, d - 1], lower)

    def gather_c(b, cc):
        part = qbuf.at[b, cc]
        return remote(part, part, ac_s.at[b], ac_r.at[b], core_peer)

    def sum_c(b, hf):
        rows = pl.ds(hf * 16, 16)
        return remote(o_full.at[b, 1 - c, :, :, rows], rc_c.at[b, :, :, rows], oc_s.at[b, hf], oc_r.at[b, hf], core_peer)

    def stat_c(b):
        return remote(ml0.at[b, 1 - c], ml_c.at[b], mc_s.at[b], mc_r.at[b], core_peer)

    def sum_y(b):
        return (remote(o_full.at[b, c, 1 - y], rc_y.at[b], oy_s.at[b], oy_r.at[b], y_peer),
                remote(ml1.at[b], ml_y.at[b], my_s.at[b], my_r.at[b], y_peer))

    def sum_up(b, dest, d):
        return remote(o_full.at[b, c, y, dest], rc_u.at[b, dest], ou_s.at[b, d - 1], ou_r.at[b, d - 1], upper)

    def stat_up(b, stat):
        return remote(stat.at[b], ml_u.at[b], mu_s.at[b], mu_r.at[b], upper)

    def sum_down(b, dest, d):
        return remote(o_full.at[b, c, y, dest], rc_d.at[b, dest], od_s.at[b, d - 1], od_r.at[b, d - 1], lower)

    def stat_down(b, stat):
        return remote(stat.at[b], ml_d.at[b], md_s.at[b], md_r.at[b], lower)

    def pass_on(b, d):
        @pl.when((z < NZ - 1) & (z - (d - 1) >= 0))
        def _():
            gather_up(b, z - (d - 1), d).start()

        @pl.when((z > 0) & (z + (d - 1) < NZ))
        def _():
            gather_down(b, z + (d - 1), d).start()

    def arrive(b, d):
        @pl.when(z - d >= 0)
        def _():
            gather_up(b, z - d, d).wait_recv()

        @pl.when(z + d < NZ)
        def _():
            gather_down(b, z + d, d).wait_recv()

    def step_z1(b):
        gather_y(b, 1 - y).wait_recv()
        pass_on(b, 1)

    def step_z2(b):
        arrive(b, 1)
        pass_on(b, 2)

    def step_z3(b):
        arrive(b, 2)
        pass_on(b, 3)

    def step_z4(b):
        arrive(b, 3)
        gather_c(b, c).start()

    def attend(b):
        gather_c(b, 1 - c).wait_recv()
        for cp in cache(b):
            cp.wait()

        @pl.when(b + slots - 1 < nb)
        def _():
            for cp in cache(b + slots - 1):
                cp.start()

        k = lax.rem(b, slots)
        row_len = lens[b]
        pos = s * local_len + lax.broadcasted_iota(jnp.int32, (512, local_len), 1)
        row = lax.broadcasted_iota(jnp.int32, (512, 1), 0)
        token = (row // 256) * 2 + lax.rem(row, 16) // 8
        lane = lax.broadcasted_iota(jnp.int32, (512, 128), 1)
        q = jnp.concatenate(
            [jnp.concatenate([qbuf[b, :, :, :, hf * 4 + j].reshape(256, 128) for j in range(4)], axis=1) for hf in range(2)], axis=0)
        both = qbuf[b, :, :, :, 8].reshape(256, 128)
        qr = jnp.concatenate([both[:, :64], both[:, 64:]], axis=0)
        sc = lax.dot_general(q, ck[k], (((1,), (1,)), ((), ())), preferred_element_type=f32)
        sc = sc + jnp.dot(qr, kr[k], preferred_element_type=f32)
        sc = jnp.where(pos <= row_len + token, sc, MASK_FILL)
        m = jnp.max(sc, axis=1, keepdims=True)
        p = jnp.exp2((sc - m) * scale)
        l = jnp.sum(p, axis=1, keepdims=True)
        o = jnp.dot(p.astype(bf16), ck[k], preferred_element_type=f32)
        stat = jnp.where(lane == 0, m * scale, jnp.where(lane == 1, l, 0.0)).T
        for hf in range(2):
            o_full[b, :, :, :, hf * 16:(hf + 1) * 16, :] = o[hf * 256:(hf + 1) * 256].reshape(2, 2, 4, 16, o.shape[1])
            for cc in range(2):
                at = hf * 256 + cc * 128
                ml0[b, cc, hf * 2:hf * 2 + 2, :] = stat[0:2, at:at + 128]
            sum_c(b, hf).start()
        stat_c(b).start()

    def merge_stats(parts, final):
        stats, factors = [], []
        for hf in range(2):
            ms, ls = [p[2 * hf:2 * hf + 1] for p in parts], [p[2 * hf + 1:2 * hf + 2] for p in parts]
            top = functools.reduce(jnp.maximum, ms)
            ws = [jnp.exp2(m - top) for m in ms]
            total = sum(w * l for w, l in zip(ws, ls))
            stats += [top, total]
            factors += [w / total for w in ws] if final else ws
        return jnp.concatenate(stats, axis=0), columns(jnp.concatenate(factors, axis=0))

    def step_d(b):
        for hf in range(2):
            sum_c(b, hf).wait_recv()
        stat_c(b).wait_recv()
        stats, cols = merge_stats([ml0[b, c, 0:4], ml_c[b, 0:4]], False)
        ml1[b, 0:4, :] = stats
        for hf in range(2):
            rows = pl.ds(hf * 16, 16)
            wa, wb = (cols[:, 2 * hf + j:2 * hf + j + 1].reshape(2, 4, 16, 1) for j in range(2))
            o_full[b, c, :, :, rows, :] = o_full[b, c, :, :, rows, :] * wa + rc_c[b, :, :, rows, :] * wb
        for cp in sum_y(b):
            cp.start()

    def step_e(b):
        for cp in sum_y(b):
            cp.wait_recv()
        stats, cols = merge_stats([ml1[b, 0:4], ml_y[b, 0:4]], False)
        ml2[b, 0:4, :] = stats
        wcol[...] = cols
        cols = wcol[pl.ds(pl.multiple_of(y * 64, 64), 64), :]
        for hf in range(2):
            rows = pl.ds(hf * 16, 16)
            wa, wb = (cols[:, 2 * hf + j:2 * hf + j + 1].reshape(4, 16, 1) for j in range(2))
            o_full[b, c, y, :, rows, :] = o_full[b, c, y, :, rows, :] * wa + rc_y[b, :, rows, :] * wb

        @pl.when(z == 0)
        def _():
            stat_up(b, ml2).start()
            for dest in range(NZ - 1, 0, -1):
                sum_up(b, dest, dest).start()

        @pl.when(z == NZ - 1)
        def _():
            stat_down(b, ml2).start()
            for dest in range(NZ - 1):
                sum_down(b, dest, NZ - 1 - dest).start()

    def relay(b, dests, stats_in, stats_out, arrived, wait, send):
        stats, cols = merge_stats([ml2[b, 0:4], stats_in[b, 0:4]], False)
        stats_out[b, 0:4, :] = stats
        wcol[...] = cols
        for i, dest in enumerate(dests):
            wait(dest)
            cols = wcol[pl.ds(pl.multiple_of(y * 64 + dest * 16, 16), 16), :]
            for hf in range(2):
                rows = pl.ds(hf * 16, 16)
                wa, wb = (cols[:, 2 * hf + j:2 * hf + j + 1] for j in range(2))
                o_full[b, c, y, dest, rows, :] = o_full[b, c, y, dest, rows, :] * wa + arrived[b, dest, rows, :] * wb
            if i == 0:
                send(None)
            send(dest)

    def step_g(hop, b):
        at = NZ - 1 - hop

        @pl.when(z == hop)
        def _():
            def send(dest):
                (stat_up(b, ml_us) if dest is None else sum_up(b, dest, dest - hop)).start()
            stat_up(b, ml2).wait_recv()
            relay(b, range(NZ - 1, hop, -1), ml_u, ml_us, rc_u, lambda dest: sum_up(b, dest, dest - hop + 1).wait_recv(), send)

        @pl.when(z == at)
        def _():
            def send(dest):
                (stat_down(b, ml_ds) if dest is None else sum_down(b, dest, at - dest)).start()
            stat_down(b, ml2).wait_recv()
            relay(b, range(at), ml_d, ml_ds, rc_d, lambda dest: sum_down(b, dest, at - dest + 1).wait_recv(), send)

    def finish(b, at):
        parts, sums = [ml2[b, 0:4]], [o_full.at[b, c, y, at]]
        if at > 0:
            sum_up(b, at, 1).wait_recv()
            if at == NZ - 1:
                stat_up(b, ml2).wait_recv()
            parts.append(ml_u[b, 0:4])
            sums.append(rc_u.at[b, at])
        if at < NZ - 1:
            sum_down(b, at, 1).wait_recv()
            if at == 0:
                stat_down(b, ml2).wait_recv()
            parts.append(ml_d[b, 0:4])
            sums.append(rc_d.at[b, at])
        wcol[...] = merge_stats(parts, True)[1]
        cols = wcol[pl.ds(pl.multiple_of(y * 64 + at * 16, 16), 16), :]
        n = len(parts)
        halves = []
        for hf in range(2):
            rows = pl.ds(hf * 16, 16)
            o = sum(part[rows, :] * cols[:, n * hf + j:n * hf + j + 1] for j, part in enumerate(sums))
            halves.append(o.astype(bf16))
        o = jnp.concatenate(halves, axis=0)
        head = lax.rem(lax.broadcasted_iota(jnp.int32, (32, 128), 0), 8)
        for h in range(8):
            v = jnp.dot(o, wuv[h], preferred_element_type=f32)
            v = jnp.where(head == h, v, 0.0).reshape(4, 8, 128).sum(axis=1)
            out[b, :, h * 128:(h + 1) * 128] = v.astype(bf16)

    def step_f(b):
        for at in range(NZ):
            @pl.when(z == at)
            def _(at=at):
                finish(b, at)

    @pl.loop(0, nb)
    def _(b):
        gather_y(b, y).start()

    steps = ((7, step_e), (8, functools.partial(step_g, 1)), (9, functools.partial(step_g, 2)), (10, step_f),
             (0, step_z1), (1, step_z2), (2, step_z3), (3, step_z4), (5, step_d), (4, attend))

    @pl.loop(0, nb + 10)
    def _(it):
        for lag, fn in steps:
            b = it - lag

            @pl.when((b >= 0) & (b < nb))
            def _(fn=fn, b=b):
                fn(b)

    own_h.wait()

    @pl.loop(0, nb)
    def _(b):
        gather_y(b, y).wait_send()
        gather_c(b, c).wait_send()
        for d in (1, 2, 3):
            @pl.when((z < NZ - 1) & (z - (d - 1) >= 0))
            def _(d=d):
                gather_up(b, z - (d - 1), d).wait_send()

            @pl.when((z > 0) & (z + (d - 1) < NZ))
            def _(d=d):
                gather_down(b, z + (d - 1), d).wait_send()
        sum_c(b, 0).wait_send()
        sum_c(b, 1).wait_send()
        stat_c(b).wait_send()
        for cp in sum_y(b):
            cp.wait_send()
        for at in range(NZ):
            @pl.when(z == at)
            def _(at=at):
                for dest in range(at + 1, NZ):
                    sum_up(b, dest, dest - at).wait_send()
                if at < NZ - 1:
                    stat_up(b, ml2).wait_send()
                for dest in range(at):
                    sum_down(b, dest, at - dest).wait_send()
                if at > 0:
                    stat_down(b, ml2).wait_send()


def attend_all(q, q_rope, lens, c_kv, k_t, hidden, w_uv, score_scale):
    nb, local_len, lat = c_kv.shape
    nq, dim = hidden.shape[1:]
    slots = 3
    dma = pltpu.SemaphoreType.DMA
    return pl.pallas_call(
        functools.partial(attend_kernel, score_scale * math.log2(math.e)),
        out_shape=(jax.ShapeDtypeStruct((nb, nq, w_uv.shape[0] * w_uv.shape[2]), bf16),
                   jax.ShapeDtypeStruct((nb // NZ, nq, dim // 4), bf16)),
        in_specs=[pl.BlockSpec(memory_space=pltpu.SMEM)] + [pl.BlockSpec(memory_space=pl.ANY)] * 5
        + [pl.BlockSpec(memory_space=pltpu.VMEM)],
        out_specs=(pl.BlockSpec(memory_space=pltpu.VMEM), pl.BlockSpec(memory_space=pltpu.VMEM)),
        scratch_shapes=[
            pltpu.VMEM((nb, 2, 2, 4, 9, 16, 128), bf16),
            pltpu.VMEM((slots, local_len, lat), bf16),
            pltpu.VMEM((slots, k_t.shape[1], local_len), bf16),
            pltpu.VMEM((nb, 2, 2, 4, 32, lat), f32),
            pltpu.VMEM((nb, 2, 8, 128), f32),
            pltpu.VMEM((nb, 8, 128), f32),
            pltpu.VMEM((nb, 8, 128), f32),
            pltpu.VMEM((nb, 2, 4, 32, lat), f32),
            pltpu.VMEM((nb, 8, 128), f32),
            pltpu.VMEM((nb, 4, 32, lat), f32),
            pltpu.VMEM((nb, 8, 128), f32),
            pltpu.VMEM((nb, 4, 32, lat), f32),
            pltpu.VMEM((nb, 8, 128), f32),
            pltpu.VMEM((nb, 8, 128), f32),
            pltpu.VMEM((nb, 4, 32, lat), f32),
            pltpu.VMEM((nb, 8, 128), f32),
            pltpu.VMEM((nb, 8, 128), f32),
            pltpu.VMEM((128, 128), f32),
            dma((2,)), dma, dma((slots,)), dma((slots,)),
            dma((nb,)), dma((nb,)), dma((nb, 3)), dma((nb, 3)), dma((nb, 3)), dma((nb, 3)), dma((nb,)), dma((nb,)),
            dma((nb, 2)), dma((nb, 2)), dma((nb,)), dma((nb,)), dma((nb, 3)), dma((nb, 3)), dma((nb, 3)), dma((nb, 3)),
            dma((nb,)), dma((nb,)), dma((nb,)), dma((nb,)), dma((nb,)), dma((nb,)), dma((nb,)), dma((nb,)),
        ],
        compiler_params=pltpu.CompilerParams(
            collective_id=0, has_side_effects=True, vmem_limit_bytes=64 * 1024 * 1024 - 65536),
        name="attend_all",
    )(lens, q, q_rope, c_kv, k_t, hidden, w_uv)


def rope_kernel(h_ref, w_ref, out, flat, rows):
    head = pl.program_id(0)
    nb, nq, _ = h_ref.shape

    @pl.when(head == 0)
    def _():
        flat[...] = h_ref[...].astype(f32).reshape(flat.shape).astype(bf16)

    rows[head] = lax.dot_general(flat[...], w_ref[0], (((1,), (1,)), ((), ())), preferred_element_type=f32)

    @pl.when(head == pl.num_programs(0) - 1)
    def _():
        pairs = jnp.stack([rows[h] for h in range(8)], axis=1).reshape(nb, 2, 16, 64)
        out[...] = jnp.concatenate([pairs[:, 0], pairs[:, 1]], axis=-1).astype(bf16)


def rope_queries(hidden, w_t):
    nb, nq, dim = hidden.shape
    heads, wide = w_t.shape[:2]
    return pl.pallas_call(
        rope_kernel,
        grid=(heads,),
        out_shape=jax.ShapeDtypeStruct((nb, 16, 128), bf16),
        in_specs=[pl.BlockSpec((nb, nq, dim), lambda i: (0, 0, 0)), pl.BlockSpec((1, wide, dim), lambda i: (i, 0, 0))],
        out_specs=pl.BlockSpec((nb, 16, 128), lambda i: (0, 0, 0)),
        scratch_shapes=[pltpu.VMEM((nb * nq, dim), bf16), pltpu.VMEM((heads, nb * nq, wide), f32)],
        compiler_params=pltpu.CompilerParams(dimension_semantics=("arbitrary",)),
        name="rope_queries",
    )(hidden, w_t)


def total_kernel(ov_ref, w_hbm, hbuf, out, ov_rows, wbuf, part, gat, rc_c, rc_y, rc_z,
                 w_sem, sc_s, sc_r, sy_s, sy_r, sz_s, sz_r, gz_s, gz_r, gy_s, gy_r, gc_s, gc_r):
    _, z, y, c = place()
    chunks, lanes = wbuf.shape[0], wbuf.shape[4]
    deep = part.shape[3] // NZ
    core_peer, y_peer = seq_of(z, y, 1 - c), seq_of(z, 1 - y, c)
    zs = [lax.rem(z + d, NZ) for d in (1, 2, 3)]
    zf = [lax.rem(z + NZ - d, NZ) for d in (1, 2, 3)]

    def where(cc, yy, k):
        return pl.ds(pl.multiple_of((cc * NY + yy) * (chunks * lanes) + k * lanes, 128), lanes)

    def weights(k):
        return [pltpu.make_async_copy(w_hbm.at[:, where(cc, yy, k)], wbuf.at[k, cc, yy], w_sem.at[k, cc * 2 + yy])
                for cc in range(2) for yy in range(2)]

    for k in range(chunks):
        for cp in weights(k):
            cp.start()
    nb = ov_ref.shape[0]
    ov_rows[...] = ov_ref[...].astype(f32).reshape(ov_rows.shape).astype(bf16)
    meet([core_peer, y_peer] + [seq_of(p, y, c) for p in zs])

    def band(at):
        return pl.ds(pl.multiple_of(at * deep, deep), deep)

    def sum_c(k):
        return remote(part.at[k, 1 - c], rc_c.at[k], sc_s.at[k], sc_r.at[k], core_peer)

    def sum_y(k):
        return remote(part.at[k, c, 1 - y], rc_y.at[k], sy_s.at[k], sy_r.at[k], y_peer)

    def sum_z(k, d):
        return remote(part.at[k, c, y, band(zs[d])], rc_z.at[k, d], sz_s.at[k, d], sz_r.at[k, d], seq_of(zs[d], y, c))

    def give_z(k, d, at):
        piece = gat.at[k, c, y, band(at)]
        return remote(piece, piece, gz_s.at[k, d], gz_r.at[k, d], seq_of(zs[d], y, c))

    def give_y(k, yy):
        return remote(gat.at[k, c, yy], gat.at[k, c, yy], gy_s.at[k], gy_r.at[k], y_peer)

    def give_c(k, cc):
        return remote(gat.at[k, cc], gat.at[k, cc], gc_s.at[k], gc_r.at[k], core_peer)

    def multiply(k):
        for cp in weights(k):
            cp.wait()
        ov = ov_rows[...]
        for cc in (1 - c, c):
            for yy in range(2):
                part[k, cc, yy] = jnp.dot(ov, wbuf[k, cc, yy], preferred_element_type=f32)
            if cc is not c:
                sum_c(k).start()

    def step_d(k):
        sum_c(k).wait_recv()
        part[k, c] = part[k, c] + rc_c[k]
        sum_y(k).start()

    def step_e(k):
        sum_y(k).wait_recv()
        part[k, c, y] = part[k, c, y] + rc_y[k]
        for d in range(3):
            sum_z(k, d).start()

    def step_f(k):
        for d in range(3):
            sum_z(k, d).wait_recv()
        total = part[k, c, y, band(z)] + rc_z[k, 0] + rc_z[k, 1] + rc_z[k, 2]
        own = hbuf[:, :, pl.ds(pl.multiple_of(k * lanes, 128), lanes)].astype(f32).reshape(deep, lanes)
        gat[k, c, y, band(z)] = (own + total).astype(bf16)
        for d in range(3):
            give_z(k, d, z).start()

    def step_h(k):
        for d in range(3):
            give_z(k, d, zf[d]).wait_recv()
        give_y(k, y).start()

    def step_i(k):
        give_y(k, 1 - y).wait_recv()
        give_c(k, c).start()

    def step_j(k):
        give_c(k, 1 - c).wait_recv()
        for cc in range(2):
            for yy in range(2):
                out[:, :, where(cc, yy, k)] = gat[k, cc, yy].astype(f32).reshape(nb, -1, lanes).astype(bf16)

    steps = ((10, step_j), (9, step_i), (7, step_h), (5, step_f), (3, step_e), (1, step_d), (0, multiply))

    @pl.loop(0, chunks + 10)
    def _(it):
        for lag, fn in steps:
            k = it - lag

            @pl.when((k >= 0) & (k < chunks))
            def _(fn=fn, k=k):
                fn(k)

    @pl.loop(0, chunks)
    def _(k):
        sum_c(k).wait_send()
        sum_y(k).wait_send()
        for d in range(3):
            sum_z(k, d).wait_send()
            give_z(k, d, z).wait_send()
        give_y(k, y).wait_send()
        give_c(k, c).wait_send()


def total_all(ov, w_o, own_h):
    (nb, nq, _), dim = ov.shape, w_o.shape[1]
    n = nb * nq
    chunks = next(k for k in (7, 1) if dim % (4 * k * 128) == 0)
    lanes = dim // (4 * chunks)
    dma = pltpu.SemaphoreType.DMA
    vm, hbm = pl.BlockSpec(memory_space=pltpu.VMEM), pl.BlockSpec(memory_space=pl.ANY)
    one, three = dma((chunks,)), dma((chunks, 3))
    return pl.pallas_call(
        total_kernel,
        out_shape=jax.ShapeDtypeStruct((nb, nq, dim), bf16),
        in_specs=[vm, hbm, vm],
        out_specs=vm,
        scratch_shapes=[
            pltpu.VMEM((n, w_o.shape[0]), bf16),
            pltpu.VMEM((chunks, 2, 2, w_o.shape[0], lanes), bf16),
            pltpu.VMEM((chunks, 2, 2, n, lanes), f32),
            pltpu.VMEM((chunks, 2, 2, n, lanes), bf16),
            pltpu.VMEM((chunks, 2, n, lanes), f32),
            pltpu.VMEM((chunks, n, lanes), f32),
            pltpu.VMEM((chunks, 3, n // NZ, lanes), f32),
            dma((chunks, 4)), one, one, one, one, three, three, three, three, one, one, one, one,
        ],
        compiler_params=pltpu.CompilerParams(
            collective_id=1, has_side_effects=True, vmem_limit_bytes=40 * 1024 * 1024),
        name="total_all",
    )(ov, w_o, own_h)


def solution(mesh):
    def local_step(hidden, cache_lens, c_kv, k_r, w_uq, w_qr, w_uk, w_uv, w_o):
        score_scale = (w_uq.shape[2] + w_qr.shape[2]) ** -0.5
        nb, nq, dim = hidden.shape
        nh, lat = w_uk.shape[0], w_uk.shape[2]
        q_nope = jnp.einsum("cre,eil->cril", hidden, w_uq, preferred_element_type=f32).astype(bf16)
        q_lat = jnp.einsum("bqhk,hkc->bqhc", q_nope, w_uk, preferred_element_type=f32).astype(bf16)
        q = q_lat.reshape(nb, 2, 16, 4, 128).transpose(0, 1, 3, 2, 4).reshape(nb, 8, 16, 128)
        q_rope = rope_queries(hidden, w_qr.transpose(1, 2, 0))
        o_val, own_h = attend_all(q, q_rope, cache_lens, c_kv, jnp.swapaxes(k_r, 1, 2), hidden, w_uv, score_scale)
        return total_all(o_val, w_o.reshape(-1, dim), own_h)

    specs_in = (P("batch", None, None), P("batch"), P("batch", "seq", None), P("batch", "seq", None),
                P(None, "seq", None), P(None, "seq", None), P("seq", None, None), P("seq", None, None),
                P("seq", None, None))
    return jax.shard_map(local_step, mesh=mesh, in_specs=specs_in, out_specs=P("batch", None, None), check_vma=False)
```

```python
import functools
import math

import jax
import jax.numpy as jnp
from jax import lax
from jax.experimental import pallas as pl
from jax.experimental.pallas import tpu as pltpu
from jax.sharding import PartitionSpec as P

MASK_FILL = -1e30
NZ, NY, NC = 4, 2, 2
MESH = pl.DeviceIdType.MESH
f32, bf16 = jnp.float32, jnp.bfloat16


def place():
    s = lax.axis_index("seq")
    return s, s // (NY * NC), (s // NC) % NY, s % NC


def seq_of(z, y, c):
    return (z * NY + y) * NC + c


def remote(src, dst, send_sem, recv_sem, seq):
    return pltpu.make_async_remote_copy(
        src_ref=src, dst_ref=dst, send_sem=send_sem, recv_sem=recv_sem,
        device_id={"seq": seq}, device_id_type=MESH)


def meet(peers):
    barrier = pltpu.get_barrier_semaphore()
    for p in peers:
        pl.semaphore_signal(barrier, inc=1, device_id={"seq": p}, device_id_type=MESH)
    pl.semaphore_wait(barrier, len(peers))


def columns(rows):
    pad = jnp.zeros((128 - rows.shape[0], 128), f32)
    return jnp.concatenate([rows, pad], axis=0).T


def attend_kernel(scale, lens, q_hbm, r_hbm, c_hbm, k_hbm, h_hbm, wuv, out, h_out,
                  qbuf, ck, kr, o_full, ml0, ml1, ml2, rc_c, ml_c, rc_y, ml_y,
                  rc_u, ml_u, ml_us, rc_d, ml_d, ml_ds, wcol,
                  q_sem, h_sem, c_sem, k_sem,
                  ay_s, ay_r, au_s, au_r, ad_s, ad_r, ac_s, ac_r,
                  oc_s, oc_r, oy_s, oy_r, ou_s, ou_r, od_s, od_r,
                  mc_s, mc_r, my_s, my_r, mu_s, mu_r, md_s, md_r):
    nb, slots = q_hbm.shape[0], ck.shape[0]
    local_len = ck.shape[1]
    s, z, y, c = place()
    core_peer, y_peer = seq_of(z, y, 1 - c), seq_of(z, 1 - y, c)
    upper, lower = seq_of(lax.rem(z + 1, NZ), y, c), seq_of(lax.rem(z + NZ - 1, NZ), y, c)

    own_q = (pltpu.make_async_copy(q_hbm, qbuf.at[:, c, y, z, pl.ds(0, 8)], q_sem.at[0]),
             pltpu.make_async_copy(r_hbm, qbuf.at[:, c, y, z, 8], q_sem.at[1]))
    for cp in own_q:
        cp.start()

    def cache(b):
        k = lax.rem(b, slots)
        return (pltpu.make_async_copy(c_hbm.at[b], ck.at[k], c_sem.at[k]),
                pltpu.make_async_copy(k_hbm.at[b], kr.at[k], k_sem.at[k]))

    for b in range(slots - 1):
        for cp in cache(b):
            cp.start()

    deep, wide = h_out.shape[0], h_out.shape[2]
    own_h = pltpu.make_async_copy(
        h_hbm.at[pl.ds(z * deep, deep), :, pl.ds(pl.multiple_of((c * NY + y) * wide, 128), wide)], h_out, h_sem)
    own_h.start()
    meet([core_peer, y_peer, upper, lower])
    for cp in own_q:
        cp.wait()

    def gather_y(b, yy):
        part = qbuf.at[b, c, yy, z]
        return remote(part, part, ay_s.at[b], ay_r.at[b], y_peer)

    def gather_up(b, origin, d):
        part = qbuf.at[b, c, :, origin]
        return remote(part, part, au_s.at[b, d - 1], au_r.at[b, d - 1], upper)

    def gather_down(b, origin, d):
        part = qbuf.at[b, c, :, origin]
        return remote(part, part, ad_s.at[b, d - 1], ad_r.at[b, d - 1], lower)

    def gather_c(b, cc):
        part = qbuf.at[b, cc]
        return remote(part, part, ac_s.at[b], ac_r.at[b], core_peer)

    def sum_c(b, hf):
        rows = pl.ds(hf * 16, 16)
        return remote(o_full.at[b, 1 - c, :, :, rows], rc_c.at[b, :, :, rows], oc_s.at[b, hf], oc_r.at[b, hf], core_peer)

    def stat_c(b):
        return remote(ml0.at[b, 1 - c], ml_c.at[b], mc_s.at[b], mc_r.at[b], core_peer)

    def sum_y(b):
        return (remote(o_full.at[b, c, 1 - y], rc_y.at[b], oy_s.at[b], oy_r.at[b], y_peer),
                remote(ml1.at[b], ml_y.at[b], my_s.at[b], my_r.at[b], y_peer))

    def sum_up(b, dest, d):
        return remote(o_full.at[b, c, y, dest], rc_u.at[b, dest], ou_s.at[b, d - 1], ou_r.at[b, d - 1], upper)

    def stat_up(b, stat):
        return remote(stat.at[b], ml_u.at[b], mu_s.at[b], mu_r.at[b], upper)

    def sum_down(b, dest, d):
        return remote(o_full.at[b, c, y, dest], rc_d.at[b, dest], od_s.at[b, d - 1], od_r.at[b, d - 1], lower)

    def stat_down(b, stat):
        return remote(stat.at[b], ml_d.at[b], md_s.at[b], md_r.at[b], lower)

    def pass_on(b, d):
        @pl.when((z < NZ - 1) & (z - (d - 1) >= 0))
        def _():
            gather_up(b, z - (d - 1), d).start()

        @pl.when((z > 0) & (z + (d - 1) < NZ))
        def _():
            gather_down(b, z + (d - 1), d).start()

    def arrive(b, d):
        @pl.when(z - d >= 0)
        def _():
            gather_up(b, z - d, d).wait_recv()

        @pl.when(z + d < NZ)
        def _():
            gather_down(b, z + d, d).wait_recv()

    def step_z1(b):
        gather_y(b, 1 - y).wait_recv()
        pass_on(b, 1)

    def step_z2(b):
        arrive(b, 1)
        pass_on(b, 2)

    def step_z3(b):
        arrive(b, 2)
        pass_on(b, 3)

    def step_z4(b):
        arrive(b, 3)
        gather_c(b, c).start()

    def attend(b):
        gather_c(b, 1 - c).wait_recv()
        for cp in cache(b):
            cp.wait()

        @pl.when(b + slots - 1 < nb)
        def _():
            for cp in cache(b + slots - 1):
                cp.start()

        k = lax.rem(b, slots)
        row_len = lens[b]
        pos = s * local_len + lax.broadcasted_iota(jnp.int32, (512, local_len), 1)
        row = lax.broadcasted_iota(jnp.int32, (512, 1), 0)
        token = (row // 256) * 2 + lax.rem(row, 16) // 8
        lane = lax.broadcasted_iota(jnp.int32, (512, 128), 1)
        q = jnp.concatenate(
            [jnp.concatenate([qbuf[b, :, :, :, hf * 4 + j].reshape(256, 128) for j in range(4)], axis=1) for hf in range(2)], axis=0)
        both = qbuf[b, :, :, :, 8].reshape(256, 128)
        qr = jnp.concatenate([both[:, :64], both[:, 64:]], axis=0)
        sc = lax.dot_general(q, ck[k], (((1,), (1,)), ((), ())), preferred_element_type=f32)
        sc = sc + jnp.dot(qr, kr[k], preferred_element_type=f32)
        sc = jnp.where(pos <= row_len + token, sc, MASK_FILL)
        m = jnp.max(sc, axis=1, keepdims=True)
        p = jnp.exp2((sc - m) * scale)
        l = jnp.sum(p, axis=1, keepdims=True)
        o = jnp.dot(p.astype(bf16), ck[k], preferred_element_type=f32)
        stat = jnp.where(lane == 0, m * scale, jnp.where(lane == 1, l, 0.0)).T
        for hf in range(2):
            o_full[b, :, :, :, hf * 16:(hf + 1) * 16, :] = o[hf * 256:(hf + 1) * 256].reshape(2, 2, 4, 16, o.shape[1])
            for cc in range(2):
                at = hf * 256 + cc * 128
                ml0[b, cc, hf * 2:hf * 2 + 2, :] = stat[0:2, at:at + 128]
            sum_c(b, hf).start()
        stat_c(b).start()

    def merge_stats(parts, final):
        stats, factors = [], []
        for hf in range(2):
            ms, ls = [p[2 * hf:2 * hf + 1] for p in parts], [p[2 * hf + 1:2 * hf + 2] for p in parts]
            top = functools.reduce(jnp.maximum, ms)
            ws = [jnp.exp2(m - top) for m in ms]
            total = sum(w * l for w, l in zip(ws, ls))
            stats += [top, total]
            factors += [w / total for w in ws] if final else ws
        return jnp.concatenate(stats, axis=0), columns(jnp.concatenate(factors, axis=0))

    def step_d(b):
        for hf in range(2):
            sum_c(b, hf).wait_recv()
        stat_c(b).wait_recv()
        stats, cols = merge_stats([ml0[b, c, 0:4], ml_c[b, 0:4]], False)
        ml1[b, 0:4, :] = stats
        for hf in range(2):
            rows = pl.ds(hf * 16, 16)
            wa, wb = (cols[:, 2 * hf + j:2 * hf + j + 1].reshape(2, 4, 16, 1) for j in range(2))
            o_full[b, c, :, :, rows, :] = o_full[b, c, :, :, rows, :] * wa + rc_c[b, :, :, rows, :] * wb
        for cp in sum_y(b):
            cp.start()

    def step_e(b):
        for cp in sum_y(b):
            cp.wait_recv()
        stats, cols = merge_stats([ml1[b, 0:4], ml_y[b, 0:4]], False)
        ml2[b, 0:4, :] = stats
        wcol[...] = cols
        cols = wcol[pl.ds(pl.multiple_of(y * 64, 64), 64), :]
        for hf in range(2):
            rows = pl.ds(hf * 16, 16)
            wa, wb = (cols[:, 2 * hf + j:2 * hf + j + 1].reshape(4, 16, 1) for j in range(2))
            o_full[b, c, y, :, rows, :] = o_full[b, c, y, :, rows, :] * wa + rc_y[b, :, rows, :] * wb

        @pl.when(z == 0)
        def _():
            stat_up(b, ml2).start()
            for dest in range(NZ - 1, 0, -1):
                sum_up(b, dest, dest).start()

        @pl.when(z == NZ - 1)
        def _():
            stat_down(b, ml2).start()
            for dest in range(NZ - 1):
                sum_down(b, dest, NZ - 1 - dest).start()

    def relay(b, dests, stats_in, stats_out, arrived, wait, send):
        stats, cols = merge_stats([ml2[b, 0:4], stats_in[b, 0:4]], False)
        stats_out[b, 0:4, :] = stats
        wcol[...] = cols
        for i, dest in enumerate(dests):
            wait(dest)
            cols = wcol[pl.ds(pl.multiple_of(y * 64 + dest * 16, 16), 16), :]
            for hf in range(2):
                rows = pl.ds(hf * 16, 16)
                wa, wb = (cols[:, 2 * hf + j:2 * hf + j + 1] for j in range(2))
                o_full[b, c, y, dest, rows, :] = o_full[b, c, y, dest, rows, :] * wa + arrived[b, dest, rows, :] * wb
            if i == 0:
                send(None)
            send(dest)

    def step_g(hop, b):
        at = NZ - 1 - hop

        @pl.when(z == hop)
        def _():
            def send(dest):
                (stat_up(b, ml_us) if dest is None else sum_up(b, dest, dest - hop)).start()
            stat_up(b, ml2).wait_recv()
            relay(b, range(NZ - 1, hop, -1), ml_u, ml_us, rc_u, lambda dest: sum_up(b, dest, dest - hop + 1).wait_recv(), send)

        @pl.when(z == at)
        def _():
            def send(dest):
                (stat_down(b, ml_ds) if dest is None else sum_down(b, dest, at - dest)).start()
            stat_down(b, ml2).wait_recv()
            relay(b, range(at), ml_d, ml_ds, rc_d, lambda dest: sum_down(b, dest, at - dest + 1).wait_recv(), send)

    def finish(b, at):
        parts, sums = [ml2[b, 0:4]], [o_full.at[b, c, y, at]]
        if at > 0:
            sum_up(b, at, 1).wait_recv()
            if at == NZ - 1:
                stat_up(b, ml2).wait_recv()
            parts.append(ml_u[b, 0:4])
            sums.append(rc_u.at[b, at])
        if at < NZ - 1:
            sum_down(b, at, 1).wait_recv()
            if at == 0:
                stat_down(b, ml2).wait_recv()
            parts.append(ml_d[b, 0:4])
            sums.append(rc_d.at[b, at])
        wcol[...] = merge_stats(parts, True)[1]
        cols = wcol[pl.ds(pl.multiple_of(y * 64 + at * 16, 16), 16), :]
        n = len(parts)
        halves = []
        for hf in range(2):
            rows = pl.ds(hf * 16, 16)
            o = sum(part[rows, :] * cols[:, n * hf + j:n * hf + j + 1] for j, part in enumerate(sums))
            halves.append(o.astype(bf16))
        o = jnp.concatenate(halves, axis=0)
        head = lax.rem(lax.broadcasted_iota(jnp.int32, (32, 128), 0), 8)
        for h in range(8):
            v = jnp.dot(o, wuv[h], preferred_element_type=f32)
            v = jnp.where(head == h, v, 0.0).reshape(4, 8, 128).sum(axis=1)
            out[b, :, h * 128:(h + 1) * 128] = v.astype(bf16)

    def step_f(b):
        for at in range(NZ):
            @pl.when(z == at)
            def _(at=at):
                finish(b, at)

    @pl.loop(0, nb)
    def _(b):
        gather_y(b, y).start()

    steps = ((8, step_e), (6, step_d), (4, step_z4), (5, attend), (3, step_z3), (12, functools.partial(step_g, 2)),
             (2, step_z2), (0, step_z1), (14, step_f), (10, functools.partial(step_g, 1)))

    @pl.loop(0, nb + 14)
    def _(it):
        for lag, fn in steps:
            b = it - lag

            @pl.when((b >= 0) & (b < nb))
            def _(fn=fn, b=b):
                fn(b)

    own_h.wait()

    @pl.loop(0, nb)
    def _(b):
        gather_y(b, y).wait_send()
        gather_c(b, c).wait_send()
        for d in (1, 2, 3):
            @pl.when((z < NZ - 1) & (z - (d - 1) >= 0))
            def _(d=d):
                gather_up(b, z - (d - 1), d).wait_send()

            @pl.when((z > 0) & (z + (d - 1) < NZ))
            def _(d=d):
                gather_down(b, z + (d - 1), d).wait_send()
        sum_c(b, 0).wait_send()
        sum_c(b, 1).wait_send()
        stat_c(b).wait_send()
        for cp in sum_y(b):
            cp.wait_send()
        for at in range(NZ):
            @pl.when(z == at)
            def _(at=at):
                for dest in range(at + 1, NZ):
                    sum_up(b, dest, dest - at).wait_send()
                if at < NZ - 1:
                    stat_up(b, ml2).wait_send()
                for dest in range(at):
                    sum_down(b, dest, at - dest).wait_send()
                if at > 0:
                    stat_down(b, ml2).wait_send()


def attend_all(q, q_rope, lens, c_kv, k_t, hidden, w_uv, score_scale):
    nb, local_len, lat = c_kv.shape
    nq, dim = hidden.shape[1:]
    slots = 3
    dma = pltpu.SemaphoreType.DMA
    return pl.pallas_call(
        functools.partial(attend_kernel, score_scale * math.log2(math.e)),
        out_shape=(jax.ShapeDtypeStruct((nb, nq, w_uv.shape[0] * w_uv.shape[2]), bf16),
                   jax.ShapeDtypeStruct((nb // NZ, nq, dim // 4), bf16)),
        in_specs=[pl.BlockSpec(memory_space=pltpu.SMEM)] + [pl.BlockSpec(memory_space=pl.ANY)] * 5
        + [pl.BlockSpec(memory_space=pltpu.VMEM)],
        out_specs=(pl.BlockSpec(memory_space=pltpu.VMEM), pl.BlockSpec(memory_space=pltpu.VMEM)),
        scratch_shapes=[
            pltpu.VMEM((nb, 2, 2, 4, 9, 16, 128), bf16),
            pltpu.VMEM((slots, local_len, lat), bf16),
            pltpu.VMEM((slots, k_t.shape[1], local_len), bf16),
            pltpu.VMEM((nb, 2, 2, 4, 32, lat), f32),
            pltpu.VMEM((nb, 2, 8, 128), f32),
            pltpu.VMEM((nb, 8, 128), f32),
            pltpu.VMEM((nb, 8, 128), f32),
            pltpu.VMEM((nb, 2, 4, 32, lat), f32),
            pltpu.VMEM((nb, 8, 128), f32),
            pltpu.VMEM((nb, 4, 32, lat), f32),
            pltpu.VMEM((nb, 8, 128), f32),
            pltpu.VMEM((nb, 4, 32, lat), f32),
            pltpu.VMEM((nb, 8, 128), f32),
            pltpu.VMEM((nb, 8, 128), f32),
            pltpu.VMEM((nb, 4, 32, lat), f32),
            pltpu.VMEM((nb, 8, 128), f32),
            pltpu.VMEM((nb, 8, 128), f32),
            pltpu.VMEM((128, 128), f32),
            dma((2,)), dma, dma((slots,)), dma((slots,)),
            dma((nb,)), dma((nb,)), dma((nb, 3)), dma((nb, 3)), dma((nb, 3)), dma((nb, 3)), dma((nb,)), dma((nb,)),
            dma((nb, 2)), dma((nb, 2)), dma((nb,)), dma((nb,)), dma((nb, 3)), dma((nb, 3)), dma((nb, 3)), dma((nb, 3)),
            dma((nb,)), dma((nb,)), dma((nb,)), dma((nb,)), dma((nb,)), dma((nb,)), dma((nb,)), dma((nb,)),
        ],
        compiler_params=pltpu.CompilerParams(
            collective_id=0, has_side_effects=True, vmem_limit_bytes=64 * 1024 * 1024 - 65536),
        name="attend_all",
    )(lens, q, q_rope, c_kv, k_t, hidden, w_uv)


def rope_kernel(h_ref, w_ref, out, flat, rows):
    head = pl.program_id(0)
    nb, nq, _ = h_ref.shape

    @pl.when(head == 0)
    def _():
        flat[...] = h_ref[...].astype(f32).reshape(flat.shape).astype(bf16)

    rows[head] = lax.dot_general(flat[...], w_ref[0], (((1,), (1,)), ((), ())), preferred_element_type=f32)

    @pl.when(head == pl.num_programs(0) - 1)
    def _():
        pairs = jnp.stack([rows[h] for h in range(8)], axis=1).reshape(nb, 2, 16, 64)
        out[...] = jnp.concatenate([pairs[:, 0], pairs[:, 1]], axis=-1).astype(bf16)


def rope_queries(hidden, w_t):
    nb, nq, dim = hidden.shape
    heads, wide = w_t.shape[:2]
    return pl.pallas_call(
        rope_kernel,
        grid=(heads,),
        out_shape=jax.ShapeDtypeStruct((nb, 16, 128), bf16),
        in_specs=[pl.BlockSpec((nb, nq, dim), lambda i: (0, 0, 0)), pl.BlockSpec((1, wide, dim), lambda i: (i, 0, 0))],
        out_specs=pl.BlockSpec((nb, 16, 128), lambda i: (0, 0, 0)),
        scratch_shapes=[pltpu.VMEM((nb * nq, dim), bf16), pltpu.VMEM((heads, nb * nq, wide), f32)],
        compiler_params=pltpu.CompilerParams(dimension_semantics=("arbitrary",)),
        name="rope_queries",
    )(hidden, w_t)


def total_kernel(ov_ref, w_hbm, hbuf, out, ov_rows, wbuf, part, gat, rc_c, rc_y, rc_z,
                 w_sem, sc_s, sc_r, sy_s, sy_r, sz_s, sz_r, gz_s, gz_r, gy_s, gy_r, gc_s, gc_r):
    _, z, y, c = place()
    chunks, lanes = wbuf.shape[0], wbuf.shape[4]
    deep = part.shape[3] // NZ
    core_peer, y_peer = seq_of(z, y, 1 - c), seq_of(z, 1 - y, c)
    zs = [lax.rem(z + d, NZ) for d in (1, 2, 3)]
    zf = [lax.rem(z + NZ - d, NZ) for d in (1, 2, 3)]

    def where(cc, yy, k):
        return pl.ds(pl.multiple_of((cc * NY + yy) * (chunks * lanes) + k * lanes, 128), lanes)

    def weights(k):
        return [pltpu.make_async_copy(w_hbm.at[:, where(cc, yy, k)], wbuf.at[k, cc, yy], w_sem.at[k, cc * 2 + yy])
                for cc in range(2) for yy in range(2)]

    for k in range(chunks):
        for cp in weights(k):
            cp.start()
    nb = ov_ref.shape[0]
    ov_rows[...] = ov_ref[...].astype(f32).reshape(ov_rows.shape).astype(bf16)
    meet([core_peer, y_peer] + [seq_of(p, y, c) for p in zs])

    def band(at):
        return pl.ds(pl.multiple_of(at * deep, deep), deep)

    def sum_c(k):
        return remote(part.at[k, 1 - c], rc_c.at[k], sc_s.at[k], sc_r.at[k], core_peer)

    def sum_y(k):
        return remote(part.at[k, c, 1 - y], rc_y.at[k], sy_s.at[k], sy_r.at[k], y_peer)

    def sum_z(k, d):
        return remote(part.at[k, c, y, band(zs[d])], rc_z.at[k, d], sz_s.at[k, d], sz_r.at[k, d], seq_of(zs[d], y, c))

    def give_z(k, d, at):
        piece = gat.at[k, c, y, band(at)]
        return remote(piece, piece, gz_s.at[k, d], gz_r.at[k, d], seq_of(zs[d], y, c))

    def give_y(k, yy):
        return remote(gat.at[k, c, yy], gat.at[k, c, yy], gy_s.at[k], gy_r.at[k], y_peer)

    def give_c(k, cc):
        return remote(gat.at[k, cc], gat.at[k, cc], gc_s.at[k], gc_r.at[k], core_peer)

    def multiply(k):
        for cp in weights(k):
            cp.wait()
        ov = ov_rows[...]
        for cc in (1 - c, c):
            for yy in range(2):
                part[k, cc, yy] = jnp.dot(ov, wbuf[k, cc, yy], preferred_element_type=f32)
            if cc is not c:
                sum_c(k).start()

    def step_d(k):
        sum_c(k).wait_recv()
        part[k, c] = part[k, c] + rc_c[k]
        sum_y(k).start()

    def step_e(k):
        sum_y(k).wait_recv()
        part[k, c, y] = part[k, c, y] + rc_y[k]
        for d in range(3):
            sum_z(k, d).start()

    def step_f(k):
        for d in range(3):
            sum_z(k, d).wait_recv()
        total = part[k, c, y, band(z)] + rc_z[k, 0] + rc_z[k, 1] + rc_z[k, 2]
        own = hbuf[:, :, pl.ds(pl.multiple_of(k * lanes, 128), lanes)].astype(f32).reshape(deep, lanes)
        gat[k, c, y, band(z)] = (own + total).astype(bf16)
        for d in range(3):
            give_z(k, d, z).start()

    def step_h(k):
        for d in range(3):
            give_z(k, d, zf[d]).wait_recv()
        give_y(k, y).start()

    def step_i(k):
        give_y(k, 1 - y).wait_recv()
        give_c(k, c).start()

    def step_j(k):
        give_c(k, 1 - c).wait_recv()
        for cc in range(2):
            for yy in range(2):
                out[:, :, where(cc, yy, k)] = gat[k, cc, yy].astype(f32).reshape(nb, -1, lanes).astype(bf16)

    steps = ((10, step_j), (9, step_i), (7, step_h), (5, step_f), (3, step_e), (1, step_d), (0, multiply))

    @pl.loop(0, chunks + 10)
    def _(it):
        for lag, fn in steps:
            k = it - lag

            @pl.when((k >= 0) & (k < chunks))
            def _(fn=fn, k=k):
                fn(k)

    @pl.loop(0, chunks)
    def _(k):
        sum_c(k).wait_send()
        sum_y(k).wait_send()
        for d in range(3):
            sum_z(k, d).wait_send()
            give_z(k, d, z).wait_send()
        give_y(k, y).wait_send()
        give_c(k, c).wait_send()


def total_all(ov, w_o, own_h):
    (nb, nq, _), dim = ov.shape, w_o.shape[1]
    n = nb * nq
    chunks = next(k for k in (7, 1) if dim % (4 * k * 128) == 0)
    lanes = dim // (4 * chunks)
    dma = pltpu.SemaphoreType.DMA
    vm, hbm = pl.BlockSpec(memory_space=pltpu.VMEM), pl.BlockSpec(memory_space=pl.ANY)
    one, three = dma((chunks,)), dma((chunks, 3))
    return pl.pallas_call(
        total_kernel,
        out_shape=jax.ShapeDtypeStruct((nb, nq, dim), bf16),
        in_specs=[vm, hbm, vm],
        out_specs=vm,
        scratch_shapes=[
            pltpu.VMEM((n, w_o.shape[0]), bf16),
            pltpu.VMEM((chunks, 2, 2, w_o.shape[0], lanes), bf16),
            pltpu.VMEM((chunks, 2, 2, n, lanes), f32),
            pltpu.VMEM((chunks, 2, 2, n, lanes), bf16),
            pltpu.VMEM((chunks, 2, n, lanes), f32),
            pltpu.VMEM((chunks, n, lanes), f32),
            pltpu.VMEM((chunks, 3, n // NZ, lanes), f32),
            dma((chunks, 4)), one, one, one, one, three, three, three, three, one, one, one, one,
        ],
        compiler_params=pltpu.CompilerParams(
            collective_id=1, has_side_effects=True, vmem_limit_bytes=40 * 1024 * 1024),
        name="total_all",
    )(ov, w_o, own_h)


def solution(mesh):
    def local_step(hidden, cache_lens, c_kv, k_r, w_uq, w_qr, w_uk, w_uv, w_o):
        score_scale = (w_uq.shape[2] + w_qr.shape[2]) ** -0.5
        nb, nq, dim = hidden.shape
        nh, lat = w_uk.shape[0], w_uk.shape[2]
        q_nope = jnp.einsum("cre,eil->cril", hidden, w_uq, preferred_element_type=f32).astype(bf16)
        q_lat = jnp.einsum("bqhk,hkc->bqhc", q_nope, w_uk, preferred_element_type=f32).astype(bf16)
        q = q_lat.reshape(nb, 2, 16, 4, 128).transpose(0, 1, 3, 2, 4).reshape(nb, 8, 16, 128)
        q_rope = rope_queries(hidden, w_qr.transpose(1, 2, 0))
        o_val, own_h = attend_all(q, q_rope, cache_lens, c_kv, jnp.swapaxes(k_r, 1, 2), hidden, w_uv, score_scale)
        return total_all(o_val, w_o.reshape(-1, dim), own_h)

    specs_in = (P("batch", None, None), P("batch"), P("batch", "seq", None), P("batch", "seq", None),
                P(None, "seq", None), P(None, "seq", None), P("seq", None, None), P("seq", None, None),
                P("seq", None, None))
    return jax.shard_map(local_step, mesh=mesh, in_specs=specs_in, out_specs=P("batch", None, None), check_vma=False)
```

```python
import functools
import math

import jax
import jax.numpy as jnp
from jax import lax
from jax.experimental import pallas as pl
from jax.experimental.pallas import tpu as pltpu
from jax.sharding import PartitionSpec as P

MASK_FILL = -1e30
ATTEND_VMEM = 46 * 1024 * 1024
NZ, NY, NC = 4, 2, 2
MESH = pl.DeviceIdType.MESH
f32, bf16 = jnp.float32, jnp.bfloat16


def place():
    s = lax.axis_index("seq")
    return s, s // (NY * NC), (s // NC) % NY, s % NC


def seq_of(z, y, c):
    return (z * NY + y) * NC + c


def remote(src, dst, send_sem, recv_sem, seq):
    return pltpu.make_async_remote_copy(
        src_ref=src, dst_ref=dst, send_sem=send_sem, recv_sem=recv_sem,
        device_id={"seq": seq}, device_id_type=MESH)


def meet(peers):
    barrier = pltpu.get_barrier_semaphore()
    for p in peers:
        pl.semaphore_signal(barrier, inc=1, device_id={"seq": p}, device_id_type=MESH)
    pl.semaphore_wait(barrier, len(peers))


def columns(rows):
    pad = jnp.zeros((128 - rows.shape[0], 128), f32)
    return jnp.concatenate([rows, pad], axis=0).T


def attend_kernel(scale, lens, q_hbm, r_hbm, c_hbm, k_hbm, h_hbm, w_hbm, wuv, out, h_out, w_out,
                  qbuf, ck, kr, o_full, ml0, ml1, ml2, rc_c, ml_c, rc_y, ml_y,
                  rc_u, ml_u, ml_us, rc_d, ml_d, ml_ds, wcol,
                  q_sem, h_sem, w_sem, c_sem, k_sem,
                  ay_s, ay_r, au_s, au_r, ad_s, ad_r, ac_s, ac_r,
                  oc_s, oc_r, oy_s, oy_r, ou_s, ou_r, od_s, od_r,
                  mc_s, mc_r, my_s, my_r, mu_s, mu_r, md_s, md_r):
    nb, slots, ring = q_hbm.shape[0], ck.shape[0], rc_c.shape[0]
    local_len = ck.shape[1]
    s, z, y, c = place()
    core_peer, y_peer = seq_of(z, y, 1 - c), seq_of(z, 1 - y, c)
    upper, lower = seq_of(lax.rem(z + 1, NZ), y, c), seq_of(lax.rem(z + NZ - 1, NZ), y, c)

    own_q = (pltpu.make_async_copy(q_hbm, qbuf.at[:, c, y, z, pl.ds(0, 8)], q_sem.at[0]),
             pltpu.make_async_copy(r_hbm, qbuf.at[:, c, y, z, 8], q_sem.at[1]))
    for cp in own_q:
        cp.start()

    def cache(b):
        k = lax.rem(b, slots)
        return (pltpu.make_async_copy(c_hbm.at[b], ck.at[k], c_sem.at[k]),
                pltpu.make_async_copy(k_hbm.at[b], kr.at[k], k_sem.at[k]))

    for b in range(slots - 1):
        for cp in cache(b):
            cp.start()

    deep, wide = h_out.shape[0], h_out.shape[2]
    own_h = pltpu.make_async_copy(
        h_hbm.at[pl.ds(z * deep, deep), :, pl.ds(pl.multiple_of((c * NY + y) * wide, 128), wide)], h_out, h_sem)
    own_h.start()
    own_w = pltpu.make_async_copy(w_hbm, w_out, w_sem)
    own_w.start()
    meet([core_peer, y_peer, upper, lower])
    for cp in own_q:
        cp.wait()

    def gather_y(b, yy):
        part = qbuf.at[b, c, yy, z]
        return remote(part, part, ay_s.at[b], ay_r.at[b], y_peer)

    def gather_up(b, origin, d):
        part = qbuf.at[b, c, :, origin]
        return remote(part, part, au_s.at[b, d - 1], au_r.at[b, d - 1], upper)

    def gather_down(b, origin, d):
        part = qbuf.at[b, c, :, origin]
        return remote(part, part, ad_s.at[b, d - 1], ad_r.at[b, d - 1], lower)

    def gather_c(b, cc):
        part = qbuf.at[b, cc]
        return remote(part, part, ac_s.at[b], ac_r.at[b], core_peer)

    def sum_c(b, hf):
        rows = pl.ds(hf * 16, 16)
        return remote(o_full.at[b, 1 - c, :, :, rows], rc_c.at[lax.rem(b, ring), :, :, rows], oc_s.at[b, hf], oc_r.at[b, hf], core_peer)

    def stat_c(b):
        return remote(ml0.at[b, 1 - c], ml_c.at[b], mc_s.at[b], mc_r.at[b], core_peer)

    def sum_y(b):
        return (remote(o_full.at[b, c, 1 - y], rc_y.at[lax.rem(b, ring)], oy_s.at[b], oy_r.at[b], y_peer),
                remote(ml1.at[b], ml_y.at[b], my_s.at[b], my_r.at[b], y_peer))

    def sum_up(b, dest, d):
        return remote(o_full.at[b, c, y, dest], rc_u.at[b, dest], ou_s.at[b, d - 1], ou_r.at[b, d - 1], upper)

    def stat_up(b, stat):
        return remote(stat.at[b], ml_u.at[b], mu_s.at[b], mu_r.at[b], upper)

    def sum_down(b, dest, d):
        return remote(o_full.at[b, c, y, dest], rc_d.at[b, dest], od_s.at[b, d - 1], od_r.at[b, d - 1], lower)

    def stat_down(b, stat):
        return remote(stat.at[b], ml_d.at[b], md_s.at[b], md_r.at[b], lower)

    def pass_on(b, d):
        @pl.when((z < NZ - 1) & (z - (d - 1) >= 0))
        def _():
            gather_up(b, z - (d - 1), d).start()

        @pl.when((z > 0) & (z + (d - 1) < NZ))
        def _():
            gather_down(b, z + (d - 1), d).start()

    def arrive(b, d):
        @pl.when(z - d >= 0)
        def _():
            gather_up(b, z - d, d).wait_recv()

        @pl.when(z + d < NZ)
        def _():
            gather_down(b, z + d, d).wait_recv()

    def step_z1(b):
        gather_y(b, 1 - y).wait_recv()
        pass_on(b, 1)

    def step_z2(b):
        arrive(b, 1)
        pass_on(b, 2)

    def step_z3(b):
        arrive(b, 2)
        pass_on(b, 3)

    def step_z4(b):
        arrive(b, 3)
        gather_c(b, c).start()

    def attend(b):
        gather_c(b, 1 - c).wait_recv()
        for cp in cache(b):
            cp.wait()

        @pl.when(b + slots - 1 < nb)
        def _():
            for cp in cache(b + slots - 1):
                cp.start()

        k = lax.rem(b, slots)
        row_len = lens[b]
        pos = s * local_len + lax.broadcasted_iota(jnp.int32, (512, local_len), 1)
        row = lax.broadcasted_iota(jnp.int32, (512, 1), 0)
        token = (row // 256) * 2 + lax.rem(row, 16) // 8
        lane = lax.broadcasted_iota(jnp.int32, (512, 128), 1)
        q = jnp.concatenate(
            [jnp.concatenate([qbuf[b, :, :, :, hf * 4 + j].reshape(256, 128) for j in range(4)], axis=1) for hf in range(2)], axis=0)
        both = qbuf[b, :, :, :, 8].reshape(256, 128)
        qr = jnp.concatenate([both[:, :64], both[:, 64:]], axis=0)
        sc = lax.dot_general(q, ck[k], (((1,), (1,)), ((), ())), preferred_element_type=f32)
        sc = sc + jnp.dot(qr, kr[k], preferred_element_type=f32)
        sc = jnp.where(pos <= row_len + token, sc, MASK_FILL)
        m = jnp.max(sc, axis=1, keepdims=True)
        p = jnp.exp2((sc - m) * scale)
        l = jnp.sum(p, axis=1, keepdims=True)
        o = jnp.dot(p.astype(bf16), ck[k], preferred_element_type=f32)
        stat = jnp.where(lane == 0, m * scale, jnp.where(lane == 1, l, 0.0)).T
        for hf in range(2):
            o_full[b, :, :, :, hf * 16:(hf + 1) * 16, :] = o[hf * 256:(hf + 1) * 256].reshape(2, 2, 4, 16, o.shape[1])
            for cc in range(2):
                at = hf * 256 + cc * 128
                ml0[b, cc, hf * 2:hf * 2 + 2, :] = stat[0:2, at:at + 128]
            sum_c(b, hf).start()
        stat_c(b).start()

    def merge_stats(parts, final):
        stats, factors = [], []
        for hf in range(2):
            ms, ls = [p[2 * hf:2 * hf + 1] for p in parts], [p[2 * hf + 1:2 * hf + 2] for p in parts]
            top = functools.reduce(jnp.maximum, ms)
            ws = [jnp.exp2(m - top) for m in ms]
            total = sum(w * l for w, l in zip(ws, ls))
            stats += [top, total]
            factors += [w / total for w in ws] if final else ws
        return jnp.concatenate(stats, axis=0), columns(jnp.concatenate(factors, axis=0))

    def step_d(b):
        for hf in range(2):
            sum_c(b, hf).wait_recv()
        stat_c(b).wait_recv()
        stats, cols = merge_stats([ml0[b, c, 0:4], ml_c[b, 0:4]], False)
        ml1[b, 0:4, :] = stats
        for hf in range(2):
            rows = pl.ds(hf * 16, 16)
            wa, wb = (cols[:, 2 * hf + j:2 * hf + j + 1].reshape(2, 4, 16, 1) for j in range(2))
            o_full[b, c, :, :, rows, :] = o_full[b, c, :, :, rows, :] * wa + rc_c[lax.rem(b, ring), :, :, rows, :] * wb
        for cp in sum_y(b):
            cp.start()

    def step_e(b):
        for cp in sum_y(b):
            cp.wait_recv()
        stats, cols = merge_stats([ml1[b, 0:4], ml_y[b, 0:4]], False)
        ml2[b, 0:4, :] = stats
        wcol[...] = cols
        cols = wcol[pl.ds(pl.multiple_of(y * 64, 64), 64), :]
        for hf in range(2):
            rows = pl.ds(hf * 16, 16)
            wa, wb = (cols[:, 2 * hf + j:2 * hf + j + 1].reshape(4, 16, 1) for j in range(2))
            o_full[b, c, y, :, rows, :] = o_full[b, c, y, :, rows, :] * wa + rc_y[lax.rem(b, ring), :, rows, :] * wb

        @pl.when(z == 0)
        def _():
            stat_up(b, ml2).start()
            for dest in range(NZ - 1, 0, -1):
                sum_up(b, dest, dest).start()

        @pl.when(z == NZ - 1)
        def _():
            stat_down(b, ml2).start()
            for dest in range(NZ - 1):
                sum_down(b, dest, NZ - 1 - dest).start()

    def relay(b, dests, stats_in, stats_out, arrived, wait, send):
        stats, cols = merge_stats([ml2[b, 0:4], stats_in[b, 0:4]], False)
        stats_out[b, 0:4, :] = stats
        wcol[...] = cols
        for i, dest in enumerate(dests):
            wait(dest)
            cols = wcol[pl.ds(pl.multiple_of(y * 64 + dest * 16, 16), 16), :]
            for hf in range(2):
                rows = pl.ds(hf * 16, 16)
                wa, wb = (cols[:, 2 * hf + j:2 * hf + j + 1] for j in range(2))
                o_full[b, c, y, dest, rows, :] = o_full[b, c, y, dest, rows, :] * wa + arrived[b, dest, rows, :] * wb
            if i == 0:
                send(None)
            send(dest)

    def step_g(hop, b):
        at = NZ - 1 - hop

        @pl.when(z == hop)
        def _():
            def send(dest):
                (stat_up(b, ml_us) if dest is None else sum_up(b, dest, dest - hop)).start()
            stat_up(b, ml2).wait_recv()
            relay(b, range(NZ - 1, hop, -1), ml_u, ml_us, rc_u, lambda dest: sum_up(b, dest, dest - hop + 1).wait_recv(), send)

        @pl.when(z == at)
        def _():
            def send(dest):
                (stat_down(b, ml_ds) if dest is None else sum_down(b, dest, at - dest)).start()
            stat_down(b, ml2).wait_recv()
            relay(b, range(at), ml_d, ml_ds, rc_d, lambda dest: sum_down(b, dest, at - dest + 1).wait_recv(), send)

    def finish(b, at):
        parts, sums = [ml2[b, 0:4]], [o_full.at[b, c, y, at]]
        if at > 0:
            sum_up(b, at, 1).wait_recv()
            if at == NZ - 1:
                stat_up(b, ml2).wait_recv()
            parts.append(ml_u[b, 0:4])
            sums.append(rc_u.at[b, at])
        if at < NZ - 1:
            sum_down(b, at, 1).wait_recv()
            if at == 0:
                stat_down(b, ml2).wait_recv()
            parts.append(ml_d[b, 0:4])
            sums.append(rc_d.at[b, at])
        wcol[...] = merge_stats(parts, True)[1]
        cols = wcol[pl.ds(pl.multiple_of(y * 64 + at * 16, 16), 16), :]
        n = len(parts)
        halves = []
        for hf in range(2):
            rows = pl.ds(hf * 16, 16)
            o = sum(part[rows, :] * cols[:, n * hf + j:n * hf + j + 1] for j, part in enumerate(sums))
            halves.append(o.astype(bf16))
        o = jnp.concatenate(halves, axis=0)
        head = lax.rem(lax.broadcasted_iota(jnp.int32, (32, 128), 0), 8)
        for h in range(8):
            v = jnp.dot(o, wuv[h], preferred_element_type=f32)
            v = jnp.where(head == h, v, 0.0).reshape(4, 8, 128).sum(axis=1)
            out[b, :, h * 128:(h + 1) * 128] = v.astype(bf16)

    def step_f(b):
        for at in range(NZ):
            @pl.when(z == at)
            def _(at=at):
                finish(b, at)

    @pl.loop(0, nb)
    def _(b):
        gather_y(b, y).start()

    steps = ((8, step_e), (6, step_d), (4, step_z4), (5, attend), (3, step_z3), (12, functools.partial(step_g, 2)),
             (2, step_z2), (0, step_z1), (14, step_f), (10, functools.partial(step_g, 1)))

    @pl.loop(0, nb + 14)
    def _(it):
        for lag, fn in steps:
            b = it - lag

            @pl.when((b >= 0) & (b < nb))
            def _(fn=fn, b=b):
                fn(b)

    own_h.wait()
    own_w.wait()

    @pl.loop(0, nb)
    def _(b):
        gather_y(b, y).wait_send()
        gather_c(b, c).wait_send()
        for d in (1, 2, 3):
            @pl.when((z < NZ - 1) & (z - (d - 1) >= 0))
            def _(d=d):
                gather_up(b, z - (d - 1), d).wait_send()

            @pl.when((z > 0) & (z + (d - 1) < NZ))
            def _(d=d):
                gather_down(b, z + (d - 1), d).wait_send()
        sum_c(b, 0).wait_send()
        sum_c(b, 1).wait_send()
        stat_c(b).wait_send()
        for cp in sum_y(b):
            cp.wait_send()
        for at in range(NZ):
            @pl.when(z == at)
            def _(at=at):
                for dest in range(at + 1, NZ):
                    sum_up(b, dest, dest - at).wait_send()
                if at < NZ - 1:
                    stat_up(b, ml2).wait_send()
                for dest in range(at):
                    sum_down(b, dest, at - dest).wait_send()
                if at > 0:
                    stat_down(b, ml2).wait_send()


def attend_all(q, q_rope, lens, c_kv, k_t, hidden, w_o, w_uv, score_scale):
    nb, local_len, lat = c_kv.shape
    nq, dim = hidden.shape[1:]
    slots = 3
    dma = pltpu.SemaphoreType.DMA
    return pl.pallas_call(
        functools.partial(attend_kernel, score_scale * math.log2(math.e)),
        out_shape=(pltpu.VMEM((nb, nq, w_uv.shape[0] * w_uv.shape[2]), bf16),
                   pltpu.VMEM((nb // NZ, nq, dim // 4), bf16),
                   pltpu.VMEM(w_o.shape, bf16)),
        in_specs=[pl.BlockSpec(memory_space=pltpu.SMEM)] + [pl.BlockSpec(memory_space=pl.ANY)] * 6
        + [pl.BlockSpec(memory_space=pltpu.VMEM)],
        out_specs=(pl.BlockSpec(memory_space=pltpu.VMEM), pl.BlockSpec(memory_space=pltpu.VMEM),
                   pl.BlockSpec(memory_space=pl.ANY)),
        scratch_shapes=[
            pltpu.VMEM((nb, 2, 2, 4, 9, 16, 128), bf16),
            pltpu.VMEM((slots, local_len, lat), bf16),
            pltpu.VMEM((slots, k_t.shape[1], local_len), bf16),
            pltpu.VMEM((nb, 2, 2, 4, 32, lat), f32),
            pltpu.VMEM((nb, 2, 8, 128), f32),
            pltpu.VMEM((nb, 8, 128), f32),
            pltpu.VMEM((nb, 8, 128), f32),
            pltpu.VMEM((4, 2, 4, 32, lat), f32),
            pltpu.VMEM((nb, 8, 128), f32),
            pltpu.VMEM((4, 4, 32, lat), f32),
            pltpu.VMEM((nb, 8, 128), f32),
            pltpu.VMEM((nb, 4, 32, lat), f32),
            pltpu.VMEM((nb, 8, 128), f32),
            pltpu.VMEM((nb, 8, 128), f32),
            pltpu.VMEM((nb, 4, 32, lat), f32),
            pltpu.VMEM((nb, 8, 128), f32),
            pltpu.VMEM((nb, 8, 128), f32),
            pltpu.VMEM((128, 128), f32),
            dma((2,)), dma, dma, dma((slots,)), dma((slots,)),
            dma((nb,)), dma((nb,)), dma((nb, 3)), dma((nb, 3)), dma((nb, 3)), dma((nb, 3)), dma((nb,)), dma((nb,)),
            dma((nb, 2)), dma((nb, 2)), dma((nb,)), dma((nb,)), dma((nb, 3)), dma((nb, 3)), dma((nb, 3)), dma((nb, 3)),
            dma((nb,)), dma((nb,)), dma((nb,)), dma((nb,)), dma((nb,)), dma((nb,)), dma((nb,)), dma((nb,)),
        ],
        compiler_params=pltpu.CompilerParams(
            collective_id=0, has_side_effects=True, vmem_limit_bytes=ATTEND_VMEM),
        name="attend_all",
    )(lens, q, q_rope, c_kv, k_t, hidden, w_o, w_uv)


def rope_kernel(h_ref, w_ref, out, flat, rows):
    head = pl.program_id(0)
    nb, nq, _ = h_ref.shape

    @pl.when(head == 0)
    def _():
        flat[...] = h_ref[...].astype(f32).reshape(flat.shape).astype(bf16)

    rows[head] = lax.dot_general(flat[...], w_ref[0], (((1,), (1,)), ((), ())), preferred_element_type=f32)

    @pl.when(head == pl.num_programs(0) - 1)
    def _():
        pairs = jnp.stack([rows[h] for h in range(8)], axis=1).reshape(nb, 2, 16, 64)
        out[...] = jnp.concatenate([pairs[:, 0], pairs[:, 1]], axis=-1).astype(bf16)


def rope_queries(hidden, w_t):
    nb, nq, dim = hidden.shape
    heads, wide = w_t.shape[:2]
    return pl.pallas_call(
        rope_kernel,
        grid=(heads,),
        out_shape=jax.ShapeDtypeStruct((nb, 16, 128), bf16),
        in_specs=[pl.BlockSpec((nb, nq, dim), lambda i: (0, 0, 0)), pl.BlockSpec((1, wide, dim), lambda i: (i, 0, 0))],
        out_specs=pl.BlockSpec((nb, 16, 128), lambda i: (0, 0, 0)),
        scratch_shapes=[pltpu.VMEM((nb * nq, dim), bf16), pltpu.VMEM((heads, nb * nq, wide), f32)],
        compiler_params=pltpu.CompilerParams(dimension_semantics=("arbitrary",)),
        name="rope_queries",
    )(hidden, w_t)


def total_kernel(ov_ref, w_ref, hbuf, out, ov_rows, part, gat, rc_c, rc_y, rc_z,
                 sc_s, sc_r, sy_s, sy_r, sz_s, sz_r, gz_s, gz_r, gy_s, gy_r, gc_s, gc_r):
    _, z, y, c = place()
    chunks, lanes = part.shape[0], part.shape[4]
    deep = part.shape[3] // NZ
    core_peer, y_peer = seq_of(z, y, 1 - c), seq_of(z, 1 - y, c)
    zs = [lax.rem(z + d, NZ) for d in (1, 2, 3)]
    zf = [lax.rem(z + NZ - d, NZ) for d in (1, 2, 3)]

    def where(cc, yy, k):
        return pl.ds(pl.multiple_of((cc * NY + yy) * (chunks * lanes) + k * lanes, 128), lanes)

    nb = ov_ref.shape[0]
    ov_rows[...] = ov_ref[...].astype(f32).reshape(ov_rows.shape).astype(bf16)
    meet([core_peer, y_peer] + [seq_of(p, y, c) for p in zs])

    def band(at):
        return pl.ds(pl.multiple_of(at * deep, deep), deep)

    def sum_c(k):
        return remote(part.at[k, 1 - c], rc_c.at[k], sc_s.at[k], sc_r.at[k], core_peer)

    def sum_y(k):
        return remote(part.at[k, c, 1 - y], rc_y.at[k], sy_s.at[k], sy_r.at[k], y_peer)

    def sum_z(k, d):
        return remote(part.at[k, c, y, band(zs[d])], rc_z.at[k, d], sz_s.at[k, d], sz_r.at[k, d], seq_of(zs[d], y, c))

    def give_z(k, d, at):
        piece = gat.at[k, c, y, band(at)]
        return remote(piece, piece, gz_s.at[k, d], gz_r.at[k, d], seq_of(zs[d], y, c))

    def give_y(k, yy):
        return remote(gat.at[k, c, yy], gat.at[k, c, yy], gy_s.at[k], gy_r.at[k], y_peer)

    def give_c(k, cc):
        return remote(gat.at[k, cc], gat.at[k, cc], gc_s.at[k], gc_r.at[k], core_peer)

    def multiply(k):
        ov = ov_rows[...]
        for cc in (1 - c, c):
            for yy in range(2):
                part[k, cc, yy] = jnp.dot(ov, w_ref[:, where(cc, yy, k)], preferred_element_type=f32)
            if cc is not c:
                sum_c(k).start()

    def step_d(k):
        sum_c(k).wait_recv()
        part[k, c] = part[k, c] + rc_c[k]
        sum_y(k).start()

    def step_e(k):
        sum_y(k).wait_recv()
        part[k, c, y] = part[k, c, y] + rc_y[k]
        for d in range(3):
            sum_z(k, d).start()

    def step_f(k):
        for d in range(3):
            sum_z(k, d).wait_recv()
        total = part[k, c, y, band(z)] + rc_z[k, 0] + rc_z[k, 1] + rc_z[k, 2]
        own = hbuf[:, :, pl.ds(pl.multiple_of(k * lanes, 128), lanes)].astype(f32).reshape(deep, lanes)
        gat[k, c, y, band(z)] = (own + total).astype(bf16)
        for d in range(3):
            give_z(k, d, z).start()

    def step_h(k):
        for d in range(3):
            give_z(k, d, zf[d]).wait_recv()
        give_y(k, y).start()

    def step_i(k):
        give_y(k, 1 - y).wait_recv()
        give_c(k, c).start()

    def step_j(k):
        give_c(k, 1 - c).wait_recv()
        for cc in range(2):
            for yy in range(2):
                out[:, :, where(cc, yy, k)] = gat[k, cc, yy].astype(f32).reshape(nb, -1, lanes).astype(bf16)

    steps = ((10, step_j), (9, step_i), (7, step_h), (5, step_f), (3, step_e), (1, step_d), (0, multiply))

    @pl.loop(0, chunks + 10)
    def _(it):
        for lag, fn in steps:
            k = it - lag

            @pl.when((k >= 0) & (k < chunks))
            def _(fn=fn, k=k):
                fn(k)

    @pl.loop(0, chunks)
    def _(k):
        sum_c(k).wait_send()
        sum_y(k).wait_send()
        for d in range(3):
            sum_z(k, d).wait_send()
            give_z(k, d, z).wait_send()
        give_y(k, y).wait_send()
        give_c(k, c).wait_send()


def total_all(ov, w_o, own_h):
    (nb, nq, _), dim = ov.shape, w_o.shape[1]
    n = nb * nq
    chunks = next(k for k in (7, 1) if dim % (4 * k * 128) == 0)
    lanes = dim // (4 * chunks)
    dma = pltpu.SemaphoreType.DMA
    vm = pl.BlockSpec(memory_space=pltpu.VMEM)
    one, three = dma((chunks,)), dma((chunks, 3))
    return pl.pallas_call(
        total_kernel,
        out_shape=pltpu.VMEM((nb, nq, dim), bf16),
        in_specs=[vm, vm, vm],
        out_specs=vm,
        scratch_shapes=[
            pltpu.VMEM((n, w_o.shape[0]), bf16),
            pltpu.VMEM((chunks, 2, 2, n, lanes), f32),
            pltpu.VMEM((chunks, 2, 2, n, lanes), bf16),
            pltpu.VMEM((chunks, 2, n, lanes), f32),
            pltpu.VMEM((chunks, n, lanes), f32),
            pltpu.VMEM((chunks, 3, n // NZ, lanes), f32),
            one, one, one, one, three, three, three, three, one, one, one, one,
        ],
        compiler_params=pltpu.CompilerParams(
            collective_id=1, has_side_effects=True, vmem_limit_bytes=24 * 1024 * 1024),
        name="total_all",
    )(ov, w_o, own_h)


def solution(mesh):
    def local_step(hidden, cache_lens, c_kv, k_r, w_uq, w_qr, w_uk, w_uv, w_o):
        score_scale = (w_uq.shape[2] + w_qr.shape[2]) ** -0.5
        nb, nq, dim = hidden.shape
        nh, lat = w_uk.shape[0], w_uk.shape[2]
        q_nope = jnp.einsum("cre,eil->cril", hidden, w_uq, preferred_element_type=f32).astype(bf16)
        q_lat = jnp.einsum("bqhk,hkc->bqhc", q_nope, w_uk, preferred_element_type=f32).astype(bf16)
        q = q_lat.reshape(nb, 2, 16, 4, 128).transpose(0, 1, 3, 2, 4).reshape(nb, 8, 16, 128)
        q_rope = rope_queries(hidden, w_qr.transpose(1, 2, 0))
        o_val, own_h, own_w = attend_all(q, q_rope, cache_lens, c_kv, jnp.swapaxes(k_r, 1, 2), hidden, w_o.reshape(-1, dim), w_uv, score_scale)
        return total_all(*(pltpu.with_memory_space_constraint(v, pltpu.VMEM) for v in (o_val, own_w, own_h)))

    specs_in = (P("batch", None, None), P("batch"), P("batch", "seq", None), P("batch", "seq", None),
                P(None, "seq", None), P(None, "seq", None), P("seq", None, None), P("seq", None, None),
                P("seq", None, None))
    return jax.shard_map(local_step, mesh=mesh, in_specs=specs_in, out_specs=P("batch", None, None), check_vma=False)
```

```python
import functools
import math

import jax
import jax.numpy as jnp
from jax import lax
from jax.experimental import pallas as pl
from jax.experimental.pallas import tpu as pltpu
from jax.sharding import PartitionSpec as P

MASK_FILL = -1e30
ATTEND_VMEM = 46 * 1024 * 1024
NZ, NY, NC = 4, 2, 2
MESH = pl.DeviceIdType.MESH
f32, bf16 = jnp.float32, jnp.bfloat16


def place():
    s = lax.axis_index("seq")
    return s, s // (NY * NC), (s // NC) % NY, s % NC


def seq_of(z, y, c):
    return (z * NY + y) * NC + c


def remote(src, dst, send_sem, recv_sem, seq):
    return pltpu.make_async_remote_copy(
        src_ref=src, dst_ref=dst, send_sem=send_sem, recv_sem=recv_sem,
        device_id={"seq": seq}, device_id_type=MESH)


def meet(peers):
    barrier = pltpu.get_barrier_semaphore()
    for p in peers:
        pl.semaphore_signal(barrier, inc=1, device_id={"seq": p}, device_id_type=MESH)
    pl.semaphore_wait(barrier, len(peers))


def columns(rows):
    pad = jnp.zeros((128 - rows.shape[0], 128), f32)
    return jnp.concatenate([rows, pad], axis=0).T


def attend_kernel(scale, lens, q_hbm, r_hbm, c_hbm, k_hbm, h_hbm, w_hbm, wuv, out, h_out, w_out,
                  qbuf, ck, kr, o_full, ml0, ml1, ml2, rc_c, ml_c, rc_y, ml_y,
                  rc_u, ml_u, ml_us, rc_d, ml_d, ml_ds, wcol,
                  q_sem, h_sem, w_sem, c_sem, k_sem,
                  ay_s, ay_r, au_s, au_r, ad_s, ad_r, ac_s, ac_r,
                  oc_s, oc_r, oy_s, oy_r, ou_s, ou_r, od_s, od_r,
                  mc_s, mc_r, my_s, my_r, mu_s, mu_r, md_s, md_r):
    nb, slots, ring = q_hbm.shape[0], ck.shape[0], rc_c.shape[0]
    local_len = ck.shape[1]
    s, z, y, c = place()
    core_peer, y_peer = seq_of(z, y, 1 - c), seq_of(z, 1 - y, c)
    upper, lower = seq_of(lax.rem(z + 1, NZ), y, c), seq_of(lax.rem(z + NZ - 1, NZ), y, c)

    own_q = (pltpu.make_async_copy(q_hbm, qbuf.at[:, c, y, z, pl.ds(0, 8)], q_sem.at[0]),
             pltpu.make_async_copy(r_hbm, qbuf.at[:, c, y, z, 8], q_sem.at[1]))
    for cp in own_q:
        cp.start()

    def cache(b):
        k = lax.rem(b, slots)
        return (pltpu.make_async_copy(c_hbm.at[b], ck.at[k], c_sem.at[k]),
                pltpu.make_async_copy(k_hbm.at[b], kr.at[k], k_sem.at[k]))

    for b in range(slots - 1):
        for cp in cache(b):
            cp.start()

    deep, wide = h_out.shape[0], h_out.shape[2]
    own_h = pltpu.make_async_copy(
        h_hbm.at[pl.ds(z * deep, deep), :, pl.ds(pl.multiple_of((c * NY + y) * wide, 128), wide)], h_out, h_sem)
    own_h.start()
    own_w = pltpu.make_async_copy(w_hbm, w_out, w_sem)
    own_w.start()
    meet([core_peer, y_peer, upper, lower])
    for cp in own_q:
        cp.wait()

    def gather_y(b, yy):
        part = qbuf.at[b, c, yy, z]
        return remote(part, part, ay_s.at[b], ay_r.at[b], y_peer)

    def gather_up(b, origin, d):
        part = qbuf.at[b, c, :, origin]
        return remote(part, part, au_s.at[b, d - 1], au_r.at[b, d - 1], upper)

    def gather_down(b, origin, d):
        part = qbuf.at[b, c, :, origin]
        return remote(part, part, ad_s.at[b, d - 1], ad_r.at[b, d - 1], lower)

    def gather_c(b, cc):
        part = qbuf.at[b, cc]
        return remote(part, part, ac_s.at[b], ac_r.at[b], core_peer)

    def sum_c(b, hf):
        rows = pl.ds(hf * 16, 16)
        return remote(o_full.at[b, 1 - c, :, :, rows], rc_c.at[lax.rem(b, ring), :, :, rows], oc_s.at[b, hf], oc_r.at[b, hf], core_peer)

    def stat_c(b):
        return remote(ml0.at[b, 1 - c], ml_c.at[b], mc_s.at[b], mc_r.at[b], core_peer)

    def sum_y(b):
        return (remote(o_full.at[b, c, 1 - y], rc_y.at[lax.rem(b, ring)], oy_s.at[b], oy_r.at[b], y_peer),
                remote(ml1.at[b], ml_y.at[b], my_s.at[b], my_r.at[b], y_peer))

    def sum_up(b, dest, d):
        return remote(o_full.at[b, c, y, dest], rc_u.at[b, dest], ou_s.at[b, d - 1], ou_r.at[b, d - 1], upper)

    def stat_up(b, stat):
        return remote(stat.at[b], ml_u.at[b], mu_s.at[b], mu_r.at[b], upper)

    def sum_down(b, dest, d):
        return remote(o_full.at[b, c, y, dest], rc_d.at[b, dest], od_s.at[b, d - 1], od_r.at[b, d - 1], lower)

    def stat_down(b, stat):
        return remote(stat.at[b], ml_d.at[b], md_s.at[b], md_r.at[b], lower)

    def pass_on(b, d):
        @pl.when((z < NZ - 1) & (z - (d - 1) >= 0))
        def _():
            gather_up(b, z - (d - 1), d).start()

        @pl.when((z > 0) & (z + (d - 1) < NZ))
        def _():
            gather_down(b, z + (d - 1), d).start()

    def arrive(b, d):
        @pl.when(z - d >= 0)
        def _():
            gather_up(b, z - d, d).wait_recv()

        @pl.when(z + d < NZ)
        def _():
            gather_down(b, z + d, d).wait_recv()

    def step_z1(b):
        gather_y(b, 1 - y).wait_recv()
        pass_on(b, 1)

    def step_z2(b):
        arrive(b, 1)
        pass_on(b, 2)

    def step_z3(b):
        arrive(b, 2)
        pass_on(b, 3)

    def step_z4(b):
        arrive(b, 3)
        gather_c(b, c).start()

    def attend(b):
        gather_c(b, 1 - c).wait_recv()
        for cp in cache(b):
            cp.wait()

        @pl.when(b + slots - 1 < nb)
        def _():
            for cp in cache(b + slots - 1):
                cp.start()

        k = lax.rem(b, slots)
        row_len = lens[b]
        pos = s * local_len + lax.broadcasted_iota(jnp.int32, (512, local_len), 1)
        row = lax.broadcasted_iota(jnp.int32, (512, 1), 0)
        token = (row // 256) * 2 + lax.rem(row, 16) // 8
        lane = lax.broadcasted_iota(jnp.int32, (512, 128), 1)
        q = jnp.concatenate(
            [jnp.concatenate([qbuf[b, :, :, :, hf * 4 + j].reshape(256, 128) for j in range(4)], axis=1) for hf in range(2)], axis=0)
        both = qbuf[b, :, :, :, 8].reshape(256, 128)
        qr = jnp.concatenate([both[:, :64], both[:, 64:]], axis=0)
        sc = lax.dot_general(q, ck[k], (((1,), (1,)), ((), ())), preferred_element_type=f32)
        sc = sc + jnp.dot(qr, kr[k], preferred_element_type=f32)
        sc = jnp.where(pos <= row_len + token, sc, MASK_FILL)
        m = jnp.max(sc, axis=1, keepdims=True)
        p = jnp.exp2((sc - m) * scale)
        l = jnp.sum(p, axis=1, keepdims=True)
        o = jnp.dot(p.astype(bf16), ck[k], preferred_element_type=f32)
        stat = jnp.where(lane == 0, m * scale, jnp.where(lane == 1, l, 0.0)).T
        for hf in range(2):
            o_full[b, :, :, :, hf * 16:(hf + 1) * 16, :] = o[hf * 256:(hf + 1) * 256].reshape(2, 2, 4, 16, o.shape[1])
            for cc in range(2):
                at = hf * 256 + cc * 128
                ml0[b, cc, hf * 2:hf * 2 + 2, :] = stat[0:2, at:at + 128]
            sum_c(b, hf).start()
        stat_c(b).start()

    def merge_stats(parts, final):
        stats, factors = [], []
        for hf in range(2):
            ms, ls = [p[2 * hf:2 * hf + 1] for p in parts], [p[2 * hf + 1:2 * hf + 2] for p in parts]
            top = functools.reduce(jnp.maximum, ms)
            ws = [jnp.exp2(m - top) for m in ms]
            total = sum(w * l for w, l in zip(ws, ls))
            stats += [top, total]
            factors += [w / total for w in ws] if final else ws
        return jnp.concatenate(stats, axis=0), columns(jnp.concatenate(factors, axis=0))

    def step_d(b):
        for hf in range(2):
            sum_c(b, hf).wait_recv()
        stat_c(b).wait_recv()
        stats, cols = merge_stats([ml0[b, c, 0:4], ml_c[b, 0:4]], False)
        ml1[b, 0:4, :] = stats
        for hf in range(2):
            rows = pl.ds(hf * 16, 16)
            wa, wb = (cols[:, 2 * hf + j:2 * hf + j + 1].reshape(2, 4, 16, 1) for j in range(2))
            o_full[b, c, :, :, rows, :] = o_full[b, c, :, :, rows, :] * wa + rc_c[lax.rem(b, ring), :, :, rows, :] * wb
        for cp in sum_y(b):
            cp.start()

    def step_e(b):
        for cp in sum_y(b):
            cp.wait_recv()
        stats, cols = merge_stats([ml1[b, 0:4], ml_y[b, 0:4]], False)
        ml2[b, 0:4, :] = stats
        wcol[...] = cols
        cols = wcol[pl.ds(pl.multiple_of(y * 64, 64), 64), :]
        for hf in range(2):
            rows = pl.ds(hf * 16, 16)
            wa, wb = (cols[:, 2 * hf + j:2 * hf + j + 1].reshape(4, 16, 1) for j in range(2))
            o_full[b, c, y, :, rows, :] = o_full[b, c, y, :, rows, :] * wa + rc_y[lax.rem(b, ring), :, rows, :] * wb

        @pl.when(z == 0)
        def _():
            stat_up(b, ml2).start()
            for dest in range(NZ - 1, 0, -1):
                sum_up(b, dest, dest).start()

        @pl.when(z == NZ - 1)
        def _():
            stat_down(b, ml2).start()
            for dest in range(NZ - 1):
                sum_down(b, dest, NZ - 1 - dest).start()

    def relay(b, dests, stats_in, stats_out, arrived, wait, send):
        stats, cols = merge_stats([ml2[b, 0:4], stats_in[b, 0:4]], False)
        stats_out[b, 0:4, :] = stats
        wcol[...] = cols
        for i, dest in enumerate(dests):
            wait(dest)
            cols = wcol[pl.ds(pl.multiple_of(y * 64 + dest * 16, 16), 16), :]
            for hf in range(2):
                rows = pl.ds(hf * 16, 16)
                wa, wb = (cols[:, 2 * hf + j:2 * hf + j + 1] for j in range(2))
                o_full[b, c, y, dest, rows, :] = o_full[b, c, y, dest, rows, :] * wa + arrived[b, dest, rows, :] * wb
            if i == 0:
                send(None)
            send(dest)

    def step_g(hop, b):
        at = NZ - 1 - hop

        @pl.when(z == hop)
        def _():
            def send(dest):
                (stat_up(b, ml_us) if dest is None else sum_up(b, dest, dest - hop)).start()
            stat_up(b, ml2).wait_recv()
            relay(b, range(NZ - 1, hop, -1), ml_u, ml_us, rc_u, lambda dest: sum_up(b, dest, dest - hop + 1).wait_recv(), send)

        @pl.when(z == at)
        def _():
            def send(dest):
                (stat_down(b, ml_ds) if dest is None else sum_down(b, dest, at - dest)).start()
            stat_down(b, ml2).wait_recv()
            relay(b, range(at), ml_d, ml_ds, rc_d, lambda dest: sum_down(b, dest, at - dest + 1).wait_recv(), send)

    def finish(b, at):
        parts, sums = [ml2[b, 0:4]], [o_full.at[b, c, y, at]]
        if at > 0:
            sum_up(b, at, 1).wait_recv()
            if at == NZ - 1:
                stat_up(b, ml2).wait_recv()
            parts.append(ml_u[b, 0:4])
            sums.append(rc_u.at[b, at])
        if at < NZ - 1:
            sum_down(b, at, 1).wait_recv()
            if at == 0:
                stat_down(b, ml2).wait_recv()
            parts.append(ml_d[b, 0:4])
            sums.append(rc_d.at[b, at])
        wcol[...] = merge_stats(parts, True)[1]
        cols = wcol[pl.ds(pl.multiple_of(y * 64 + at * 16, 16), 16), :]
        n = len(parts)
        halves = []
        for hf in range(2):
            rows = pl.ds(hf * 16, 16)
            o = sum(part[rows, :] * cols[:, n * hf + j:n * hf + j + 1] for j, part in enumerate(sums))
            halves.append(o.astype(bf16))
        o = jnp.concatenate(halves, axis=0)
        head = lax.rem(lax.broadcasted_iota(jnp.int32, (32, 128), 0), 8)
        for h in range(8):
            v = jnp.dot(o, wuv[h], preferred_element_type=f32)
            v = jnp.where(head == h, v, 0.0).reshape(4, 8, 128).sum(axis=1)
            out[b, :, h * 128:(h + 1) * 128] = v.astype(bf16)

    def step_f(b):
        for at in range(NZ):
            @pl.when(z == at)
            def _(at=at):
                finish(b, at)

    @pl.loop(0, nb)
    def _(b):
        gather_y(b, y).start()

    steps = ((8, step_e), (6, step_d), (4, step_z4), (5, attend), (3, step_z3), (12, functools.partial(step_g, 2)),
             (2, step_z2), (0, step_z1), (14, step_f), (10, functools.partial(step_g, 1)))

    @pl.loop(0, nb + 14)
    def _(it):
        for lag, fn in steps:
            b = it - lag

            @pl.when((b >= 0) & (b < nb))
            def _(fn=fn, b=b):
                fn(b)

    own_h.wait()
    own_w.wait()

    @pl.loop(0, nb)
    def _(b):
        gather_y(b, y).wait_send()
        gather_c(b, c).wait_send()
        for d in (1, 2, 3):
            @pl.when((z < NZ - 1) & (z - (d - 1) >= 0))
            def _(d=d):
                gather_up(b, z - (d - 1), d).wait_send()

            @pl.when((z > 0) & (z + (d - 1) < NZ))
            def _(d=d):
                gather_down(b, z + (d - 1), d).wait_send()
        sum_c(b, 0).wait_send()
        sum_c(b, 1).wait_send()
        stat_c(b).wait_send()
        for cp in sum_y(b):
            cp.wait_send()
        for at in range(NZ):
            @pl.when(z == at)
            def _(at=at):
                for dest in range(at + 1, NZ):
                    sum_up(b, dest, dest - at).wait_send()
                if at < NZ - 1:
                    stat_up(b, ml2).wait_send()
                for dest in range(at):
                    sum_down(b, dest, at - dest).wait_send()
                if at > 0:
                    stat_down(b, ml2).wait_send()


def attend_all(q, q_rope, lens, c_kv, k_t, hidden, w_o, w_uv, score_scale):
    nb, local_len, lat = c_kv.shape
    nq, dim = hidden.shape[1:]
    slots = 3
    dma = pltpu.SemaphoreType.DMA
    return pl.pallas_call(
        functools.partial(attend_kernel, score_scale * math.log2(math.e)),
        out_shape=(pltpu.VMEM((nb, nq, w_uv.shape[0] * w_uv.shape[2]), bf16),
                   pltpu.VMEM((nb // NZ, nq, dim // 4), bf16),
                   pltpu.VMEM(w_o.shape, bf16)),
        in_specs=[pl.BlockSpec(memory_space=pltpu.SMEM)] + [pl.BlockSpec(memory_space=pl.ANY)] * 6
        + [pl.BlockSpec(memory_space=pltpu.VMEM)],
        out_specs=(pl.BlockSpec(memory_space=pltpu.VMEM), pl.BlockSpec(memory_space=pltpu.VMEM),
                   pl.BlockSpec(memory_space=pl.ANY)),
        scratch_shapes=[
            pltpu.VMEM((nb, 2, 2, 4, 9, 16, 128), bf16),
            pltpu.VMEM((slots, local_len, lat), bf16),
            pltpu.VMEM((slots, k_t.shape[1], local_len), bf16),
            pltpu.VMEM((nb, 2, 2, 4, 32, lat), f32),
            pltpu.VMEM((nb, 2, 8, 128), f32),
            pltpu.VMEM((nb, 8, 128), f32),
            pltpu.VMEM((nb, 8, 128), f32),
            pltpu.VMEM((4, 2, 4, 32, lat), f32),
            pltpu.VMEM((nb, 8, 128), f32),
            pltpu.VMEM((4, 4, 32, lat), f32),
            pltpu.VMEM((nb, 8, 128), f32),
            pltpu.VMEM((nb, 4, 32, lat), f32),
            pltpu.VMEM((nb, 8, 128), f32),
            pltpu.VMEM((nb, 8, 128), f32),
            pltpu.VMEM((nb, 4, 32, lat), f32),
            pltpu.VMEM((nb, 8, 128), f32),
            pltpu.VMEM((nb, 8, 128), f32),
            pltpu.VMEM((128, 128), f32),
            dma((2,)), dma, dma, dma((slots,)), dma((slots,)),
            dma((nb,)), dma((nb,)), dma((nb, 3)), dma((nb, 3)), dma((nb, 3)), dma((nb, 3)), dma((nb,)), dma((nb,)),
            dma((nb, 2)), dma((nb, 2)), dma((nb,)), dma((nb,)), dma((nb, 3)), dma((nb, 3)), dma((nb, 3)), dma((nb, 3)),
            dma((nb,)), dma((nb,)), dma((nb,)), dma((nb,)), dma((nb,)), dma((nb,)), dma((nb,)), dma((nb,)),
        ],
        compiler_params=pltpu.CompilerParams(
            collective_id=0, has_side_effects=True, vmem_limit_bytes=ATTEND_VMEM),
        name="attend_all",
    )(lens, q, q_rope, c_kv, k_t, hidden, w_o, w_uv)


def rope_kernel(h_ref, w_ref, out, flat, rows):
    head = pl.program_id(0)
    nb, nq, _ = h_ref.shape

    @pl.when(head == 0)
    def _():
        flat[...] = h_ref[...].astype(f32).reshape(flat.shape).astype(bf16)

    rows[head] = lax.dot_general(flat[...], w_ref[0], (((1,), (1,)), ((), ())), preferred_element_type=f32)

    @pl.when(head == pl.num_programs(0) - 1)
    def _():
        pairs = jnp.stack([rows[h] for h in range(8)], axis=1).reshape(nb, 2, 16, 64)
        out[...] = jnp.concatenate([pairs[:, 0], pairs[:, 1]], axis=-1).astype(bf16)


def rope_queries(hidden, w_t):
    nb, nq, dim = hidden.shape
    heads, wide = w_t.shape[:2]
    return pl.pallas_call(
        rope_kernel,
        grid=(heads,),
        out_shape=jax.ShapeDtypeStruct((nb, 16, 128), bf16),
        in_specs=[pl.BlockSpec((nb, nq, dim), lambda i: (0, 0, 0)), pl.BlockSpec((1, wide, dim), lambda i: (i, 0, 0))],
        out_specs=pl.BlockSpec((nb, 16, 128), lambda i: (0, 0, 0)),
        scratch_shapes=[pltpu.VMEM((nb * nq, dim), bf16), pltpu.VMEM((heads, nb * nq, wide), f32)],
        compiler_params=pltpu.CompilerParams(dimension_semantics=("arbitrary",)),
        name="rope_queries",
    )(hidden, w_t)


def total_kernel(ov_ref, w_ref, hbuf, out, ov_rows, part, gat, rc_c, rc_y, rc_z,
                 sc_s, sc_r, sy_s, sy_r, sz_s, sz_r, gz_s, gz_r, gy_s, gy_r, gc_s, gc_r):
    _, z, y, c = place()
    chunks, lanes = part.shape[0], part.shape[4]
    deep = part.shape[3] // NZ
    core_peer, y_peer = seq_of(z, y, 1 - c), seq_of(z, 1 - y, c)
    zs = [lax.rem(z + d, NZ) for d in (1, 2, 3)]
    zf = [lax.rem(z + NZ - d, NZ) for d in (1, 2, 3)]

    def where(cc, yy, k):
        return pl.ds(pl.multiple_of((cc * NY + yy) * (chunks * lanes) + k * lanes, 128), lanes)

    nb = ov_ref.shape[0]
    ov_rows[...] = ov_ref[...].astype(f32).reshape(ov_rows.shape).astype(bf16)
    meet([core_peer, y_peer] + [seq_of(p, y, c) for p in zs])

    def band(at):
        return pl.ds(pl.multiple_of(at * deep, deep), deep)

    def sum_c(k):
        return remote(part.at[k, 1 - c], rc_c.at[k], sc_s.at[k], sc_r.at[k], core_peer)

    def sum_y(k):
        return remote(part.at[k, c, 1 - y], rc_y.at[k], sy_s.at[k], sy_r.at[k], y_peer)

    def sum_z(k, d):
        return remote(part.at[k, c, y, band(zs[d])], rc_z.at[k, d], sz_s.at[k, d], sz_r.at[k, d], seq_of(zs[d], y, c))

    def give_z(k, d, at):
        piece = gat.at[k, c, y, band(at)]
        return remote(piece, piece, gz_s.at[k, d], gz_r.at[k, d], seq_of(zs[d], y, c))

    def give_y(k, yy):
        return remote(gat.at[k, c, yy], gat.at[k, c, yy], gy_s.at[k], gy_r.at[k], y_peer)

    def give_c(k, cc):
        return remote(gat.at[k, cc], gat.at[k, cc], gc_s.at[k], gc_r.at[k], core_peer)

    def multiply(k):
        ov = ov_rows[...]
        for cc in (1 - c, c):
            for yy in range(2):
                part[k, cc, yy] = jnp.dot(ov, w_ref[:, where(cc, yy, k)], preferred_element_type=f32)
            if cc is not c:
                sum_c(k).start()

    def step_d(k):
        sum_c(k).wait_recv()
        part[k, c] = part[k, c] + rc_c[k]
        sum_y(k).start()

    def step_e(k):
        sum_y(k).wait_recv()
        part[k, c, y] = part[k, c, y] + rc_y[k]
        for d in range(3):
            sum_z(k, d).start()

    def step_f(k):
        for d in range(3):
            sum_z(k, d).wait_recv()
        total = part[k, c, y, band(z)] + rc_z[k, 0] + rc_z[k, 1] + rc_z[k, 2]
        own = hbuf[:, :, pl.ds(pl.multiple_of(k * lanes, 128), lanes)].astype(f32).reshape(deep, lanes)
        gat[k, c, y, band(z)] = (own + total).astype(bf16)
        for d in range(3):
            give_z(k, d, z).start()

    def step_h(k):
        for d in range(3):
            give_z(k, d, zf[d]).wait_recv()
        give_y(k, y).start()

    def step_i(k):
        give_y(k, 1 - y).wait_recv()
        give_c(k, c).start()

    def step_j(k):
        give_c(k, 1 - c).wait_recv()
        for cc in range(2):
            for yy in range(2):
                out[:, :, where(cc, yy, k)] = gat[k, cc, yy].astype(f32).reshape(nb, -1, lanes).astype(bf16)

    steps = ((4, step_e), (12, step_h), (15, step_i), (0, multiply), (1, step_d), (17, step_j), (7, step_f))

    @pl.loop(0, chunks + 17)
    def _(it):
        for lag, fn in steps:
            k = it - lag

            @pl.when((k >= 0) & (k < chunks))
            def _(fn=fn, k=k):
                fn(k)

    @pl.loop(0, chunks)
    def _(k):
        sum_c(k).wait_send()
        sum_y(k).wait_send()
        for d in range(3):
            sum_z(k, d).wait_send()
            give_z(k, d, z).wait_send()
        give_y(k, y).wait_send()
        give_c(k, c).wait_send()


def total_all(ov, w_o, own_h):
    (nb, nq, _), dim = ov.shape, w_o.shape[1]
    n = nb * nq
    chunks = next(k for k in (7, 1) if dim % (4 * k * 128) == 0)
    lanes = dim // (4 * chunks)
    dma = pltpu.SemaphoreType.DMA
    vm = pl.BlockSpec(memory_space=pltpu.VMEM)
    one, three = dma((chunks,)), dma((chunks, 3))
    return pl.pallas_call(
        total_kernel,
        out_shape=pltpu.VMEM((nb, nq, dim), bf16),
        in_specs=[vm, vm, vm],
        out_specs=vm,
        scratch_shapes=[
            pltpu.VMEM((n, w_o.shape[0]), bf16),
            pltpu.VMEM((chunks, 2, 2, n, lanes), f32),
            pltpu.VMEM((chunks, 2, 2, n, lanes), bf16),
            pltpu.VMEM((chunks, 2, n, lanes), f32),
            pltpu.VMEM((chunks, n, lanes), f32),
            pltpu.VMEM((chunks, 3, n // NZ, lanes), f32),
            one, one, one, one, three, three, three, three, one, one, one, one,
        ],
        compiler_params=pltpu.CompilerParams(
            collective_id=1, has_side_effects=True, vmem_limit_bytes=24 * 1024 * 1024),
        name="total_all",
    )(ov, w_o, own_h)


def solution(mesh):
    def local_step(hidden, cache_lens, c_kv, k_r, w_uq, w_qr, w_uk, w_uv, w_o):
        score_scale = (w_uq.shape[2] + w_qr.shape[2]) ** -0.5
        nb, nq, dim = hidden.shape
        nh, lat = w_uk.shape[0], w_uk.shape[2]
        q_nope = jnp.einsum("cre,eil->cril", hidden, w_uq, preferred_element_type=f32).astype(bf16)
        q_lat = jnp.einsum("bqhk,hkc->bqhc", q_nope, w_uk, preferred_element_type=f32).astype(bf16)
        q = q_lat.reshape(nb, 2, 16, 4, 128).transpose(0, 1, 3, 2, 4).reshape(nb, 8, 16, 128)
        q_rope = rope_queries(hidden, w_qr.transpose(1, 2, 0))
        o_val, own_h, own_w = attend_all(q, q_rope, cache_lens, c_kv, jnp.swapaxes(k_r, 1, 2), hidden, w_o.reshape(-1, dim), w_uv, score_scale)
        return total_all(*(pltpu.with_memory_space_constraint(v, pltpu.VMEM) for v in (o_val, own_w, own_h)))

    specs_in = (P("batch", None, None), P("batch"), P("batch", "seq", None), P("batch", "seq", None),
                P(None, "seq", None), P(None, "seq", None), P("seq", None, None), P("seq", None, None),
                P("seq", None, None))
    return jax.shard_map(local_step, mesh=mesh, in_specs=specs_in, out_specs=P("batch", None, None), check_vma=False)
```
